16 devices in a mesh: dp: 2 (over y, z), dcp: 8 (over x, core).
Axes of the slice: x: 4, y: 2, z: 1, core: 2. Of those that a mesh axis runs over, the one named last changes fastest.
The devices are a block of a 4x4x8 slice.
Arguments:
- q_abs: bfloat16 [128, 128, 576], P('dp', 'dcp'), parts along dimension 0
- cache: bfloat16 [128, 8192, 576], P('dp', 'dcp'), parts along dimension 0
- lengths: int32 [128], P('dp'), parts along dimension 0
Outputs:
- output: bfloat16 [128, 128, 512], P('dp', 'dcp'), parts along dimension 0
There are 2 independent parts. The reference program is written for one: setup_inputs(seed, part) draws one part's arguments, and reference() takes and returns one part's arrays. A program takes and returns all parts, laid end to end along the dimension named above; each array names one.
All inputs are finite; a program needn't handle non-finite values.
Results may differ from the reference program's by a relative error of at most 0.00748833.
Values are sent between devices in bfloat16 or wider.
A program may use at most 768 MiB of HBM per device.

```python
import jax
import jax.numpy as jnp
from jax import lax

HEADS = 128
KV_RANK = 512
ROPE = 64
QK_NOPE = 128
B = 64
S = 8192
NDEV = 8

WIDTH = KV_RANK + ROPE
SCALE = (QK_NOPE + ROPE) ** -0.5
BLOCK = S // NDEV
SEG = S // 32


def setup_inputs(seed: int = 0, part: int = 0) -> dict:
    key = jax.random.fold_in(jax.random.key(seed), part)
    kq, kc, kf, ks = jax.random.split(key, 4)
    q_abs = (jax.random.normal(kq, (B, HEADS, WIDTH), jnp.float32) * 0.6).astype(jnp.bfloat16)

    def draw(k):
        k1, k2, k3 = jax.random.split(k, 3)
        seg = jax.random.normal(k1, (32, KV_RANK), jnp.float32)
        lat = jax.random.normal(k2, (S, KV_RANK), jnp.float32) + jnp.repeat(seg, SEG, axis=0)
        rope = jax.random.normal(k3, (S, ROPE), jnp.float32) * 3.0
        return jnp.concatenate([lat, rope], axis=1).astype(jnp.bfloat16)

    cache = lax.map(draw, jax.random.split(kc, B))
    full = S - jax.random.randint(kf, (B,), 0, S // 64)
    short = jax.random.randint(ks, (B,), 1, S + 1)
    lengths = jnp.where(jnp.arange(B) % 2 == 0, full, short).astype(jnp.int32)
    return {'q_abs': q_abs, 'cache': cache, 'lengths': lengths}


def reference(q_abs, cache, lengths):
    pos = jnp.arange(S).reshape(NDEV, BLOCK)

    def one(args):
        qb, cb, lb = args
        cf = cb.astype(jnp.float32).reshape(NDEV, BLOCK, WIDTH)
        s = jnp.einsum('hk,ntk->nht', qb.astype(jnp.float32), cf) * SCALE
        valid = pos < lb
        s = jnp.where(valid[:, None, :], s, -jnp.inf)
        m = jnp.max(s, axis=2)
        m0 = jnp.where(jnp.isfinite(m), m, 0.0)
        p = jnp.exp(s - m0[:, :, None])
        l = jnp.sum(p, axis=2)
        pb = p.astype(jnp.bfloat16).astype(jnp.float32)
        pv = jnp.einsum('nht,ntc->nhc', pb, cf[:, :, :KV_RANK])
        has = l > 0.0
        l1 = jnp.where(has, l, 1.0)
        od = (pv / l1[:, :, None]).astype(jnp.bfloat16).astype(jnp.float32)
        lse_d = jnp.where(has, m0 + jnp.log(l1), -jnp.inf)
        mx = jnp.max(lse_d, axis=0)
        lse = mx + jnp.log(jnp.sum(jnp.exp(lse_d - mx[None, :]), axis=0))
        o = jnp.sum(jnp.exp(lse_d - lse[None, :])[:, :, None] * od, axis=0)
        return o.astype(jnp.bfloat16)

    return lax.map(one, (q_abs, cache, lengths))
```

```python
import functools

import jax
import jax.numpy as jnp
from jax import lax
from jax.experimental import pallas as pl
from jax.experimental.pallas import tpu as pltpu
from jax.sharding import PartitionSpec as P

ROPE = 64
SCALE = 192 ** -0.5
CORES = 2
CHUNK = 8
PAIRS = 4
LAG_R = 1
LAG_F = 2

MESH = pl.DeviceIdType.MESH
F32 = jnp.float32
BF16 = jnp.bfloat16
VIA, DIRECT, MINE, PASS, SUM = 0, 2, 4, 5, 6


def weights(stats):
    top = functools.reduce(jnp.maximum, stats)
    top = jnp.maximum(top, jnp.finfo(F32).min)
    w = [jnp.exp(t - top) for t in stats]
    total = functools.reduce(jnp.add, w)
    inv = 1.0 / jnp.maximum(total, 1.0)
    return [x * inv for x in w], top + jnp.log(total)


def kernel(n, len_ref, q_ref, ct_ref, o_ref, qraw, qg, od, st, inc, ins, lg, rs, rss, obuf, cbuf,
           raw_sem, cache_sem, out_sem, q_send, q_recv, o_send, o_recv, t_send, t_recv):
    chips = n // CORES
    nb, hl, wd = q_ref.shape
    lat = wd - ROPE
    heads = n * hl
    sl = ct_ref.shape[2]
    nc = nb // CHUNK
    half = CHUNK // 2
    npair = nb // 2

    me = lax.axis_index('dcp')
    x = me // CORES
    k = me % CORES
    partner = x * CORES + (1 - k)

    def dev(step, core):
        return ((x + step + chips) % chips) * CORES + core

    def cache_copies(pair, par):
        slot = (pair % PAIRS) * 2 + par
        b = pair * 2 + par
        if par == 0:
            return [pltpu.make_async_copy(ct_ref.at[b], cbuf.at[slot, pl.ds(0, wd)], cache_sem.at[slot, 0])]
        return [
            pltpu.make_async_copy(ct_ref.at[b, pl.ds(0, lat)], cbuf.at[slot, pl.ds(0, lat)], cache_sem.at[slot, 0]),
            pltpu.make_async_copy(ct_ref.at[b, pl.ds(lat, ROPE)], cbuf.at[slot, pl.ds(wd, ROPE)], cache_sem.at[slot, 1]),
        ]

    def fetch(pair):
        for par in range(2):
            for cp in cache_copies(pair, par):
                cp.start()

    raw = pltpu.make_async_copy(q_ref, qraw, raw_sem)
    raw.start()

    barrier = pltpu.get_barrier_semaphore()
    peers = [partner, dev(1, 0), dev(1, 1), dev(-1, 0), dev(-1, 1)]
    for peer in peers:
        pl.semaphore_signal(barrier, inc=1, device_id={'dcp': peer}, device_id_type=MESH)

    for g in range(PAIRS):
        cbuf[2 * g, pl.ds(wd, ROPE), :] = jnp.zeros((ROPE, sl), BF16)
        cbuf[2 * g + 1, pl.ds(lat, ROPE), :] = jnp.zeros((ROPE, sl), BF16)
    raw.wait()

    def pack(g, _):
        for par in range(2):
            qg[me, g, :, pl.ds(par * lat, lat)] = qraw[2 * g + par, :, pl.ds(0, lat)]
        r0 = qraw[2 * g, :, pl.ds(lat, ROPE)]
        r1 = qraw[2 * g + 1, :, pl.ds(lat, ROPE)]
        qg[me, g, :, pl.ds(2 * lat, 2 * ROPE)] = jnp.concatenate([r0, r1], axis=1)
        return 0

    lax.fori_loop(0, npair, pack, 0)
    for g in range(PAIRS):
        fetch(g)
    pl.semaphore_wait(barrier, len(peers))

    def q_copy(kind, src, c, to):
        part = qg.at[src, pl.ds(c * half, half)]
        return pltpu.make_async_remote_copy(
            src_ref=part, dst_ref=part, send_sem=q_send.at[kind, c], recv_sem=q_recv.at[kind, c],
            device_id={'dcp': to}, device_id_type=MESH)

    def q_wait(kind, src, c):
        q_copy(kind, src, c, me).wait_recv()

    def sign(c):
        return 1 - 2 * (c % 2)

    def q0(c, _):
        q_copy(0, me, c, dev(1, k)).start()
        q_copy(1, me, c, dev(-1, k)).start()
        q_copy(2, me, c, partner).start()
        return 0

    lax.fori_loop(0, nc, q0, 0)

    def q1(c, _):
        way = -sign(c)
        q_wait(0, dev(-1, k), c)
        q_copy(3, dev(-1, k), c, partner).start()
        q_wait(1, dev(1, k), c)
        q_copy(4, dev(1, k), c, partner).start()
        q_copy(5, dev(-way, k), c, dev(way, k)).start()
        return 0

    lax.fori_loop(0, nc, q1, 0)

    def q2(c):
        q_wait(5, dev(2, k), c)
        q_copy(6, dev(2, k), c, partner).start()

    def q3(c):
        q_wait(2, partner, c)
        q_wait(3, dev(-1, 1 - k), c)
        q_wait(4, dev(1, 1 - k), c)
        q_wait(6, dev(2, 1 - k), c)

    lane = lax.broadcasted_iota(jnp.int32, (heads, 128), 1)
    where_t = lax.broadcasted_iota(jnp.int32, (1, sl), 1)
    base = me * sl

    def attend(c):
        def pair_step(i, stat):
            g = c * half + i
            for par in range(2):
                b = g * 2 + par
                slot = (g % PAIRS) * 2 + par
                for cp in cache_copies(g, par):
                    cp.wait()
                qa = qg[:, g, :, pl.ds(par * lat, lat)].reshape(heads, lat)
                qr = qg[:, g, :, pl.ds(2 * lat, 2 * ROPE)].reshape(heads, 2 * ROPE)
                s = jnp.dot(qa, cbuf[slot, pl.ds(0, lat), :], preferred_element_type=F32)
                s = s + jnp.dot(qr, cbuf[slot, pl.ds(lat, 2 * ROPE), :], preferred_element_type=F32)
                s = jnp.where(where_t < len_ref[b] - base, s * SCALE, -jnp.inf)
                m = jnp.maximum(jnp.max(s, axis=1, keepdims=True), jnp.finfo(F32).min)
                p = jnp.exp(s - m)
                l = jnp.sum(p, axis=1, keepdims=True)
                pv = lax.dot_general(p.astype(BF16), cbuf[slot, pl.ds(0, lat), :], (((1,), (1,)), ((), ())),
                                     preferred_element_type=F32)
                o = (pv * (1.0 / jnp.maximum(l, 1.0))).astype(BF16)
                od[:, b, :, :] = o.reshape(n, hl, lat)
                stat = jnp.where(lane == i * 2 + par, m + jnp.log(l), stat)

            @pl.when(g + PAIRS < npair)
            def _():
                fetch(g + PAIRS)

            return stat

        stat = lax.fori_loop(0, half, pair_step, jnp.full((heads, 128), -jnp.inf, F32))
        st[:, c, :, :] = stat.reshape(n, hl, 128)

    def rows(c):
        return pl.ds(c * CHUNK, CHUNK)

    def o_copies(c, head, slot_s, slot_r, to):
        return [
            pltpu.make_async_remote_copy(
                src_ref=od.at[head, rows(c)], dst_ref=inc.at[slot_r, rows(c)],
                send_sem=o_send.at[slot_s, c], recv_sem=o_recv.at[slot_r, c],
                device_id={'dcp': to}, device_id_type=MESH),
            pltpu.make_async_remote_copy(
                src_ref=st.at[head, c], dst_ref=ins.at[slot_r, c],
                send_sem=t_send.at[slot_s, c], recv_sem=t_recv.at[slot_r, c],
                device_id={'dcp': to}, device_id_type=MESH),
        ]

    def sends(c):
        way = sign(c)
        out = []
        for kk in range(CORES):
            out += o_copies(c, dev(2, kk), VIA + kk, VIA + k, dev(way, kk))
        out += o_copies(c, dev(way, 1 - k), PASS, PASS, partner)
        out += o_copies(c, partner, MINE, MINE, partner)
        for kk in range(CORES):
            out += o_copies(c, dev(-way, kk), DIRECT + kk, DIRECT + k, dev(-way, kk))
        return out

    def sum_copies(c):
        to = dev(sign(c), k)
        return [
            pltpu.make_async_remote_copy(
                src_ref=rs.at[rows(c)], dst_ref=lg.at[rows(c)], send_sem=o_send.at[SUM, c], recv_sem=o_recv.at[SUM, c],
                device_id={'dcp': to}, device_id_type=MESH),
            pltpu.make_async_remote_copy(
                src_ref=rss.at[c], dst_ref=ins.at[SUM, c], send_sem=t_send.at[SUM, c], recv_sem=t_recv.at[SUM, c],
                device_id={'dcp': to}, device_id_type=MESH),
        ]

    def o_wait(c, slot):
        for cp in o_copies(c, me, slot, slot, me):
            cp.wait_recv()

    def relay(c):
        for slot in (PASS, VIA, VIA + 1):
            o_wait(c, slot)
        mine = dev(sign(c), k)
        w, lse = weights([st[mine, c], ins[PASS, c], ins[VIA, c], ins[VIA + 1, c]])
        for i in range(CHUNK):
            b = c * CHUNK + i
            acc = w[0][:, i:i + 1] * od[mine, b].astype(F32)
            for j, slot in ((1, PASS), (2, VIA), (3, VIA + 1)):
                acc = acc + w[j][:, i:i + 1] * inc[slot, b].astype(F32)
            rs[b] = acc
        rss[c] = lse
        for cp in sum_copies(c):
            cp.start()

    def out_copy(c):
        return pltpu.make_async_copy(obuf.at[rows(c)], o_ref.at[rows(c)], out_sem.at[c])

    def merge(c):
        for slot in (MINE, DIRECT, DIRECT + 1):
            o_wait(c, slot)
        for cp in sum_copies(c):
            cp.wait_recv()
        w, _ = weights([st[me, c], ins[MINE, c], ins[DIRECT, c], ins[DIRECT + 1, c], ins[SUM, c]])
        for i in range(CHUNK):
            b = c * CHUNK + i
            acc = w[0][:, i:i + 1] * od[me, b].astype(F32)
            for j, slot in ((1, MINE), (2, DIRECT), (3, DIRECT + 1)):
                acc = acc + w[j][:, i:i + 1] * inc[slot, b].astype(F32)
            acc = acc + w[4][:, i:i + 1] * lg[b]
            obuf[b] = acc.astype(BF16)
        out_copy(c).start()

    q2(0)

    def step(t, _):
        @pl.when(t < nc)
        def _():
            @pl.when(t + 1 < nc)
            def _():
                q2(t + 1)

            q3(t)
            attend(t)
            for cp in sends(t):
                cp.start()

        @pl.when(jnp.logical_and(t >= LAG_R, t < nc + LAG_R))
        def _():
            relay(t - LAG_R)

        @pl.when(t >= LAG_F)
        def _():
            merge(t - LAG_F)

        return 0

    lax.fori_loop(0, nc + LAG_F, step, 0)

    def drain(c, _):
        for kind in range(7):
            q_copy(kind, me, c, me).wait_send()
        for cp in sends(c) + sum_copies(c):
            cp.wait_send()
        out_copy(c).wait()
        return 0

    lax.fori_loop(0, nc, drain, 0)


def solution(mesh):
    n = mesh.shape['dcp']

    def local(q, cache, lengths):
        nb, hl, wd = q.shape
        sl = cache.shape[1]
        lat = wd - ROPE
        nc = nb // CHUNK
        anyspace = pl.BlockSpec(memory_space=pl.ANY)
        dma = pltpu.SemaphoreType.DMA
        return pl.pallas_call(
            functools.partial(kernel, n),
            out_shape=jax.ShapeDtypeStruct((nb, hl, lat), BF16),
            in_specs=[pl.BlockSpec(memory_space=pltpu.SMEM), anyspace, anyspace],
            out_specs=anyspace,
            scratch_shapes=[
                pltpu.VMEM((nb, hl, wd), BF16),
                pltpu.VMEM((n, nb // 2, hl, 2 * wd), BF16),
                pltpu.VMEM((n, nb, hl, lat), BF16),
                pltpu.VMEM((n, nc, hl, 128), F32),
                pltpu.VMEM((6, nb, hl, lat), BF16),
                pltpu.VMEM((7, nc, hl, 128), F32),
                pltpu.VMEM((nb, hl, lat), F32),
                pltpu.VMEM((nb, hl, lat), F32),
                pltpu.VMEM((nc, hl, 128), F32),
                pltpu.VMEM((nb, hl, lat), BF16),
                pltpu.VMEM((2 * PAIRS, wd + ROPE, sl), BF16),
                dma,
                dma((2 * PAIRS, 2)),
                dma((nc,)),
                dma((7, nc)),
                dma((7, nc)),
                dma((7, nc)),
                dma((7, nc)),
                dma((7, nc)),
                dma((7, nc)),
            ],
            compiler_params=pltpu.CompilerParams(
                collective_id=0, has_side_effects=True, vmem_limit_bytes=63 * 1024 * 1024),
            name='mla_decode',
        )(lengths, q, jnp.swapaxes(cache, 1, 2))

    return jax.shard_map(local, mesh=mesh, in_specs=(P('dp', 'dcp', None), P('dp', 'dcp', None), P('dp')),
                         out_specs=P('dp', 'dcp', None), check_vma=False)
```

```python
import functools

import jax
import jax.numpy as jnp
from jax import lax
from jax.experimental import pallas as pl
from jax.experimental.pallas import tpu as pltpu
from jax.sharding import PartitionSpec as P

ROPE = 64
SCALE = 192 ** -0.5
CORES = 2
CHUNK = 8
PAIRS = 4
LAG_R = 2
LAG_F = 4

MESH = pl.DeviceIdType.MESH
F32 = jnp.float32
BF16 = jnp.bfloat16
VIA, DIRECT, MINE, PASS, SUM = 0, 2, 4, 5, 6


def weights(stats):
    top = functools.reduce(jnp.maximum, stats)
    top = jnp.maximum(top, jnp.finfo(F32).min)
    w = [jnp.exp(t - top) for t in stats]
    total = functools.reduce(jnp.add, w)
    inv = 1.0 / jnp.maximum(total, 1.0)
    return [x * inv for x in w], top + jnp.log(total)


def kernel(n, len_ref, q_ref, ct_ref, o_ref, qraw, qg, od, st, inc, ins, lg, rs, rss, obuf, cbuf,
           raw_sem, cache_sem, out_sem, q_send, q_recv, o_send, o_recv, t_send, t_recv):
    chips = n // CORES
    nb, hl, wd = q_ref.shape
    lat = wd - ROPE
    heads = n * hl
    sl = ct_ref.shape[2]
    nc = nb // CHUNK
    half = CHUNK // 2
    npair = nb // 2

    me = lax.axis_index('dcp')
    x = me // CORES
    k = me % CORES
    partner = x * CORES + (1 - k)

    def dev(step, core):
        return ((x + step + chips) % chips) * CORES + core

    def cache_copies(pair, par):
        slot = (pair % PAIRS) * 2 + par
        b = pair * 2 + par
        if par == 0:
            return [pltpu.make_async_copy(ct_ref.at[b], cbuf.at[slot, pl.ds(0, wd)], cache_sem.at[slot, 0])]
        return [
            pltpu.make_async_copy(ct_ref.at[b, pl.ds(0, lat)], cbuf.at[slot, pl.ds(0, lat)], cache_sem.at[slot, 0]),
            pltpu.make_async_copy(ct_ref.at[b, pl.ds(lat, ROPE)], cbuf.at[slot, pl.ds(wd, ROPE)], cache_sem.at[slot, 1]),
        ]

    def fetch(pair):
        for par in range(2):
            for cp in cache_copies(pair, par):
                cp.start()

    raw = pltpu.make_async_copy(q_ref, qraw, raw_sem)
    raw.start()

    barrier = pltpu.get_barrier_semaphore()
    peers = [partner, dev(1, 0), dev(1, 1), dev(-1, 0), dev(-1, 1)]
    for peer in peers:
        pl.semaphore_signal(barrier, inc=1, device_id={'dcp': peer}, device_id_type=MESH)

    for g in range(PAIRS):
        cbuf[2 * g, pl.ds(wd, ROPE), :] = jnp.zeros((ROPE, sl), BF16)
        cbuf[2 * g + 1, pl.ds(lat, ROPE), :] = jnp.zeros((ROPE, sl), BF16)
    raw.wait()

    def pack(g, _):
        for par in range(2):
            qg[me, g, :, pl.ds(par * lat, lat)] = qraw[2 * g + par, :, pl.ds(0, lat)]
        r0 = qraw[2 * g, :, pl.ds(lat, ROPE)]
        r1 = qraw[2 * g + 1, :, pl.ds(lat, ROPE)]
        qg[me, g, :, pl.ds(2 * lat, 2 * ROPE)] = jnp.concatenate([r0, r1], axis=1)
        return 0

    lax.fori_loop(0, npair, pack, 0)
    for g in range(PAIRS):
        fetch(g)
    pl.semaphore_wait(barrier, len(peers))

    def q_copy(kind, src, c, to):
        part = qg.at[src, pl.ds(c * half, half)]
        return pltpu.make_async_remote_copy(
            src_ref=part, dst_ref=part, send_sem=q_send.at[kind, c], recv_sem=q_recv.at[kind, c],
            device_id={'dcp': to}, device_id_type=MESH)

    def q_wait(kind, src, c):
        q_copy(kind, src, c, me).wait_recv()

    def sign(c):
        return 1 - 2 * (c % 2)

    def q0(c, _):
        q_copy(0, me, c, dev(1, k)).start()
        q_copy(1, me, c, dev(-1, k)).start()
        q_copy(2, me, c, partner).start()
        return 0

    lax.fori_loop(0, nc, q0, 0)

    def q1(c, _):
        way = -sign(c)
        q_wait(0, dev(-1, k), c)
        q_copy(3, dev(-1, k), c, partner).start()
        q_wait(1, dev(1, k), c)
        q_copy(4, dev(1, k), c, partner).start()
        q_copy(5, dev(-way, k), c, dev(way, k)).start()
        return 0

    lax.fori_loop(0, nc, q1, 0)

    def q2(c):
        q_wait(5, dev(2, k), c)
        q_copy(6, dev(2, k), c, partner).start()

    def q3(c):
        q_wait(2, partner, c)
        q_wait(3, dev(-1, 1 - k), c)
        q_wait(4, dev(1, 1 - k), c)
        q_wait(6, dev(2, 1 - k), c)

    lane = lax.broadcasted_iota(jnp.int32, (heads, 128), 1)
    where_t = lax.broadcasted_iota(jnp.int32, (1, sl), 1)
    base = me * sl

    def attend(c):
        def pair_step(i, stat):
            g = c * half + i
            for par in range(2):
                b = g * 2 + par
                slot = (g % PAIRS) * 2 + par
                for cp in cache_copies(g, par):
                    cp.wait()
                qa = qg[:, g, :, pl.ds(par * lat, lat)].reshape(heads, lat)
                qr = qg[:, g, :, pl.ds(2 * lat, 2 * ROPE)].reshape(heads, 2 * ROPE)
                s = jnp.dot(qa, cbuf[slot, pl.ds(0, lat), :], preferred_element_type=F32)
                s = s + jnp.dot(qr, cbuf[slot, pl.ds(lat, 2 * ROPE), :], preferred_element_type=F32)
                s = jnp.where(where_t < len_ref[b] - base, s * SCALE, -jnp.inf)
                m = jnp.maximum(jnp.max(s, axis=1, keepdims=True), jnp.finfo(F32).min)
                p = jnp.exp(s - m)
                l = jnp.sum(p, axis=1, keepdims=True)
                pv = lax.dot_general(p.astype(BF16), cbuf[slot, pl.ds(0, lat), :], (((1,), (1,)), ((), ())),
                                     preferred_element_type=F32)
                o = (pv * (1.0 / jnp.maximum(l, 1.0))).astype(BF16)
                od[:, b, :, :] = o.reshape(n, hl, lat)
                stat = jnp.where(lane == i * 2 + par, m + jnp.log(l), stat)

            @pl.when(g + PAIRS < npair)
            def _():
                fetch(g + PAIRS)

            return stat

        stat = lax.fori_loop(0, half, pair_step, jnp.full((heads, 128), -jnp.inf, F32))
        st[:, c, :, :] = stat.reshape(n, hl, 128)

    def rows(c):
        return pl.ds(c * CHUNK, CHUNK)

    def o_copies(c, head, slot_s, slot_r, to):
        return [
            pltpu.make_async_remote_copy(
                src_ref=od.at[head, rows(c)], dst_ref=inc.at[slot_r, rows(c)],
                send_sem=o_send.at[slot_s, c], recv_sem=o_recv.at[slot_r, c],
                device_id={'dcp': to}, device_id_type=MESH),
            pltpu.make_async_remote_copy(
                src_ref=st.at[head, c], dst_ref=ins.at[slot_r, c],
                send_sem=t_send.at[slot_s, c], recv_sem=t_recv.at[slot_r, c],
                device_id={'dcp': to}, device_id_type=MESH),
        ]

    def sends(c):
        way = sign(c)
        out = []
        for kk in range(CORES):
            out += o_copies(c, dev(2, kk), VIA + kk, VIA + k, dev(way, kk))
        out += o_copies(c, dev(way, 1 - k), PASS, PASS, partner)
        out += o_copies(c, partner, MINE, MINE, partner)
        for kk in range(CORES):
            out += o_copies(c, dev(-way, kk), DIRECT + kk, DIRECT + k, dev(-way, kk))
        return out

    def sum_copies(c):
        to = dev(sign(c), k)
        return [
            pltpu.make_async_remote_copy(
                src_ref=rs.at[rows(c)], dst_ref=lg.at[rows(c)], send_sem=o_send.at[SUM, c], recv_sem=o_recv.at[SUM, c],
                device_id={'dcp': to}, device_id_type=MESH),
            pltpu.make_async_remote_copy(
                src_ref=rss.at[c], dst_ref=ins.at[SUM, c], send_sem=t_send.at[SUM, c], recv_sem=t_recv.at[SUM, c],
                device_id={'dcp': to}, device_id_type=MESH),
        ]

    def o_wait(c, slot):
        for cp in o_copies(c, me, slot, slot, me):
            cp.wait_recv()

    def relay(c):
        for slot in (PASS, VIA, VIA + 1):
            o_wait(c, slot)
        mine = dev(sign(c), k)
        w, lse = weights([st[mine, c], ins[PASS, c], ins[VIA, c], ins[VIA + 1, c]])
        for i in range(CHUNK):
            b = c * CHUNK + i
            acc = w[0][:, i:i + 1] * od[mine, b].astype(F32)
            for j, slot in ((1, PASS), (2, VIA), (3, VIA + 1)):
                acc = acc + w[j][:, i:i + 1] * inc[slot, b].astype(F32)
            rs[b] = acc
        rss[c] = lse
        for cp in sum_copies(c):
            cp.start()

    def out_copy(c):
        return pltpu.make_async_copy(obuf.at[rows(c)], o_ref.at[rows(c)], out_sem.at[c])

    def merge(c):
        for slot in (MINE, DIRECT, DIRECT + 1):
            o_wait(c, slot)
        for cp in sum_copies(c):
            cp.wait_recv()
        w, _ = weights([st[me, c], ins[MINE, c], ins[DIRECT, c], ins[DIRECT + 1, c], ins[SUM, c]])
        for i in range(CHUNK):
            b = c * CHUNK + i
            acc = w[0][:, i:i + 1] * od[me, b].astype(F32)
            for j, slot in ((1, MINE), (2, DIRECT), (3, DIRECT + 1)):
                acc = acc + w[j][:, i:i + 1] * inc[slot, b].astype(F32)
            acc = acc + w[4][:, i:i + 1] * lg[b]
            obuf[b] = acc.astype(BF16)
        out_copy(c).start()

    q2(0)

    def step(t, _):
        @pl.when(t < nc)
        def _():
            @pl.when(t + 1 < nc)
            def _():
                q2(t + 1)

            q3(t)
            attend(t)
            for cp in sends(t):
                cp.start()

        @pl.when(jnp.logical_and(t >= LAG_R, t < nc + LAG_R))
        def _():
            relay(t - LAG_R)

        @pl.when(t >= LAG_F)
        def _():
            merge(t - LAG_F)

        return 0

    lax.fori_loop(0, nc + LAG_F, step, 0)

    def drain(c, _):
        for kind in range(7):
            q_copy(kind, me, c, me).wait_send()
        for cp in sends(c) + sum_copies(c):
            cp.wait_send()
        out_copy(c).wait()
        return 0

    lax.fori_loop(0, nc, drain, 0)


def solution(mesh):
    n = mesh.shape['dcp']

    def local(q, cache, lengths):
        nb, hl, wd = q.shape
        sl = cache.shape[1]
        lat = wd - ROPE
        nc = nb // CHUNK
        anyspace = pl.BlockSpec(memory_space=pl.ANY)
        dma = pltpu.SemaphoreType.DMA
        return pl.pallas_call(
            functools.partial(kernel, n),
            out_shape=jax.ShapeDtypeStruct((nb, hl, lat), BF16),
            in_specs=[pl.BlockSpec(memory_space=pltpu.SMEM), anyspace, anyspace],
            out_specs=anyspace,
            scratch_shapes=[
                pltpu.VMEM((nb, hl, wd), BF16),
                pltpu.VMEM((n, nb // 2, hl, 2 * wd), BF16),
                pltpu.VMEM((n, nb, hl, lat), BF16),
                pltpu.VMEM((n, nc, hl, 128), F32),
                pltpu.VMEM((6, nb, hl, lat), BF16),
                pltpu.VMEM((7, nc, hl, 128), F32),
                pltpu.VMEM((nb, hl, lat), F32),
                pltpu.VMEM((nb, hl, lat), F32),
                pltpu.VMEM((nc, hl, 128), F32),
                pltpu.VMEM((nb, hl, lat), BF16),
                pltpu.VMEM((2 * PAIRS, wd + ROPE, sl), BF16),
                dma,
                dma((2 * PAIRS, 2)),
                dma((nc,)),
                dma((7, nc)),
                dma((7, nc)),
                dma((7, nc)),
                dma((7, nc)),
                dma((7, nc)),
                dma((7, nc)),
            ],
            compiler_params=pltpu.CompilerParams(
                collective_id=0, has_side_effects=True, vmem_limit_bytes=63 * 1024 * 1024),
            name='mla_decode',
        )(lengths, q, jnp.swapaxes(cache, 1, 2))

    return jax.shard_map(local, mesh=mesh, in_specs=(P('dp', 'dcp', None), P('dp', 'dcp', None), P('dp')),
                         out_specs=P('dp', 'dcp', None), check_vma=False)
```

```python
import functools

import jax
import jax.numpy as jnp
from jax import lax
from jax.experimental import pallas as pl
from jax.experimental.pallas import tpu as pltpu
from jax.sharding import PartitionSpec as P

ROPE = 64
SCALE = 192 ** -0.5
CORES = 2
CHUNK = 8
PAIRS = 4
LAG_R = 2
LAG_F = 4

MESH = pl.DeviceIdType.MESH
F32 = jnp.float32
BF16 = jnp.bfloat16
VIA, DIRECT, MINE, PASS, SUM = 0, 2, 4, 5, 6


def weights(stats):
    top = functools.reduce(jnp.maximum, stats)
    top = jnp.maximum(top, jnp.finfo(F32).min)
    w = [jnp.exp(t - top) for t in stats]
    total = functools.reduce(jnp.add, w)
    inv = 1.0 / jnp.maximum(total, 1.0)
    return [x * inv for x in w], top + jnp.log(total)


def by_owner(stat, n, hl):
    t = stat.T[:n]
    block = lax.broadcasted_iota(jnp.int32, t.shape, 1) // hl
    row = lax.broadcasted_iota(jnp.int32, t.shape, 0)
    out = t
    for r in range(1, n):
        moved = pltpu.roll(pltpu.roll(t, r * hl, 1), n - r, 0)
        out = jnp.where((block - row + n) % n == r, moved, out)
    return out


def columns(row):
    return jnp.broadcast_to(row, (128, 128)).T


def scaled(w, i, o):
    hl, lat = o.shape
    return jnp.concatenate([w[i * hl:(i + 1) * hl]] * (lat // 128), axis=1) * o.astype(F32)


def kernel(n, len_ref, q_ref, ct_ref, o_ref, qraw, qg, od, st, inc, ins, lg, rs, rss, obuf, cbuf,
           raw_sem, cache_sem, out_sem, q_send, q_recv, o_send, o_recv, t_send, t_recv):
    chips = n // CORES
    nb, hl, wd = q_ref.shape
    lat = wd - ROPE
    heads = n * hl
    sl = ct_ref.shape[2]
    nc = nb // CHUNK
    half = CHUNK // 2
    npair = nb // 2

    me = lax.axis_index('dcp')
    x = me // CORES
    k = me % CORES
    partner = x * CORES + (1 - k)

    def dev(step, core):
        return ((x + step + chips) % chips) * CORES + core

    def cache_copies(pair, par):
        slot = (pair % PAIRS) * 2 + par
        b = pair * 2 + par
        if par == 0:
            return [pltpu.make_async_copy(ct_ref.at[b], cbuf.at[slot, pl.ds(0, wd)], cache_sem.at[slot, 0])]
        return [
            pltpu.make_async_copy(ct_ref.at[b, pl.ds(0, lat)], cbuf.at[slot, pl.ds(0, lat)], cache_sem.at[slot, 0]),
            pltpu.make_async_copy(ct_ref.at[b, pl.ds(lat, ROPE)], cbuf.at[slot, pl.ds(wd, ROPE)], cache_sem.at[slot, 1]),
        ]

    def fetch(pair):
        for par in range(2):
            for cp in cache_copies(pair, par):
                cp.start()

    raw = pltpu.make_async_copy(q_ref, qraw, raw_sem)
    raw.start()

    barrier = pltpu.get_barrier_semaphore()
    peers = [partner, dev(1, 0), dev(1, 1), dev(-1, 0), dev(-1, 1)]
    for peer in peers:
        pl.semaphore_signal(barrier, inc=1, device_id={'dcp': peer}, device_id_type=MESH)

    for g in range(PAIRS):
        cbuf[2 * g, pl.ds(wd, ROPE), :] = jnp.zeros((ROPE, sl), BF16)
        cbuf[2 * g + 1, pl.ds(lat, ROPE), :] = jnp.zeros((ROPE, sl), BF16)
    raw.wait()

    def pack(g, _):
        for par in range(2):
            qg[me, g, :, pl.ds(par * lat, lat)] = qraw[2 * g + par, :, pl.ds(0, lat)]
        r0 = qraw[2 * g, :, pl.ds(lat, ROPE)]
        r1 = qraw[2 * g + 1, :, pl.ds(lat, ROPE)]
        qg[me, g, :, pl.ds(2 * lat, 2 * ROPE)] = jnp.concatenate([r0, r1], axis=1)
        return 0

    lax.fori_loop(0, npair, pack, 0)
    for g in range(PAIRS):
        fetch(g)
    pl.semaphore_wait(barrier, len(peers))

    def q_copy(kind, src, c, to):
        part = qg.at[src, pl.ds(c * half, half)]
        return pltpu.make_async_remote_copy(
            src_ref=part, dst_ref=part, send_sem=q_send.at[kind, c], recv_sem=q_recv.at[kind, c],
            device_id={'dcp': to}, device_id_type=MESH)

    def q_wait(kind, src, c):
        q_copy(kind, src, c, me).wait_recv()

    def sign(c):
        return 1 - 2 * (c % 2)

    def q0(c, _):
        q_copy(0, me, c, dev(1, k)).start()
        q_copy(1, me, c, dev(-1, k)).start()
        q_copy(2, me, c, partner).start()
        return 0

    lax.fori_loop(0, nc, q0, 0)

    def q1(c, _):
        way = -sign(c)
        q_wait(0, dev(-1, k), c)
        q_copy(3, dev(-1, k), c, partner).start()
        q_wait(1, dev(1, k), c)
        q_copy(4, dev(1, k), c, partner).start()
        q_copy(5, dev(-way, k), c, dev(way, k)).start()
        return 0

    lax.fori_loop(0, nc, q1, 0)

    def q2(c):
        q_wait(5, dev(2, k), c)
        q_copy(6, dev(2, k), c, partner).start()

    def q3(c):
        q_wait(2, partner, c)
        q_wait(3, dev(-1, 1 - k), c)
        q_wait(4, dev(1, 1 - k), c)
        q_wait(6, dev(2, 1 - k), c)

    lane = lax.broadcasted_iota(jnp.int32, (heads, 128), 1)
    where_t = lax.broadcasted_iota(jnp.int32, (1, sl), 1)
    base = me * sl

    def attend(c):
        def pair_step(i, stat):
            g = c * half + i
            for par in range(2):
                b = g * 2 + par
                slot = (g % PAIRS) * 2 + par
                for cp in cache_copies(g, par):
                    cp.wait()
                qa = qg[:, g, :, pl.ds(par * lat, lat)].reshape(heads, lat)
                qr = qg[:, g, :, pl.ds(2 * lat, 2 * ROPE)].reshape(heads, 2 * ROPE)
                s = jnp.dot(qa, cbuf[slot, pl.ds(0, lat), :], preferred_element_type=F32)
                s = s + jnp.dot(qr, cbuf[slot, pl.ds(lat, 2 * ROPE), :], preferred_element_type=F32)
                s = jnp.where(where_t < len_ref[b] - base, s * SCALE, -jnp.inf)
                m = jnp.maximum(jnp.max(s, axis=1, keepdims=True), jnp.finfo(F32).min)
                p = jnp.exp(s - m)
                l = jnp.sum(p, axis=1, keepdims=True)
                pv = lax.dot_general(p.astype(BF16), cbuf[slot, pl.ds(0, lat), :], (((1,), (1,)), ((), ())),
                                     preferred_element_type=F32)
                o = (pv * (1.0 / jnp.maximum(l, 1.0))).astype(BF16)
                od[:, b, :, :] = o.reshape(n, hl, lat)
                stat = jnp.where(lane == i * 2 + par, m + jnp.log(l), stat)

            @pl.when(g + PAIRS < npair)
            def _():
                fetch(g + PAIRS)

            return stat

        stat = lax.fori_loop(0, half, pair_step, jnp.full((heads, 128), -jnp.inf, F32))
        lse = by_owner(stat, n, hl)
        for j in range(n):
            st[j, c] = lse[j:j + 1]

    def rows(c):
        return pl.ds(c * CHUNK, CHUNK)

    def o_copies(c, head, slot_s, slot_r, to):
        return [
            pltpu.make_async_remote_copy(
                src_ref=od.at[head, rows(c)], dst_ref=inc.at[slot_r, rows(c)],
                send_sem=o_send.at[slot_s, c], recv_sem=o_recv.at[slot_r, c],
                device_id={'dcp': to}, device_id_type=MESH),
            pltpu.make_async_remote_copy(
                src_ref=st.at[head, c], dst_ref=ins.at[slot_r, c],
                send_sem=t_send.at[slot_s, c], recv_sem=t_recv.at[slot_r, c],
                device_id={'dcp': to}, device_id_type=MESH),
        ]

    def sends(c):
        way = sign(c)
        out = []
        for kk in range(CORES):
            out += o_copies(c, dev(2, kk), VIA + kk, VIA + k, dev(way, kk))
        out += o_copies(c, dev(way, 1 - k), PASS, PASS, partner)
        out += o_copies(c, partner, MINE, MINE, partner)
        for kk in range(CORES):
            out += o_copies(c, dev(-way, kk), DIRECT + kk, DIRECT + k, dev(-way, kk))
        return out

    def sum_copies(c):
        to = dev(sign(c), k)
        return [
            pltpu.make_async_remote_copy(
                src_ref=rs.at[rows(c)], dst_ref=lg.at[rows(c)], send_sem=o_send.at[SUM, c], recv_sem=o_recv.at[SUM, c],
                device_id={'dcp': to}, device_id_type=MESH),
            pltpu.make_async_remote_copy(
                src_ref=rss.at[c], dst_ref=ins.at[SUM, c], send_sem=t_send.at[SUM, c], recv_sem=t_recv.at[SUM, c],
                device_id={'dcp': to}, device_id_type=MESH),
        ]

    def o_wait(c, slot):
        for cp in o_copies(c, me, slot, slot, me):
            cp.wait_recv()

    def relay(c):
        for slot in (PASS, VIA, VIA + 1):
            o_wait(c, slot)
        mine = dev(sign(c), k)
        w, lse = weights([st[mine, c], ins[PASS, c], ins[VIA, c], ins[VIA + 1, c]])
        w = [columns(r) for r in w]
        for i in range(CHUNK):
            b = c * CHUNK + i
            acc = scaled(w[0], i, od[mine, b])
            for j, slot in ((1, PASS), (2, VIA), (3, VIA + 1)):
                acc = acc + scaled(w[j], i, inc[slot, b])
            rs[b] = acc
        rss[c] = lse
        for cp in sum_copies(c):
            cp.start()

    def out_copy(c):
        return pltpu.make_async_copy(obuf.at[rows(c)], o_ref.at[rows(c)], out_sem.at[c])

    def merge(c):
        for slot in (MINE, DIRECT, DIRECT + 1):
            o_wait(c, slot)
        for cp in sum_copies(c):
            cp.wait_recv()
        w, _ = weights([st[me, c], ins[MINE, c], ins[DIRECT, c], ins[DIRECT + 1, c], ins[SUM, c]])
        w = [columns(r) for r in w]
        for i in range(CHUNK):
            b = c * CHUNK + i
            acc = scaled(w[0], i, od[me, b])
            for j, slot in ((1, MINE), (2, DIRECT), (3, DIRECT + 1)):
                acc = acc + scaled(w[j], i, inc[slot, b])
            acc = acc + scaled(w[4], i, lg[b])
            obuf[b] = acc.astype(BF16)
        out_copy(c).start()

    q2(0)

    def step(t, _):
        @pl.when(t < nc)
        def _():
            @pl.when(t + 1 < nc)
            def _():
                q2(t + 1)

            q3(t)
            attend(t)
            for cp in sends(t):
                cp.start()

        @pl.when(jnp.logical_and(t >= LAG_R, t < nc + LAG_R))
        def _():
            relay(t - LAG_R)

        @pl.when(t >= LAG_F)
        def _():
            merge(t - LAG_F)

        return 0

    lax.fori_loop(0, nc + LAG_F, step, 0)

    def drain(c, _):
        for kind in range(7):
            q_copy(kind, me, c, me).wait_send()
        for cp in sends(c) + sum_copies(c):
            cp.wait_send()
        out_copy(c).wait()
        return 0

    lax.fori_loop(0, nc, drain, 0)


def solution(mesh):
    n = mesh.shape['dcp']

    def local(q, cache, lengths):
        nb, hl, wd = q.shape
        sl = cache.shape[1]
        lat = wd - ROPE
        nc = nb // CHUNK
        anyspace = pl.BlockSpec(memory_space=pl.ANY)
        dma = pltpu.SemaphoreType.DMA
        return pl.pallas_call(
            functools.partial(kernel, n),
            out_shape=jax.ShapeDtypeStruct((nb, hl, lat), BF16),
            in_specs=[pl.BlockSpec(memory_space=pltpu.SMEM), anyspace, anyspace],
            out_specs=anyspace,
            scratch_shapes=[
                pltpu.VMEM((nb, hl, wd), BF16),
                pltpu.VMEM((n, nb // 2, hl, 2 * wd), BF16),
                pltpu.VMEM((n, nb, hl, lat), BF16),
                pltpu.VMEM((n, nc, 1, 128), F32),
                pltpu.VMEM((6, nb, hl, lat), BF16),
                pltpu.VMEM((7, nc, 1, 128), F32),
                pltpu.VMEM((nb, hl, lat), F32),
                pltpu.VMEM((nb, hl, lat), F32),
                pltpu.VMEM((nc, 1, 128), F32),
                pltpu.VMEM((nb, hl, lat), BF16),
                pltpu.VMEM((2 * PAIRS, wd + ROPE, sl), BF16),
                dma,
                dma((2 * PAIRS, 2)),
                dma((nc,)),
                dma((7, nc)),
                dma((7, nc)),
                dma((7, nc)),
                dma((7, nc)),
                dma((7, nc)),
                dma((7, nc)),
            ],
            compiler_params=pltpu.CompilerParams(
                collective_id=0, has_side_effects=True, vmem_limit_bytes=63 * 1024 * 1024),
            name='mla_decode',
        )(lengths, q, jnp.swapaxes(cache, 1, 2))

    return jax.shard_map(local, mesh=mesh, in_specs=(P('dp', 'dcp', None), P('dp', 'dcp', None), P('dp')),
                         out_specs=P('dp', 'dcp', None), check_vma=False)
```

```python
import functools

import jax
import jax.numpy as jnp
from jax import lax
from jax.experimental import pallas as pl
from jax.experimental.pallas import tpu as pltpu
from jax.sharding import PartitionSpec as P

ROPE = 64
SCALE = 192 ** -0.5
CORES = 2
CHUNK = 8
PAIRS = 4
AHEAD = 4
LEAD = 3
LAG_R = 2
LAG_F = 4

MESH = pl.DeviceIdType.MESH
F32 = jnp.float32
BF16 = jnp.bfloat16
VIA, DIRECT, MINE, PASS, SUM = 0, 2, 4, 5, 6


def weights(stats):
    top = functools.reduce(jnp.maximum, stats)
    top = jnp.maximum(top, jnp.finfo(F32).min)
    w = [jnp.exp(t - top) for t in stats]
    total = functools.reduce(jnp.add, w)
    inv = 1.0 / jnp.maximum(total, 1.0)
    return [x * inv for x in w], top + jnp.log(total)


def by_owner(stat, n, hl):
    t = stat.T[:n]
    block = lax.broadcasted_iota(jnp.int32, t.shape, 1) // hl
    row = lax.broadcasted_iota(jnp.int32, t.shape, 0)
    out = t
    for r in range(1, n):
        moved = pltpu.roll(pltpu.roll(t, r * hl, 1), n - r, 0)
        out = jnp.where((block - row + n) % n == r, moved, out)
    return out


def columns(row):
    return jnp.broadcast_to(row, (128, 128)).T


def scaled(w, i, o):
    hl, lat = o.shape
    return jnp.concatenate([w[i * hl:(i + 1) * hl]] * (lat // 128), axis=1) * o.astype(F32)


def kernel(n, len_ref, q_ref, ct_ref, o_ref, qraw, qg, od, st, inc, ins, lg, rs, rss, obuf, cbuf,
           raw_sem, cache_sem, out_sem, q_send, q_recv, o_send, o_recv, t_send, t_recv):
    chips = n // CORES
    nb, hl, wd = q_ref.shape
    lat = wd - ROPE
    heads = n * hl
    sl = ct_ref.shape[2]
    nc = nb // CHUNK
    half = CHUNK // 2
    npair = nb // 2

    me = lax.axis_index('dcp')
    x = me // CORES
    k = me % CORES
    partner = x * CORES + (1 - k)

    def dev(step, core):
        return ((x + step + chips) % chips) * CORES + core

    def cache_copies(pair, par):
        slot = (pair % PAIRS) * 2 + par
        b = pair * 2 + par
        if par == 0:
            return [pltpu.make_async_copy(ct_ref.at[b], cbuf.at[slot, pl.ds(0, wd)], cache_sem.at[slot, 0])]
        return [
            pltpu.make_async_copy(ct_ref.at[b, pl.ds(0, lat)], cbuf.at[slot, pl.ds(0, lat)], cache_sem.at[slot, 0]),
            pltpu.make_async_copy(ct_ref.at[b, pl.ds(lat, ROPE)], cbuf.at[slot, pl.ds(wd, ROPE)], cache_sem.at[slot, 1]),
        ]

    def fetch(pair):
        for par in range(2):
            for cp in cache_copies(pair, par):
                cp.start()

    raw = pltpu.make_async_copy(q_ref, qraw, raw_sem)
    raw.start()

    barrier = pltpu.get_barrier_semaphore()
    peers = [partner, dev(1, 0), dev(1, 1), dev(-1, 0), dev(-1, 1)]
    for peer in peers:
        pl.semaphore_signal(barrier, inc=1, device_id={'dcp': peer}, device_id_type=MESH)

    for g in range(PAIRS):
        cbuf[2 * g, pl.ds(wd, ROPE), :] = jnp.zeros((ROPE, sl), BF16)
        cbuf[2 * g + 1, pl.ds(lat, ROPE), :] = jnp.zeros((ROPE, sl), BF16)
    raw.wait()

    def pack(g, _):
        for par in range(2):
            qg[me, g, :, pl.ds(par * lat, lat)] = qraw[2 * g + par, :, pl.ds(0, lat)]
        r0 = qraw[2 * g, :, pl.ds(lat, ROPE)]
        r1 = qraw[2 * g + 1, :, pl.ds(lat, ROPE)]
        qg[me, g, :, pl.ds(2 * lat, 2 * ROPE)] = jnp.concatenate([r0, r1], axis=1)
        return 0

    lax.fori_loop(0, npair, pack, 0)
    for g in range(PAIRS):
        fetch(g)
    pl.semaphore_wait(barrier, len(peers))

    def q_copy(kind, src, c, to):
        part = qg.at[src, pl.ds(c * half, half)]
        return pltpu.make_async_remote_copy(
            src_ref=part, dst_ref=part, send_sem=q_send.at[kind, c], recv_sem=q_recv.at[kind, c],
            device_id={'dcp': to}, device_id_type=MESH)

    def q_wait(kind, src, c):
        q_copy(kind, src, c, me).wait_recv()

    def sign(c):
        return 1 - 2 * (c % 2)

    def q0(c, _):
        q_copy(0, me, c, dev(1, k)).start()
        q_copy(1, me, c, dev(-1, k)).start()
        q_copy(2, me, c, partner).start()
        return 0

    lax.fori_loop(0, AHEAD, q0, 0)

    def q1(c, _):
        way = -sign(c)
        q_wait(0, dev(-1, k), c)
        q_copy(3, dev(-1, k), c, partner).start()
        q_wait(1, dev(1, k), c)
        q_copy(4, dev(1, k), c, partner).start()
        q_copy(5, dev(-way, k), c, dev(way, k)).start()

        @pl.when(c + AHEAD < nc)
        def _():
            q0(c + AHEAD, 0)

        return 0

    lax.fori_loop(0, LEAD, q1, 0)

    def q2(c):
        q_wait(5, dev(2, k), c)
        q_copy(6, dev(2, k), c, partner).start()

    def q3(c):
        q_wait(2, partner, c)
        q_wait(3, dev(-1, 1 - k), c)
        q_wait(4, dev(1, 1 - k), c)
        q_wait(6, dev(2, 1 - k), c)

    lane = lax.broadcasted_iota(jnp.int32, (heads, 128), 1)
    where_t = lax.broadcasted_iota(jnp.int32, (1, sl), 1)
    base = me * sl

    def attend(c):
        def pair_step(i, stat):
            g = c * half + i
            for par in range(2):
                b = g * 2 + par
                slot = (g % PAIRS) * 2 + par
                for cp in cache_copies(g, par):
                    cp.wait()
                qa = qg[:, g, :, pl.ds(par * lat, lat)].reshape(heads, lat)
                qr = qg[:, g, :, pl.ds(2 * lat, 2 * ROPE)].reshape(heads, 2 * ROPE)
                s = jnp.dot(qa, cbuf[slot, pl.ds(0, lat), :], preferred_element_type=F32)
                s = s + jnp.dot(qr, cbuf[slot, pl.ds(lat, 2 * ROPE), :], preferred_element_type=F32)
                s = jnp.where(where_t < len_ref[b] - base, s * SCALE, -jnp.inf)
                m = jnp.maximum(jnp.max(s, axis=1, keepdims=True), jnp.finfo(F32).min)
                p = jnp.exp(s - m)
                l = jnp.sum(p, axis=1, keepdims=True)
                pv = lax.dot_general(p.astype(BF16), cbuf[slot, pl.ds(0, lat), :], (((1,), (1,)), ((), ())),
                                     preferred_element_type=F32)
                o = (pv * (1.0 / jnp.maximum(l, 1.0))).astype(BF16)
                od[:, b, :, :] = o.reshape(n, hl, lat)
                stat = jnp.where(lane == i * 2 + par, m + jnp.log(l), stat)

            @pl.when(g + PAIRS < npair)
            def _():
                fetch(g + PAIRS)

            return stat

        stat = lax.fori_loop(0, half, pair_step, jnp.full((heads, 128), -jnp.inf, F32))
        lse = by_owner(stat, n, hl)
        for j in range(n):
            st[j, c] = lse[j:j + 1]

    def rows(c):
        return pl.ds(c * CHUNK, CHUNK)

    def o_copies(c, head, slot_s, slot_r, to):
        return [
            pltpu.make_async_remote_copy(
                src_ref=od.at[head, rows(c)], dst_ref=inc.at[slot_r, rows(c)],
                send_sem=o_send.at[slot_s, c], recv_sem=o_recv.at[slot_r, c],
                device_id={'dcp': to}, device_id_type=MESH),
            pltpu.make_async_remote_copy(
                src_ref=st.at[head, c], dst_ref=ins.at[slot_r, c],
                send_sem=t_send.at[slot_s, c], recv_sem=t_recv.at[slot_r, c],
                device_id={'dcp': to}, device_id_type=MESH),
        ]

    def sends(c):
        way = sign(c)
        out = []
        for kk in range(CORES):
            out += o_copies(c, dev(2, kk), VIA + kk, VIA + k, dev(way, kk))
        out += o_copies(c, dev(way, 1 - k), PASS, PASS, partner)
        out += o_copies(c, partner, MINE, MINE, partner)
        for kk in range(CORES):
            out += o_copies(c, dev(-way, kk), DIRECT + kk, DIRECT + k, dev(-way, kk))
        return out

    def sum_copies(c):
        to = dev(sign(c), k)
        return [
            pltpu.make_async_remote_copy(
                src_ref=rs.at[rows(c)], dst_ref=lg.at[rows(c)], send_sem=o_send.at[SUM, c], recv_sem=o_recv.at[SUM, c],
                device_id={'dcp': to}, device_id_type=MESH),
            pltpu.make_async_remote_copy(
                src_ref=rss.at[c], dst_ref=ins.at[SUM, c], send_sem=t_send.at[SUM, c], recv_sem=t_recv.at[SUM, c],
                device_id={'dcp': to}, device_id_type=MESH),
        ]

    def o_wait(c, slot):
        for cp in o_copies(c, me, slot, slot, me):
            cp.wait_recv()

    def relay(c):
        for slot in (PASS, VIA, VIA + 1):
            o_wait(c, slot)
        mine = dev(sign(c), k)
        w, lse = weights([st[mine, c], ins[PASS, c], ins[VIA, c], ins[VIA + 1, c]])
        w = [columns(r) for r in w]
        for i in range(CHUNK):
            b = c * CHUNK + i
            acc = scaled(w[0], i, od[mine, b])
            for j, slot in ((1, PASS), (2, VIA), (3, VIA + 1)):
                acc = acc + scaled(w[j], i, inc[slot, b])
            rs[b] = acc
        rss[c] = lse
        for cp in sum_copies(c):
            cp.start()

    def out_copy(c):
        return pltpu.make_async_copy(obuf.at[rows(c)], o_ref.at[rows(c)], out_sem.at[c])

    def merge(c):
        for slot in (MINE, DIRECT, DIRECT + 1):
            o_wait(c, slot)
        for cp in sum_copies(c):
            cp.wait_recv()
        w, _ = weights([st[me, c], ins[MINE, c], ins[DIRECT, c], ins[DIRECT + 1, c], ins[SUM, c]])
        w = [columns(r) for r in w]
        for i in range(CHUNK):
            b = c * CHUNK + i
            acc = scaled(w[0], i, od[me, b])
            for j, slot in ((1, MINE), (2, DIRECT), (3, DIRECT + 1)):
                acc = acc + scaled(w[j], i, inc[slot, b])
            acc = acc + scaled(w[4], i, lg[b])
            obuf[b] = acc.astype(BF16)
        out_copy(c).start()

    def step(t, _):
        @pl.when(t + LEAD < nc)
        def _():
            q1(t + LEAD, 0)

        @pl.when(t < nc)
        def _():
            @pl.when(t == 0)
            def _():
                q2(0)

            @pl.when(t + 1 < nc)
            def _():
                q2(t + 1)

            q3(t)
            attend(t)
            for cp in sends(t):
                cp.start()

        @pl.when(jnp.logical_and(t >= LAG_R, t < nc + LAG_R))
        def _():
            relay(t - LAG_R)

        @pl.when(t >= LAG_F)
        def _():
            merge(t - LAG_F)

        return 0

    lax.fori_loop(0, nc + LAG_F, step, 0)

    def drain(c, _):
        for kind in range(7):
            q_copy(kind, me, c, me).wait_send()
        for cp in sends(c) + sum_copies(c):
            cp.wait_send()
        out_copy(c).wait()
        return 0

    lax.fori_loop(0, nc, drain, 0)


def solution(mesh):
    n = mesh.shape['dcp']

    def local(q, cache, lengths):
        nb, hl, wd = q.shape
        sl = cache.shape[1]
        lat = wd - ROPE
        nc = nb // CHUNK
        anyspace = pl.BlockSpec(memory_space=pl.ANY)
        dma = pltpu.SemaphoreType.DMA
        return pl.pallas_call(
            functools.partial(kernel, n),
            out_shape=jax.ShapeDtypeStruct((nb, hl, lat), BF16),
            in_specs=[pl.BlockSpec(memory_space=pltpu.SMEM), anyspace, anyspace],
            out_specs=anyspace,
            scratch_shapes=[
                pltpu.VMEM((nb, hl, wd), BF16),
                pltpu.VMEM((n, nb // 2, hl, 2 * wd), BF16),
                pltpu.VMEM((n, nb, hl, lat), BF16),
                pltpu.VMEM((n, nc, 1, 128), F32),
                pltpu.VMEM((6, nb, hl, lat), BF16),
                pltpu.VMEM((7, nc, 1, 128), F32),
                pltpu.VMEM((nb, hl, lat), F32),
                pltpu.VMEM((nb, hl, lat), F32),
                pltpu.VMEM((nc, 1, 128), F32),
                pltpu.VMEM((nb, hl, lat), BF16),
                pltpu.VMEM((2 * PAIRS, wd + ROPE, sl), BF16),
                dma,
                dma((2 * PAIRS, 2)),
                dma((nc,)),
                dma((7, nc)),
                dma((7, nc)),
                dma((7, nc)),
                dma((7, nc)),
                dma((7, nc)),
                dma((7, nc)),
            ],
            compiler_params=pltpu.CompilerParams(
                collective_id=0, has_side_effects=True, vmem_limit_bytes=63 * 1024 * 1024),
            name='mla_decode',
        )(lengths, q, jnp.swapaxes(cache, 1, 2))

    return jax.shard_map(local, mesh=mesh, in_specs=(P('dp', 'dcp', None), P('dp', 'dcp', None), P('dp')),
                         out_specs=P('dp', 'dcp', None), check_vma=False)
```

```python
import functools

import jax
import jax.numpy as jnp
from jax import lax
from jax.experimental import pallas as pl
from jax.experimental.pallas import tpu as pltpu
from jax.sharding import PartitionSpec as P

ROPE = 64
SCALE = 192 ** -0.5
CORES = 2
CHUNK = 8
PAIRS = 4
AHEAD = 4
LEAD = 3
LAG_R = 2
LAG_F = 4

MESH = pl.DeviceIdType.MESH
F32 = jnp.float32
BF16 = jnp.bfloat16
VIA, DIRECT, MINE, PASS, SUM = 0, 2, 4, 5, 6


def weights(stats):
    top = functools.reduce(jnp.maximum, stats)
    top = jnp.maximum(top, jnp.finfo(F32).min)
    w = [jnp.exp(t - top) for t in stats]
    total = functools.reduce(jnp.add, w)
    inv = 1.0 / jnp.maximum(total, 1.0)
    return [x * inv for x in w], top + jnp.log(total)


def by_owner(stat, n, hl):
    t = stat.T[:n]
    block = lax.broadcasted_iota(jnp.int32, t.shape, 1) // hl
    row = lax.broadcasted_iota(jnp.int32, t.shape, 0)
    out = t
    for r in range(1, n):
        moved = pltpu.roll(pltpu.roll(t, r * hl, 1), n - r, 0)
        out = jnp.where((block - row + n) % n == r, moved, out)
    return out


def columns(row):
    return jnp.broadcast_to(row, (128, 128)).T


def scaled(w, i, o):
    hl, lat = o.shape
    return jnp.concatenate([w[i * hl:(i + 1) * hl]] * (lat // 128), axis=1) * o.astype(F32)


def kernel(n, len_ref, q_ref, ct_ref, o_ref, qraw, qg, od, st, inc, ins, lg, rs, rss, cbuf,
           raw_sem, cache_sem, q_send, q_recv, o_send, o_recv, t_send, t_recv):
    chips = n // CORES
    nb, hl, wd = q_ref.shape
    lat = wd - ROPE
    heads = n * hl
    sl = ct_ref.shape[2]
    nc = nb // CHUNK
    half = CHUNK // 2
    npair = nb // 2

    me = lax.axis_index('dcp')
    x = me // CORES
    k = me % CORES
    partner = x * CORES + (1 - k)

    def dev(step, core):
        return ((x + step + chips) % chips) * CORES + core

    def cache_copies(pair, par):
        slot = (pair % PAIRS) * 2 + par
        b = pair * 2 + par
        if par == 0:
            return [pltpu.make_async_copy(ct_ref.at[b], cbuf.at[slot, pl.ds(0, wd)], cache_sem.at[slot, 0])]
        return [
            pltpu.make_async_copy(ct_ref.at[b, pl.ds(0, lat)], cbuf.at[slot, pl.ds(0, lat)], cache_sem.at[slot, 0]),
            pltpu.make_async_copy(ct_ref.at[b, pl.ds(lat, ROPE)], cbuf.at[slot, pl.ds(wd, ROPE)], cache_sem.at[slot, 1]),
        ]

    def fetch(pair):
        for par in range(2):
            for cp in cache_copies(pair, par):
                cp.start()

    raw = pltpu.make_async_copy(q_ref, qraw, raw_sem)
    raw.start()

    barrier = pltpu.get_barrier_semaphore()
    peers = [partner, dev(1, 0), dev(1, 1), dev(-1, 0), dev(-1, 1)]
    for peer in peers:
        pl.semaphore_signal(barrier, inc=1, device_id={'dcp': peer}, device_id_type=MESH)

    raw.wait()

    def pack(g, _):
        for par in range(2):
            qg[me, g, :, pl.ds(par * lat, lat)] = qraw[2 * g + par, :, pl.ds(0, lat)]
        r0 = qraw[2 * g, :, pl.ds(lat, ROPE)]
        r1 = qraw[2 * g + 1, :, pl.ds(lat, ROPE)]
        qg[me, g, :, pl.ds(2 * lat, 2 * ROPE)] = jnp.concatenate([r0, r1], axis=1)
        return 0

    lax.fori_loop(0, half, pack, 0)
    pl.semaphore_wait(barrier, len(peers))

    def q_copy(kind, src, c, to):
        part = qg.at[src, pl.ds(c * half, half)]
        return pltpu.make_async_remote_copy(
            src_ref=part, dst_ref=part, send_sem=q_send.at[kind, c], recv_sem=q_recv.at[kind, c],
            device_id={'dcp': to}, device_id_type=MESH)

    def q_wait(kind, src, c):
        q_copy(kind, src, c, me).wait_recv()

    def sign(c):
        return 1 - 2 * (c % 2)

    def q0(c, _):
        @pl.when(c + 1 < nc)
        def _():
            lax.fori_loop((c + 1) * half, (c + 2) * half, pack, 0)

        q_copy(0, me, c, dev(1, k)).start()
        q_copy(1, me, c, dev(-1, k)).start()
        q_copy(2, me, c, partner).start()
        return 0

    lax.fori_loop(0, AHEAD, q0, 0)

    for g in range(PAIRS):
        fetch(g)
        cbuf[2 * g, pl.ds(wd, ROPE), :] = jnp.zeros((ROPE, sl), BF16)
        cbuf[2 * g + 1, pl.ds(lat, ROPE), :] = jnp.zeros((ROPE, sl), BF16)

    def q1(c, _):
        way = -sign(c)
        q_wait(0, dev(-1, k), c)
        q_copy(3, dev(-1, k), c, partner).start()
        q_wait(1, dev(1, k), c)
        q_copy(4, dev(1, k), c, partner).start()
        q_copy(5, dev(-way, k), c, dev(way, k)).start()

        @pl.when(c + AHEAD < nc)
        def _():
            q0(c + AHEAD, 0)

        return 0

    lax.fori_loop(0, LEAD, q1, 0)

    def q2(c):
        q_wait(5, dev(2, k), c)
        q_copy(6, dev(2, k), c, partner).start()

    def q3(c):
        q_wait(2, partner, c)
        q_wait(3, dev(-1, 1 - k), c)
        q_wait(4, dev(1, 1 - k), c)
        q_wait(6, dev(2, 1 - k), c)

    lane = lax.broadcasted_iota(jnp.int32, (heads, 128), 1)
    where_t = lax.broadcasted_iota(jnp.int32, (1, sl), 1)
    base = me * sl

    def attend(c):
        def pair_step(i, stat):
            g = c * half + i
            for par in range(2):
                b = g * 2 + par
                slot = (g % PAIRS) * 2 + par
                for cp in cache_copies(g, par):
                    cp.wait()
                qa = qg[:, g, :, pl.ds(par * lat, lat)].reshape(heads, lat)
                qr = qg[:, g, :, pl.ds(2 * lat, 2 * ROPE)].reshape(heads, 2 * ROPE)
                s = jnp.dot(qa, cbuf[slot, pl.ds(0, lat), :], preferred_element_type=F32)
                s = s + jnp.dot(qr, cbuf[slot, pl.ds(lat, 2 * ROPE), :], preferred_element_type=F32)
                s = jnp.where(where_t < len_ref[b] - base, s * SCALE, -jnp.inf)
                m = jnp.maximum(jnp.max(s, axis=1, keepdims=True), jnp.finfo(F32).min)
                p = jnp.exp(s - m)
                l = jnp.sum(p, axis=1, keepdims=True)
                pv = lax.dot_general(p.astype(BF16), cbuf[slot, pl.ds(0, lat), :], (((1,), (1,)), ((), ())),
                                     preferred_element_type=F32)
                o = (pv * (1.0 / jnp.maximum(l, 1.0))).astype(BF16)
                od[:, b, :, :] = o.reshape(n, hl, lat)
                stat = jnp.where(lane == i * 2 + par, m + jnp.log(l), stat)

            @pl.when(g + PAIRS < npair)
            def _():
                fetch(g + PAIRS)

            return stat

        stat = lax.fori_loop(0, half, pair_step, jnp.full((heads, 128), -jnp.inf, F32))
        lse = by_owner(stat, n, hl)
        for j in range(n):
            st[j, c] = lse[j:j + 1]

    def rows(c):
        return pl.ds(c * CHUNK, CHUNK)

    def o_copies(c, head, slot_s, slot_r, to):
        return [
            pltpu.make_async_remote_copy(
                src_ref=od.at[head, rows(c)], dst_ref=inc.at[slot_r, rows(c)],
                send_sem=o_send.at[slot_s, c], recv_sem=o_recv.at[slot_r, c],
                device_id={'dcp': to}, device_id_type=MESH),
            pltpu.make_async_remote_copy(
                src_ref=st.at[head, c], dst_ref=ins.at[slot_r, c],
                send_sem=t_send.at[slot_s, c], recv_sem=t_recv.at[slot_r, c],
                device_id={'dcp': to}, device_id_type=MESH),
        ]

    def sends(c):
        way = sign(c)
        out = []
        for kk in range(CORES):
            out += o_copies(c, dev(2, kk), VIA + kk, VIA + k, dev(way, kk))
        out += o_copies(c, dev(way, 1 - k), PASS, PASS, partner)
        out += o_copies(c, partner, MINE, MINE, partner)
        for kk in range(CORES):
            out += o_copies(c, dev(-way, kk), DIRECT + kk, DIRECT + k, dev(-way, kk))
        return out

    def sum_copies(c):
        to = dev(sign(c), k)
        return [
            pltpu.make_async_remote_copy(
                src_ref=rs.at[rows(c)], dst_ref=lg.at[rows(c)], send_sem=o_send.at[SUM, c], recv_sem=o_recv.at[SUM, c],
                device_id={'dcp': to}, device_id_type=MESH),
            pltpu.make_async_remote_copy(
                src_ref=rss.at[c], dst_ref=ins.at[SUM, c], send_sem=t_send.at[SUM, c], recv_sem=t_recv.at[SUM, c],
                device_id={'dcp': to}, device_id_type=MESH),
        ]

    def o_wait(c, slot):
        for cp in o_copies(c, me, slot, slot, me):
            cp.wait_recv()

    def relay(c):
        for slot in (PASS, VIA, VIA + 1):
            o_wait(c, slot)
        mine = dev(sign(c), k)
        w, lse = weights([st[mine, c], ins[PASS, c], ins[VIA, c], ins[VIA + 1, c]])
        w = [columns(r) for r in w]
        for i in range(CHUNK):
            b = c * CHUNK + i
            acc = scaled(w[0], i, od[mine, b])
            for j, slot in ((1, PASS), (2, VIA), (3, VIA + 1)):
                acc = acc + scaled(w[j], i, inc[slot, b])
            rs[b] = acc
        rss[c] = lse
        for cp in sum_copies(c):
            cp.start()

    def merge(c):
        for slot in (MINE, DIRECT, DIRECT + 1):
            o_wait(c, slot)
        for cp in sum_copies(c):
            cp.wait_recv()
        w, _ = weights([st[me, c], ins[MINE, c], ins[DIRECT, c], ins[DIRECT + 1, c], ins[SUM, c]])
        w = [columns(r) for r in w]
        for i in range(CHUNK):
            b = c * CHUNK + i
            acc = scaled(w[0], i, od[me, b])
            for j, slot in ((1, MINE), (2, DIRECT), (3, DIRECT + 1)):
                acc = acc + scaled(w[j], i, inc[slot, b])
            acc = acc + scaled(w[4], i, lg[b])
            o_ref[b] = acc.astype(BF16)

    def step(t, _):
        @pl.when(t + LEAD < nc)
        def _():
            q1(t + LEAD, 0)

        @pl.when(t < nc)
        def _():
            @pl.when(t == 0)
            def _():
                q2(0)

            @pl.when(t + 1 < nc)
            def _():
                q2(t + 1)

            q3(t)
            attend(t)
            for cp in sends(t):
                cp.start()

        @pl.when(jnp.logical_and(t >= LAG_R, t < nc + LAG_R))
        def _():
            relay(t - LAG_R)

        @pl.when(t >= LAG_F)
        def _():
            merge(t - LAG_F)

        return 0

    lax.fori_loop(0, nc + LAG_F, step, 0)

    def drain(c, _):
        for kind in range(7):
            q_copy(kind, me, c, me).wait_send()
        for cp in sends(c) + sum_copies(c):
            cp.wait_send()
        return 0

    lax.fori_loop(0, nc, drain, 0)


def solution(mesh):
    n = mesh.shape['dcp']

    def local(q, cache, lengths):
        nb, hl, wd = q.shape
        sl = cache.shape[1]
        lat = wd - ROPE
        nc = nb // CHUNK
        anyspace = pl.BlockSpec(memory_space=pl.ANY)
        dma = pltpu.SemaphoreType.DMA
        return pl.pallas_call(
            functools.partial(kernel, n),
            out_shape=pltpu.VMEM((nb, hl, lat), BF16),
            in_specs=[pl.BlockSpec(memory_space=pltpu.SMEM), anyspace, anyspace],
            out_specs=pl.BlockSpec(memory_space=pltpu.VMEM),
            scratch_shapes=[
                pltpu.VMEM((nb, hl, wd), BF16),
                pltpu.VMEM((n, nb // 2, hl, 2 * wd), BF16),
                pltpu.VMEM((n, nb, hl, lat), BF16),
                pltpu.VMEM((n, nc, 1, 128), F32),
                pltpu.VMEM((6, nb, hl, lat), BF16),
                pltpu.VMEM((7, nc, 1, 128), F32),
                pltpu.VMEM((nb, hl, lat), F32),
                pltpu.VMEM((nb, hl, lat), F32),
                pltpu.VMEM((nc, 1, 128), F32),
                pltpu.VMEM((2 * PAIRS, wd + ROPE, sl), BF16),
                dma,
                dma((2 * PAIRS, 2)),
                dma((7, nc)),
                dma((7, nc)),
                dma((7, nc)),
                dma((7, nc)),
                dma((7, nc)),
                dma((7, nc)),
            ],
            compiler_params=pltpu.CompilerParams(
                collective_id=0, has_side_effects=True, vmem_limit_bytes=56 * 1024 * 1024),
            name='mla_decode',
        )(lengths, q, jnp.swapaxes(cache, 1, 2))

    return jax.shard_map(local, mesh=mesh, in_specs=(P('dp', 'dcp', None), P('dp', 'dcp', None), P('dp')),
                         out_specs=P('dp', 'dcp', None), check_vma=False)
```

```python
import functools

import jax
import jax.numpy as jnp
from jax import lax
from jax.experimental import pallas as pl
from jax.experimental.pallas import tpu as pltpu
from jax.sharding import PartitionSpec as P

ROPE = 64
SCALE = 192 ** -0.5
CORES = 2
CHUNK = 4
PAIRS = 4
AHEAD = 8
LEAD = 6
LAG_R = 4
LAG_F = 8

MESH = pl.DeviceIdType.MESH
F32 = jnp.float32
BF16 = jnp.bfloat16
VIA, DIRECT, MINE, PASS, SUM = 0, 2, 4, 5, 6


def weights(stats):
    top = functools.reduce(jnp.maximum, stats)
    top = jnp.maximum(top, jnp.finfo(F32).min)
    w = [jnp.exp(t - top) for t in stats]
    total = functools.reduce(jnp.add, w)
    inv = 1.0 / jnp.maximum(total, 1.0)
    return [x * inv for x in w], top + jnp.log(total)


def by_owner(stat, n, hl):
    t = stat.T[:n]
    block = lax.broadcasted_iota(jnp.int32, t.shape, 1) // hl
    row = lax.broadcasted_iota(jnp.int32, t.shape, 0)
    out = t
    for r in range(1, n):
        moved = pltpu.roll(pltpu.roll(t, r * hl, 1), n - r, 0)
        out = jnp.where((block - row + n) % n == r, moved, out)
    return out


def columns(row):
    return jnp.broadcast_to(row, (128, 128)).T


def scaled(w, i, o):
    hl, lat = o.shape
    return jnp.concatenate([w[i * hl:(i + 1) * hl]] * (lat // 128), axis=1) * o.astype(F32)


def kernel(n, len_ref, q_ref, ct_ref, o_ref, qraw, qg, od, st, inc, ins, lg, rs, rss, cbuf,
           raw_sem, cache_sem, q_send, q_recv, o_send, o_recv, t_send, t_recv):
    chips = n // CORES
    nb, hl, wd = q_ref.shape
    lat = wd - ROPE
    heads = n * hl
    sl = ct_ref.shape[2]
    nc = nb // CHUNK
    half = CHUNK // 2
    npair = nb // 2

    me = lax.axis_index('dcp')
    x = me // CORES
    k = me % CORES
    partner = x * CORES + (1 - k)

    def dev(step, core):
        return ((x + step + chips) % chips) * CORES + core

    def cache_copies(pair, par):
        slot = (pair % PAIRS) * 2 + par
        b = pair * 2 + par
        if par == 0:
            return [pltpu.make_async_copy(ct_ref.at[b], cbuf.at[slot, pl.ds(0, wd)], cache_sem.at[slot, 0])]
        return [
            pltpu.make_async_copy(ct_ref.at[b, pl.ds(0, lat)], cbuf.at[slot, pl.ds(0, lat)], cache_sem.at[slot, 0]),
            pltpu.make_async_copy(ct_ref.at[b, pl.ds(lat, ROPE)], cbuf.at[slot, pl.ds(wd, ROPE)], cache_sem.at[slot, 1]),
        ]

    def fetch(pair):
        for par in range(2):
            for cp in cache_copies(pair, par):
                cp.start()

    raw = pltpu.make_async_copy(q_ref, qraw, raw_sem)
    raw.start()

    barrier = pltpu.get_barrier_semaphore()
    peers = [partner, dev(1, 0), dev(1, 1), dev(-1, 0), dev(-1, 1)]
    for peer in peers:
        pl.semaphore_signal(barrier, inc=1, device_id={'dcp': peer}, device_id_type=MESH)

    raw.wait()

    def pack(g, _):
        for par in range(2):
            qg[me, g, :, pl.ds(par * lat, lat)] = qraw[2 * g + par, :, pl.ds(0, lat)]
        r0 = qraw[2 * g, :, pl.ds(lat, ROPE)]
        r1 = qraw[2 * g + 1, :, pl.ds(lat, ROPE)]
        qg[me, g, :, pl.ds(2 * lat, 2 * ROPE)] = jnp.concatenate([r0, r1], axis=1)
        return 0

    lax.fori_loop(0, half, pack, 0)
    pl.semaphore_wait(barrier, len(peers))

    def q_copy(kind, src, c, to):
        part = qg.at[src, pl.ds(c * half, half)]
        return pltpu.make_async_remote_copy(
            src_ref=part, dst_ref=part, send_sem=q_send.at[kind, c], recv_sem=q_recv.at[kind, c],
            device_id={'dcp': to}, device_id_type=MESH)

    def q_wait(kind, src, c):
        q_copy(kind, src, c, me).wait_recv()

    def sign(c):
        return 1 - 2 * (c % 2)

    def q0(c, _):
        @pl.when(c + 1 < nc)
        def _():
            lax.fori_loop((c + 1) * half, (c + 2) * half, pack, 0)

        q_copy(0, me, c, dev(1, k)).start()
        q_copy(1, me, c, dev(-1, k)).start()
        q_copy(2, me, c, partner).start()
        return 0

    lax.fori_loop(0, AHEAD, q0, 0)

    for g in range(PAIRS):
        fetch(g)
        cbuf[2 * g, pl.ds(wd, ROPE), :] = jnp.zeros((ROPE, sl), BF16)
        cbuf[2 * g + 1, pl.ds(lat, ROPE), :] = jnp.zeros((ROPE, sl), BF16)

    def q1(c, _):
        way = -sign(c)
        q_wait(0, dev(-1, k), c)
        q_copy(3, dev(-1, k), c, partner).start()
        q_wait(1, dev(1, k), c)
        q_copy(4, dev(1, k), c, partner).start()
        q_copy(5, dev(-way, k), c, dev(way, k)).start()

        @pl.when(c + AHEAD < nc)
        def _():
            q0(c + AHEAD, 0)

        return 0

    lax.fori_loop(0, LEAD, q1, 0)

    def q2(c):
        q_wait(5, dev(2, k), c)
        q_copy(6, dev(2, k), c, partner).start()

    def q3(c):
        q_wait(2, partner, c)
        q_wait(3, dev(-1, 1 - k), c)
        q_wait(4, dev(1, 1 - k), c)
        q_wait(6, dev(2, 1 - k), c)

    lane = lax.broadcasted_iota(jnp.int32, (heads, 128), 1)
    where_t = lax.broadcasted_iota(jnp.int32, (1, sl), 1)
    base = me * sl

    def attend(c):
        def pair_step(i, stat):
            g = c * half + i
            for par in range(2):
                b = g * 2 + par
                slot = (g % PAIRS) * 2 + par
                for cp in cache_copies(g, par):
                    cp.wait()
                qa = qg[:, g, :, pl.ds(par * lat, lat)].reshape(heads, lat)
                qr = qg[:, g, :, pl.ds(2 * lat, 2 * ROPE)].reshape(heads, 2 * ROPE)
                s = jnp.dot(qa, cbuf[slot, pl.ds(0, lat), :], preferred_element_type=F32)
                s = s + jnp.dot(qr, cbuf[slot, pl.ds(lat, 2 * ROPE), :], preferred_element_type=F32)
                s = jnp.where(where_t < len_ref[b] - base, s * SCALE, -jnp.inf)
                m = jnp.maximum(jnp.max(s, axis=1, keepdims=True), jnp.finfo(F32).min)
                p = jnp.exp(s - m)
                l = jnp.sum(p, axis=1, keepdims=True)
                pv = lax.dot_general(p.astype(BF16), cbuf[slot, pl.ds(0, lat), :], (((1,), (1,)), ((), ())),
                                     preferred_element_type=F32)
                o = (pv * (1.0 / jnp.maximum(l, 1.0))).astype(BF16)
                od[:, b, :, :] = o.reshape(n, hl, lat)
                stat = jnp.where(lane == i * 2 + par, m + jnp.log(l), stat)

            @pl.when(g + PAIRS < npair)
            def _():
                fetch(g + PAIRS)

            return stat

        stat = lax.fori_loop(0, half, pair_step, jnp.full((heads, 128), -jnp.inf, F32))
        lse = by_owner(stat, n, hl)
        for j in range(n):
            st[j, c] = lse[j:j + 1]

    def rows(c):
        return pl.ds(c * CHUNK, CHUNK)

    def o_copies(c, head, slot_s, slot_r, to):
        return [
            pltpu.make_async_remote_copy(
                src_ref=od.at[head, rows(c)], dst_ref=inc.at[slot_r, rows(c)],
                send_sem=o_send.at[slot_s, c], recv_sem=o_recv.at[slot_r, c],
                device_id={'dcp': to}, device_id_type=MESH),
            pltpu.make_async_remote_copy(
                src_ref=st.at[head, c], dst_ref=ins.at[slot_r, c],
                send_sem=t_send.at[slot_s, c], recv_sem=t_recv.at[slot_r, c],
                device_id={'dcp': to}, device_id_type=MESH),
        ]

    def sends(c):
        way = sign(c)
        out = []
        for kk in range(CORES):
            out += o_copies(c, dev(2, kk), VIA + kk, VIA + k, dev(way, kk))
        out += o_copies(c, dev(way, 1 - k), PASS, PASS, partner)
        out += o_copies(c, partner, MINE, MINE, partner)
        for kk in range(CORES):
            out += o_copies(c, dev(-way, kk), DIRECT + kk, DIRECT + k, dev(-way, kk))
        return out

    def sum_copies(c):
        to = dev(sign(c), k)
        return [
            pltpu.make_async_remote_copy(
                src_ref=rs.at[rows(c)], dst_ref=lg.at[rows(c)], send_sem=o_send.at[SUM, c], recv_sem=o_recv.at[SUM, c],
                device_id={'dcp': to}, device_id_type=MESH),
            pltpu.make_async_remote_copy(
                src_ref=rss.at[c], dst_ref=ins.at[SUM, c], send_sem=t_send.at[SUM, c], recv_sem=t_recv.at[SUM, c],
                device_id={'dcp': to}, device_id_type=MESH),
        ]

    def o_wait(c, slot):
        for cp in o_copies(c, me, slot, slot, me):
            cp.wait_recv()

    def relay(c):
        for slot in (PASS, VIA, VIA + 1):
            o_wait(c, slot)
        mine = dev(sign(c), k)
        w, lse = weights([st[mine, c], ins[PASS, c], ins[VIA, c], ins[VIA + 1, c]])
        w = [columns(r) for r in w]
        for i in range(CHUNK):
            b = c * CHUNK + i
            acc = scaled(w[0], i, od[mine, b])
            for j, slot in ((1, PASS), (2, VIA), (3, VIA + 1)):
                acc = acc + scaled(w[j], i, inc[slot, b])
            rs[b] = acc
        rss[c] = lse
        for cp in sum_copies(c):
            cp.start()

    def merge(c):
        for slot in (MINE, DIRECT, DIRECT + 1):
            o_wait(c, slot)
        for cp in sum_copies(c):
            cp.wait_recv()
        w, _ = weights([st[me, c], ins[MINE, c], ins[DIRECT, c], ins[DIRECT + 1, c], ins[SUM, c]])
        w = [columns(r) for r in w]
        for i in range(CHUNK):
            b = c * CHUNK + i
            acc = scaled(w[0], i, od[me, b])
            for j, slot in ((1, MINE), (2, DIRECT), (3, DIRECT + 1)):
                acc = acc + scaled(w[j], i, inc[slot, b])
            acc = acc + scaled(w[4], i, lg[b])
            o_ref[b] = acc.astype(BF16)

    def step(t, _):
        @pl.when(t + LEAD < nc)
        def _():
            q1(t + LEAD, 0)

        @pl.when(t < nc)
        def _():
            @pl.when(t == 0)
            def _():
                q2(0)

            @pl.when(t + 1 < nc)
            def _():
                q2(t + 1)

            q3(t)
            attend(t)
            for cp in sends(t):
                cp.start()

        @pl.when(jnp.logical_and(t >= LAG_R, t < nc + LAG_R))
        def _():
            relay(t - LAG_R)

        @pl.when(t >= LAG_F)
        def _():
            merge(t - LAG_F)

        return 0

    lax.fori_loop(0, nc + LAG_F, step, 0)

    def drain(c, _):
        for kind in range(7):
            q_copy(kind, me, c, me).wait_send()
        for cp in sends(c) + sum_copies(c):
            cp.wait_send()
        return 0

    lax.fori_loop(0, nc, drain, 0)


def solution(mesh):
    n = mesh.shape['dcp']

    def local(q, cache, lengths):
        nb, hl, wd = q.shape
        sl = cache.shape[1]
        lat = wd - ROPE
        nc = nb // CHUNK
        anyspace = pl.BlockSpec(memory_space=pl.ANY)
        dma = pltpu.SemaphoreType.DMA
        return pl.pallas_call(
            functools.partial(kernel, n),
            out_shape=pltpu.VMEM((nb, hl, lat), BF16),
            in_specs=[pl.BlockSpec(memory_space=pltpu.SMEM), anyspace, anyspace],
            out_specs=pl.BlockSpec(memory_space=pltpu.VMEM),
            scratch_shapes=[
                pltpu.VMEM((nb, hl, wd), BF16),
                pltpu.VMEM((n, nb // 2, hl, 2 * wd), BF16),
                pltpu.VMEM((n, nb, hl, lat), BF16),
                pltpu.VMEM((n, nc, 1, 128), F32),
                pltpu.VMEM((6, nb, hl, lat), BF16),
                pltpu.VMEM((7, nc, 1, 128), F32),
                pltpu.VMEM((nb, hl, lat), F32),
                pltpu.VMEM((nb, hl, lat), F32),
                pltpu.VMEM((nc, 1, 128), F32),
                pltpu.VMEM((2 * PAIRS, wd + ROPE, sl), BF16),
                dma,
                dma((2 * PAIRS, 2)),
                dma((7, nc)),
                dma((7, nc)),
                dma((7, nc)),
                dma((7, nc)),
                dma((7, nc)),
                dma((7, nc)),
            ],
            compiler_params=pltpu.CompilerParams(
                collective_id=0, has_side_effects=True, vmem_limit_bytes=56 * 1024 * 1024),
            name='mla_decode',
        )(lengths, q, jnp.swapaxes(cache, 1, 2))

    return jax.shard_map(local, mesh=mesh, in_specs=(P('dp', 'dcp', None), P('dp', 'dcp', None), P('dp')),
                         out_specs=P('dp', 'dcp', None), check_vma=False)
```

```python
import functools

import jax
import jax.numpy as jnp
from jax import lax
from jax.experimental import pallas as pl
from jax.experimental.pallas import tpu as pltpu
from jax.sharding import PartitionSpec as P

ROPE = 64
SCALE = 192 ** -0.5
CORES = 2
CHUNK = 8
PAIRS = 4
AHEAD = 4
LEAD = 3
LAG_V = 2
LAG_R = 3
LAG_D = 4
LAG_F = 6

MESH = pl.DeviceIdType.MESH
F32 = jnp.float32
BF16 = jnp.bfloat16
VIA, DIRECT, MINE, PASS, VIA2, DIRECT2, SUM = range(7)


def weights(stats):
    top = functools.reduce(jnp.maximum, stats)
    top = jnp.maximum(top, jnp.finfo(F32).min)
    w = [jnp.exp(t - top) for t in stats]
    total = functools.reduce(jnp.add, w)
    inv = 1.0 / jnp.maximum(total, 1.0)
    return [x * inv for x in w], top + jnp.log(total)


def by_owner(stat, n, hl):
    t = stat.T[:n]
    block = lax.broadcasted_iota(jnp.int32, t.shape, 1) // hl
    row = lax.broadcasted_iota(jnp.int32, t.shape, 0)
    out = t
    for r in range(1, n):
        moved = pltpu.roll(pltpu.roll(t, r * hl, 1), n - r, 0)
        out = jnp.where((block - row + n) % n == r, moved, out)
    return out


def columns(row):
    return jnp.broadcast_to(row, (128, 128)).T


def scaled(w, i, o):
    hl, lat = o.shape
    return jnp.concatenate([w[i * hl:(i + 1) * hl]] * (lat // 128), axis=1) * o.astype(F32)


def kernel(n, len_ref, q_ref, ct_ref, o_ref, qraw, qg, od, st, two, twos, inc, ins, lg, rs, rss, cbuf,
           raw_sem, cache_sem, q_send, q_recv, o_send, o_recv, t_send, t_recv):
    chips = n // CORES
    nb, hl, wd = q_ref.shape
    lat = wd - ROPE
    heads = n * hl
    sl = ct_ref.shape[2]
    nc = nb // CHUNK
    half = CHUNK // 2
    npair = nb // 2

    me = lax.axis_index('dcp')
    x = me // CORES
    k = me % CORES
    partner = x * CORES + (1 - k)

    def dev(step, core):
        return ((x + step + chips) % chips) * CORES + core

    def cache_copies(pair, par):
        slot = (pair % PAIRS) * 2 + par
        b = pair * 2 + par
        if par == 0:
            return [pltpu.make_async_copy(ct_ref.at[b], cbuf.at[slot, pl.ds(0, wd)], cache_sem.at[slot, 0])]
        return [
            pltpu.make_async_copy(ct_ref.at[b, pl.ds(0, lat)], cbuf.at[slot, pl.ds(0, lat)], cache_sem.at[slot, 0]),
            pltpu.make_async_copy(ct_ref.at[b, pl.ds(lat, ROPE)], cbuf.at[slot, pl.ds(wd, ROPE)], cache_sem.at[slot, 1]),
        ]

    def fetch(pair):
        for par in range(2):
            for cp in cache_copies(pair, par):
                cp.start()

    raw = pltpu.make_async_copy(q_ref, qraw, raw_sem)
    raw.start()

    barrier = pltpu.get_barrier_semaphore()
    peers = [partner, dev(1, 0), dev(1, 1), dev(-1, 0), dev(-1, 1)]
    for peer in peers:
        pl.semaphore_signal(barrier, inc=1, device_id={'dcp': peer}, device_id_type=MESH)

    raw.wait()

    def pack(g, _):
        for par in range(2):
            qg[me, g, :, pl.ds(par * lat, lat)] = qraw[2 * g + par, :, pl.ds(0, lat)]
        r0 = qraw[2 * g, :, pl.ds(lat, ROPE)]
        r1 = qraw[2 * g + 1, :, pl.ds(lat, ROPE)]
        qg[me, g, :, pl.ds(2 * lat, 2 * ROPE)] = jnp.concatenate([r0, r1], axis=1)
        return 0

    lax.fori_loop(0, half, pack, 0)
    pl.semaphore_wait(barrier, len(peers))

    def q_copy(kind, src, c, to):
        part = qg.at[src, pl.ds(c * half, half)]
        return pltpu.make_async_remote_copy(
            src_ref=part, dst_ref=part, send_sem=q_send.at[kind, c], recv_sem=q_recv.at[kind, c],
            device_id={'dcp': to}, device_id_type=MESH)

    def q_wait(kind, src, c):
        q_copy(kind, src, c, me).wait_recv()

    def sign(c):
        return 1 - 2 * (c % 2)

    def q0(c, _):
        @pl.when(c + 1 < nc)
        def _():
            lax.fori_loop((c + 1) * half, (c + 2) * half, pack, 0)

        q_copy(0, me, c, dev(1, k)).start()
        q_copy(1, me, c, dev(-1, k)).start()
        q_copy(2, me, c, partner).start()
        return 0

    lax.fori_loop(0, AHEAD, q0, 0)

    for g in range(PAIRS):
        fetch(g)
        cbuf[2 * g, pl.ds(wd, ROPE), :] = jnp.zeros((ROPE, sl), BF16)
        cbuf[2 * g + 1, pl.ds(lat, ROPE), :] = jnp.zeros((ROPE, sl), BF16)

    def q1(c, _):
        way = -sign(c)
        q_wait(0, dev(-1, k), c)
        q_copy(3, dev(-1, k), c, partner).start()
        q_wait(1, dev(1, k), c)
        q_copy(4, dev(1, k), c, partner).start()
        q_copy(5, dev(-way, k), c, dev(way, k)).start()

        @pl.when(c + AHEAD < nc)
        def _():
            q0(c + AHEAD, 0)

        return 0

    lax.fori_loop(0, LEAD, q1, 0)

    def q2(c):
        q_wait(5, dev(2, k), c)
        q_copy(6, dev(2, k), c, partner).start()

    def q3(c):
        q_wait(2, partner, c)
        q_wait(3, dev(-1, 1 - k), c)
        q_wait(4, dev(1, 1 - k), c)
        q_wait(6, dev(2, 1 - k), c)

    lane = lax.broadcasted_iota(jnp.int32, (heads, 128), 1)
    where_t = lax.broadcasted_iota(jnp.int32, (1, sl), 1)
    base = me * sl

    def attend(c):
        def pair_step(i, stat):
            g = c * half + i
            for par in range(2):
                b = g * 2 + par
                slot = (g % PAIRS) * 2 + par
                for cp in cache_copies(g, par):
                    cp.wait()
                qa = qg[:, g, :, pl.ds(par * lat, lat)].reshape(heads, lat)
                qr = qg[:, g, :, pl.ds(2 * lat, 2 * ROPE)].reshape(heads, 2 * ROPE)
                s = jnp.dot(qa, cbuf[slot, pl.ds(0, lat), :], preferred_element_type=F32)
                s = s + jnp.dot(qr, cbuf[slot, pl.ds(lat, 2 * ROPE), :], preferred_element_type=F32)
                s = jnp.where(where_t < len_ref[b] - base, s * SCALE, -jnp.inf)
                m = jnp.maximum(jnp.max(s, axis=1, keepdims=True), jnp.finfo(F32).min)
                p = jnp.exp(s - m)
                l = jnp.sum(p, axis=1, keepdims=True)
                pv = lax.dot_general(p.astype(BF16), cbuf[slot, pl.ds(0, lat), :], (((1,), (1,)), ((), ())),
                                     preferred_element_type=F32)
                o = (pv * (1.0 / jnp.maximum(l, 1.0))).astype(BF16)
                od[:, b] = o.reshape(chips, CORES, hl, lat)
                stat = jnp.where(lane == i * 2 + par, m + jnp.log(l), stat)

            @pl.when(g + PAIRS < npair)
            def _():
                fetch(g + PAIRS)

            return stat

        stat = lax.fori_loop(0, half, pair_step, jnp.full((heads, 128), -jnp.inf, F32))
        lse = by_owner(stat, n, hl)
        for j in range(n):
            st[j // CORES, c, j % CORES] = lse[j:j + 1]

    def rows(c):
        return pl.ds(c * CHUNK, CHUNK)

    def o_copies(c, kind, src, srcs, dst, dsts, to):
        return [
            pltpu.make_async_remote_copy(
                src_ref=src, dst_ref=dst, send_sem=o_send.at[kind, c], recv_sem=o_recv.at[kind, c],
                device_id={'dcp': to}, device_id_type=MESH),
            pltpu.make_async_remote_copy(
                src_ref=srcs, dst_ref=dsts, send_sem=t_send.at[kind, c], recv_sem=t_recv.at[kind, c],
                device_id={'dcp': to}, device_id_type=MESH),
        ]

    def to_chip(c, kind, head, step):
        return o_copies(c, kind, od.at[head, rows(c)], st.at[head, c], two.at[kind, rows(c)], twos.at[kind, c],
                        dev(step, k))

    def to_partner(c, kind, src, srcs):
        return o_copies(c, kind, src, srcs, inc.at[kind - MINE, rows(c)], ins.at[kind, c], partner)

    def chip(step):
        return (x + step + chips) % chips

    def sends(c):
        way = sign(c)
        relayed = chip(way)
        return (to_chip(c, VIA, chip(2), way)
                + to_partner(c, PASS, od.at[relayed, rows(c), 1 - k], st.at[relayed, c, 1 - k])
                + to_partner(c, MINE, od.at[x, rows(c), 1 - k], st.at[x, c, 1 - k])
                + to_chip(c, DIRECT, chip(-way), -way))

    def share(c, kind):
        return to_partner(c, kind + VIA2, two.at[kind, rows(c), 1 - k], twos.at[kind, c, 1 - k])

    def pass_on(c, kind):
        for cp in to_chip(c, kind, x, 0):
            cp.wait_recv()
        for cp in share(c, kind):
            cp.start()

    def partner_wait(c, kind):
        for cp in to_partner(c, kind, inc.at[kind - MINE, rows(c)], ins.at[kind, c]):
            cp.wait_recv()

    def sum_copies(c):
        return o_copies(c, SUM, rs.at[rows(c)], rss.at[c], lg.at[rows(c)], ins.at[SUM, c], dev(sign(c), k))

    def relay(c):
        for kind in (PASS, VIA2):
            partner_wait(c, kind)
        mine = chip(sign(c))
        w, lse = weights([st[mine, c, k], ins[PASS, c], twos[VIA, c, k], ins[VIA2, c]])
        w = [columns(r) for r in w]
        for i in range(CHUNK):
            b = c * CHUNK + i
            acc = scaled(w[0], i, od[mine, b, k])
            acc = acc + scaled(w[1], i, inc[PASS - MINE, b])
            acc = acc + scaled(w[2], i, two[VIA, b, k])
            acc = acc + scaled(w[3], i, inc[VIA2 - MINE, b])
            rs[b] = acc
        rss[c] = lse
        for cp in sum_copies(c):
            cp.start()

    def merge(c):
        for kind in (MINE, DIRECT2):
            partner_wait(c, kind)
        for cp in sum_copies(c):
            cp.wait_recv()
        w, _ = weights([st[x, c, k], ins[MINE, c], twos[DIRECT, c, k], ins[DIRECT2, c], ins[SUM, c]])
        w = [columns(r) for r in w]
        for i in range(CHUNK):
            b = c * CHUNK + i
            acc = scaled(w[0], i, od[x, b, k])
            acc = acc + scaled(w[1], i, inc[MINE - MINE, b])
            acc = acc + scaled(w[2], i, two[DIRECT, b, k])
            acc = acc + scaled(w[3], i, inc[DIRECT2 - MINE, b])
            acc = acc + scaled(w[4], i, lg[b])
            o_ref[b] = acc.astype(BF16)

    def step(t, _):
        @pl.when(t + LEAD < nc)
        def _():
            q1(t + LEAD, 0)

        @pl.when(t < nc)
        def _():
            @pl.when(t == 0)
            def _():
                q2(0)

            @pl.when(t + 1 < nc)
            def _():
                q2(t + 1)

            q3(t)
            attend(t)
            for cp in sends(t):
                cp.start()

        @pl.when(jnp.logical_and(t >= LAG_V, t < nc + LAG_V))
        def _():
            pass_on(t - LAG_V, VIA)

        @pl.when(jnp.logical_and(t >= LAG_R, t < nc + LAG_R))
        def _():
            relay(t - LAG_R)

        @pl.when(jnp.logical_and(t >= LAG_D, t < nc + LAG_D))
        def _():
            pass_on(t - LAG_D, DIRECT)

        @pl.when(t >= LAG_F)
        def _():
            merge(t - LAG_F)

        return 0

    lax.fori_loop(0, nc + LAG_F, step, 0)

    def drain(c, _):
        for kind in range(7):
            q_copy(kind, me, c, me).wait_send()
        for cp in sends(c) + share(c, VIA) + share(c, DIRECT) + sum_copies(c):
            cp.wait_send()
        return 0

    lax.fori_loop(0, nc, drain, 0)


def solution(mesh):
    n = mesh.shape['dcp']

    def local(q, cache, lengths):
        nb, hl, wd = q.shape
        sl = cache.shape[1]
        lat = wd - ROPE
        nc = nb // CHUNK
        anyspace = pl.BlockSpec(memory_space=pl.ANY)
        dma = pltpu.SemaphoreType.DMA
        return pl.pallas_call(
            functools.partial(kernel, n),
            out_shape=pltpu.VMEM((nb, hl, lat), BF16),
            in_specs=[pl.BlockSpec(memory_space=pltpu.SMEM), anyspace, anyspace],
            out_specs=pl.BlockSpec(memory_space=pltpu.VMEM),
            scratch_shapes=[
                pltpu.VMEM((nb, hl, wd), BF16),
                pltpu.VMEM((n, nb // 2, hl, 2 * wd), BF16),
                pltpu.VMEM((n // CORES, nb, CORES, hl, lat), BF16),
                pltpu.VMEM((n // CORES, nc, CORES, 1, 128), F32),
                pltpu.VMEM((2, nb, CORES, hl, lat), BF16),
                pltpu.VMEM((2, nc, CORES, 1, 128), F32),
                pltpu.VMEM((4, nb, hl, lat), BF16),
                pltpu.VMEM((7, nc, 1, 128), F32),
                pltpu.VMEM((nb, hl, lat), F32),
                pltpu.VMEM((nb, hl, lat), F32),
                pltpu.VMEM((nc, 1, 128), F32),
                pltpu.VMEM((2 * PAIRS, wd + ROPE, sl), BF16),
                dma,
                dma((2 * PAIRS, 2)),
                dma((7, nc)),
                dma((7, nc)),
                dma((7, nc)),
                dma((7, nc)),
                dma((7, nc)),
                dma((7, nc)),
            ],
            compiler_params=pltpu.CompilerParams(
                collective_id=0, has_side_effects=True, vmem_limit_bytes=56 * 1024 * 1024),
            name='mla_decode',
        )(lengths, q, jnp.swapaxes(cache, 1, 2))

    return jax.shard_map(local, mesh=mesh, in_specs=(P('dp', 'dcp', None), P('dp', 'dcp', None), P('dp')),
                         out_specs=P('dp', 'dcp', None), check_vma=False)
```

```python
import functools

import jax
import jax.numpy as jnp
from jax import lax
from jax.experimental import pallas as pl
from jax.experimental.pallas import tpu as pltpu
from jax.sharding import PartitionSpec as P

ROPE = 64
SCALE = 192 ** -0.5
CORES = 2
CHUNK = 8
PAIRS = 4
AHEAD = 4
LEAD = 3
LAG_V = 2
LAG_R = 3
LAG_D = 4
LAG_F = 6

MESH = pl.DeviceIdType.MESH
F32 = jnp.float32
BF16 = jnp.bfloat16
VIA, DIRECT, MINE, PASS, VIA2, DIRECT2, SUM = range(7)


def weights(stats):
    top = functools.reduce(jnp.maximum, stats)
    top = jnp.maximum(top, jnp.finfo(F32).min)
    w = [jnp.exp(t - top) for t in stats]
    total = functools.reduce(jnp.add, w)
    inv = 1.0 / jnp.maximum(total, 1.0)
    return [x * inv for x in w], top + jnp.log(total)


def by_owner(stat, n, hl):
    t = stat.T[:n]
    block = lax.broadcasted_iota(jnp.int32, t.shape, 1) // hl
    row = lax.broadcasted_iota(jnp.int32, t.shape, 0)
    out = t
    for r in range(1, n):
        moved = pltpu.roll(pltpu.roll(t, r * hl, 1), n - r, 0)
        out = jnp.where((block - row + n) % n == r, moved, out)
    return out


def columns(row):
    return jnp.broadcast_to(row, (128, 128)).T


def scaled(w, i, o):
    hl, lat = o.shape
    return jnp.concatenate([w[i * hl:(i + 1) * hl]] * (lat // 128), axis=1) * o.astype(F32)


def kernel(n, len_ref, q_ref, ct_ref, o_ref, qraw, qg, od, st, two, twos, inc, ins, lg, rs, rss, cbuf,
           raw_sem, cache_sem, q_send, q_recv, o_send, o_recv, t_send, t_recv):
    chips = n // CORES
    nb, hl, wd = q_ref.shape
    lat = wd - ROPE
    heads = n * hl
    sl = ct_ref.shape[2]
    nc = nb // CHUNK
    half = CHUNK // 2
    npair = nb // 2

    me = lax.axis_index('dcp')
    x = me // CORES
    k = me % CORES
    partner = x * CORES + (1 - k)

    def dev(step, core):
        return ((x + step + chips) % chips) * CORES + core

    def cache_copies(pair, par):
        slot = (pair % PAIRS) * 2 + par
        b = pair * 2 + par
        if par == 0:
            return [pltpu.make_async_copy(ct_ref.at[b], cbuf.at[slot, pl.ds(0, wd)], cache_sem.at[slot, 0])]
        return [
            pltpu.make_async_copy(ct_ref.at[b, pl.ds(0, lat)], cbuf.at[slot, pl.ds(0, lat)], cache_sem.at[slot, 0]),
            pltpu.make_async_copy(ct_ref.at[b, pl.ds(lat, ROPE)], cbuf.at[slot, pl.ds(wd, ROPE)], cache_sem.at[slot, 1]),
        ]

    def fetch(pair):
        for par in range(2):
            for cp in cache_copies(pair, par):
                cp.start()

    raw = pltpu.make_async_copy(q_ref, qraw, raw_sem)
    raw.start()

    barrier = pltpu.get_barrier_semaphore()
    peers = [partner, dev(1, 0), dev(1, 1), dev(-1, 0), dev(-1, 1)]
    for peer in peers:
        pl.semaphore_signal(barrier, inc=1, device_id={'dcp': peer}, device_id_type=MESH)

    raw.wait()

    def pack(g, _):
        for par in range(2):
            qg[me, g, :, pl.ds(par * lat, lat)] = qraw[2 * g + par, :, pl.ds(0, lat)]
        r0 = qraw[2 * g, :, pl.ds(lat, ROPE)]
        r1 = qraw[2 * g + 1, :, pl.ds(lat, ROPE)]
        qg[me, g, :, pl.ds(2 * lat, 2 * ROPE)] = jnp.concatenate([r0, r1], axis=1)
        return 0

    lax.fori_loop(0, half, pack, 0)
    pl.semaphore_wait(barrier, len(peers))

    def q_copy(kind, src, c, to):
        part = qg.at[src, pl.ds(c * half, half)]
        return pltpu.make_async_remote_copy(
            src_ref=part, dst_ref=part, send_sem=q_send.at[kind, c], recv_sem=q_recv.at[kind, c],
            device_id={'dcp': to}, device_id_type=MESH)

    def q_wait(kind, src, c):
        q_copy(kind, src, c, me).wait_recv()

    def sign(c):
        return 1 - 2 * (c % 2)

    def q0(c, _):
        @pl.when(c + 1 < nc)
        def _():
            lax.fori_loop((c + 1) * half, (c + 2) * half, pack, 0)

        q_copy(0, me, c, dev(1, k)).start()
        q_copy(1, me, c, dev(-1, k)).start()
        q_copy(2, me, c, partner).start()
        return 0

    lax.fori_loop(0, AHEAD, q0, 0)

    for g in range(PAIRS):
        fetch(g)
        cbuf[2 * g, pl.ds(wd, ROPE), :] = jnp.zeros((ROPE, sl), BF16)
        cbuf[2 * g + 1, pl.ds(lat, ROPE), :] = jnp.zeros((ROPE, sl), BF16)

    def q1(c, _):
        way = -sign(c)
        q_wait(0, dev(-1, k), c)
        q_copy(3, dev(-1, k), c, partner).start()
        q_wait(1, dev(1, k), c)
        q_copy(4, dev(1, k), c, partner).start()
        q_copy(5, dev(-way, k), c, dev(way, k)).start()

        @pl.when(c + AHEAD < nc)
        def _():
            q0(c + AHEAD, 0)

        return 0

    lax.fori_loop(0, LEAD, q1, 0)

    def q2(c):
        q_wait(5, dev(2, k), c)
        q_copy(6, dev(2, k), c, partner).start()

    def q3(c):
        q_wait(2, partner, c)
        q_wait(3, dev(-1, 1 - k), c)
        q_wait(4, dev(1, 1 - k), c)
        q_wait(6, dev(2, 1 - k), c)

    lane = lax.broadcasted_iota(jnp.int32, (heads, 128), 1)
    where_t = lax.broadcasted_iota(jnp.int32, (1, sl), 1)
    base = me * sl

    def arrive(g):
        for par in range(2):
            for cp in cache_copies(g, par):
                cp.wait()

    def scores(g, par):
        b = g * 2 + par
        slot = (g % PAIRS) * 2 + par
        qa = qg[:, g, :, pl.ds(par * lat, lat)].reshape(heads, lat)
        qr = qg[:, g, :, pl.ds(2 * lat, 2 * ROPE)].reshape(heads, 2 * ROPE)
        s = jnp.dot(qa, cbuf[slot, pl.ds(0, lat), :], preferred_element_type=F32)
        s = s + jnp.dot(qr, cbuf[slot, pl.ds(lat, 2 * ROPE), :], preferred_element_type=F32)
        return jnp.where(where_t < len_ref[b] - base, s * SCALE, -jnp.inf)

    def finish(g, par, s):
        b = g * 2 + par
        slot = (g % PAIRS) * 2 + par
        m = jnp.maximum(jnp.max(s, axis=1, keepdims=True), jnp.finfo(F32).min)
        p = jnp.exp(s - m)
        l = jnp.sum(p, axis=1, keepdims=True)
        pv = lax.dot_general(p.astype(BF16), cbuf[slot, pl.ds(0, lat), :], (((1,), (1,)), ((), ())),
                             preferred_element_type=F32)
        o = (pv * (1.0 / jnp.maximum(l, 1.0))).astype(BF16)
        od[:, b] = o.reshape(chips, CORES, hl, lat)
        return m + jnp.log(l)

    def attend(c):
        stat = jnp.full((heads, 128), -jnp.inf, F32)
        first = c * half
        arrive(first)
        s0 = scores(first, 0)
        for i in range(half):
            g = first + i
            if i + 1 < half:
                arrive(g + 1)
            s1 = scores(g, 1)
            stat = jnp.where(lane == 2 * i, finish(g, 0, s0), stat)
            if i + 1 < half:
                s0 = scores(g + 1, 0)
            stat = jnp.where(lane == 2 * i + 1, finish(g, 1, s1), stat)

            @pl.when(g + PAIRS < npair)
            def _():
                fetch(g + PAIRS)

        lse = by_owner(stat, n, hl)
        for j in range(n):
            st[j // CORES, c, j % CORES] = lse[j:j + 1]

    def rows(c):
        return pl.ds(c * CHUNK, CHUNK)

    def o_copies(c, kind, src, srcs, dst, dsts, to):
        return [
            pltpu.make_async_remote_copy(
                src_ref=src, dst_ref=dst, send_sem=o_send.at[kind, c], recv_sem=o_recv.at[kind, c],
                device_id={'dcp': to}, device_id_type=MESH),
            pltpu.make_async_remote_copy(
                src_ref=srcs, dst_ref=dsts, send_sem=t_send.at[kind, c], recv_sem=t_recv.at[kind, c],
                device_id={'dcp': to}, device_id_type=MESH),
        ]

    def to_chip(c, kind, head, step):
        return o_copies(c, kind, od.at[head, rows(c)], st.at[head, c], two.at[kind, rows(c)], twos.at[kind, c],
                        dev(step, k))

    def to_partner(c, kind, src, srcs):
        return o_copies(c, kind, src, srcs, inc.at[kind - MINE, rows(c)], ins.at[kind, c], partner)

    def chip(step):
        return (x + step + chips) % chips

    def sends(c):
        way = sign(c)
        relayed = chip(way)
        return (to_chip(c, VIA, chip(2), way)
                + to_partner(c, PASS, od.at[relayed, rows(c), 1 - k], st.at[relayed, c, 1 - k])
                + to_partner(c, MINE, od.at[x, rows(c), 1 - k], st.at[x, c, 1 - k])
                + to_chip(c, DIRECT, chip(-way), -way))

    def share(c, kind):
        return to_partner(c, kind + VIA2, two.at[kind, rows(c), 1 - k], twos.at[kind, c, 1 - k])

    def pass_on(c, kind):
        for cp in to_chip(c, kind, x, 0):
            cp.wait_recv()
        for cp in share(c, kind):
            cp.start()

    def partner_wait(c, kind):
        for cp in to_partner(c, kind, inc.at[kind - MINE, rows(c)], ins.at[kind, c]):
            cp.wait_recv()

    def sum_copies(c):
        return o_copies(c, SUM, rs.at[rows(c)], rss.at[c], lg.at[rows(c)], ins.at[SUM, c], dev(sign(c), k))

    def relay(c):
        for kind in (PASS, VIA2):
            partner_wait(c, kind)
        mine = chip(sign(c))
        w, lse = weights([st[mine, c, k], ins[PASS, c], twos[VIA, c, k], ins[VIA2, c]])
        w = [columns(r) for r in w]
        for i in range(CHUNK):
            b = c * CHUNK + i
            acc = scaled(w[0], i, od[mine, b, k])
            acc = acc + scaled(w[1], i, inc[PASS - MINE, b])
            acc = acc + scaled(w[2], i, two[VIA, b, k])
            acc = acc + scaled(w[3], i, inc[VIA2 - MINE, b])
            rs[b] = acc
        rss[c] = lse
        for cp in sum_copies(c):
            cp.start()

    def merge(c):
        for kind in (MINE, DIRECT2):
            partner_wait(c, kind)
        for cp in sum_copies(c):
            cp.wait_recv()
        w, _ = weights([st[x, c, k], ins[MINE, c], twos[DIRECT, c, k], ins[DIRECT2, c], ins[SUM, c]])
        w = [columns(r) for r in w]
        for i in range(CHUNK):
            b = c * CHUNK + i
            acc = scaled(w[0], i, od[x, b, k])
            acc = acc + scaled(w[1], i, inc[MINE - MINE, b])
            acc = acc + scaled(w[2], i, two[DIRECT, b, k])
            acc = acc + scaled(w[3], i, inc[DIRECT2 - MINE, b])
            acc = acc + scaled(w[4], i, lg[b])
            o_ref[b] = acc.astype(BF16)

    def step(t, _):
        @pl.when(t + LEAD < nc)
        def _():
            q1(t + LEAD, 0)

        @pl.when(t < nc)
        def _():
            @pl.when(t == 0)
            def _():
                q2(0)

            @pl.when(t + 1 < nc)
            def _():
                q2(t + 1)

            q3(t)
            attend(t)
            for cp in sends(t):
                cp.start()

        @pl.when(jnp.logical_and(t >= LAG_V, t < nc + LAG_V))
        def _():
            pass_on(t - LAG_V, VIA)

        @pl.when(jnp.logical_and(t >= LAG_R, t < nc + LAG_R))
        def _():
            relay(t - LAG_R)

        @pl.when(jnp.logical_and(t >= LAG_D, t < nc + LAG_D))
        def _():
            pass_on(t - LAG_D, DIRECT)

        @pl.when(t >= LAG_F)
        def _():
            merge(t - LAG_F)

        return 0

    lax.fori_loop(0, nc + LAG_F, step, 0)

    def drain(c, _):
        for kind in range(7):
            q_copy(kind, me, c, me).wait_send()
        for cp in sends(c) + share(c, VIA) + share(c, DIRECT) + sum_copies(c):
            cp.wait_send()
        return 0

    lax.fori_loop(0, nc, drain, 0)


def solution(mesh):
    n = mesh.shape['dcp']

    def local(q, cache, lengths):
        nb, hl, wd = q.shape
        sl = cache.shape[1]
        lat = wd - ROPE
        nc = nb // CHUNK
        anyspace = pl.BlockSpec(memory_space=pl.ANY)
        dma = pltpu.SemaphoreType.DMA
        return pl.pallas_call(
            functools.partial(kernel, n),
            out_shape=pltpu.VMEM((nb, hl, lat), BF16),
            in_specs=[pl.BlockSpec(memory_space=pltpu.SMEM), anyspace, anyspace],
            out_specs=pl.BlockSpec(memory_space=pltpu.VMEM),
            scratch_shapes=[
                pltpu.VMEM((nb, hl, wd), BF16),
                pltpu.VMEM((n, nb // 2, hl, 2 * wd), BF16),
                pltpu.VMEM((n // CORES, nb, CORES, hl, lat), BF16),
                pltpu.VMEM((n // CORES, nc, CORES, 1, 128), F32),
                pltpu.VMEM((2, nb, CORES, hl, lat), BF16),
                pltpu.VMEM((2, nc, CORES, 1, 128), F32),
                pltpu.VMEM((4, nb, hl, lat), BF16),
                pltpu.VMEM((7, nc, 1, 128), F32),
                pltpu.VMEM((nb, hl, lat), F32),
                pltpu.VMEM((nb, hl, lat), F32),
                pltpu.VMEM((nc, 1, 128), F32),
                pltpu.VMEM((2 * PAIRS, wd + ROPE, sl), BF16),
                dma,
                dma((2 * PAIRS, 2)),
                dma((7, nc)),
                dma((7, nc)),
                dma((7, nc)),
                dma((7, nc)),
                dma((7, nc)),
                dma((7, nc)),
            ],
            compiler_params=pltpu.CompilerParams(
                collective_id=0, has_side_effects=True, vmem_limit_bytes=56 * 1024 * 1024),
            name='mla_decode',
        )(lengths, q, jnp.swapaxes(cache, 1, 2))

    return jax.shard_map(local, mesh=mesh, in_specs=(P('dp', 'dcp', None), P('dp', 'dcp', None), P('dp')),
                         out_specs=P('dp', 'dcp', None), check_vma=False)
```

```python
import functools

import jax
import jax.numpy as jnp
from jax import lax
from jax.experimental import pallas as pl
from jax.experimental.pallas import tpu as pltpu
from jax.sharding import PartitionSpec as P

ROPE = 64
SCALE = 192 ** -0.5
CORES = 2
CHUNK = 8
PAIRS = 4
AHEAD = 4
LEAD = 3
LAG_V = 2
LAG_R = 3
LAG_D = 4
LAG_F = 6

MESH = pl.DeviceIdType.MESH
F32 = jnp.float32
BF16 = jnp.bfloat16
VIA, DIRECT, MINE, PASS, VIA2, DIRECT2, SUM = range(7)


def weights(stats):
    top = functools.reduce(jnp.maximum, stats)
    top = jnp.maximum(top, jnp.finfo(F32).min)
    w = [jnp.exp(t - top) for t in stats]
    total = functools.reduce(jnp.add, w)
    inv = 1.0 / jnp.maximum(total, 1.0)
    return [x * inv for x in w], top + jnp.log(total)


def by_owner(stat, n, hl):
    t = stat.T[:n]
    block = lax.broadcasted_iota(jnp.int32, t.shape, 1) // hl
    row = lax.broadcasted_iota(jnp.int32, t.shape, 0)
    out = t
    for r in range(1, n):
        moved = pltpu.roll(pltpu.roll(t, r * hl, 1), n - r, 0)
        out = jnp.where((block - row + n) % n == r, moved, out)
    return out


def columns(row):
    return jnp.broadcast_to(row, (128, 128)).T


def scaled(w, i, o):
    hl, lat = o.shape
    return jnp.concatenate([w[i * hl:(i + 1) * hl]] * (lat // 128), axis=1) * o.astype(F32)


def kernel(n, len_hbm, q_ref, ct_ref, o_ref, len_ref, qraw, qg, od, st, two, twos, inc, ins, lg, rs, rss, cbuf,
           len_sem, raw_sem, cache_sem, q_send, q_recv, o_send, o_recv, t_send, t_recv):
    chips = n // CORES
    nb, hl, wd = q_ref.shape
    lat = wd - ROPE
    heads = n * hl
    sl = ct_ref.shape[2]
    nc = nb // CHUNK
    half = CHUNK // 2
    npair = nb // 2

    me = lax.axis_index('dcp')
    x = me // CORES
    k = me % CORES
    partner = x * CORES + (1 - k)

    def dev(step, core):
        return ((x + step + chips) % chips) * CORES + core

    def cache_copies(pair, par):
        slot = (pair % PAIRS) * 2 + par
        b = pair * 2 + par
        if par == 0:
            return [pltpu.make_async_copy(ct_ref.at[b], cbuf.at[slot, pl.ds(0, wd)], cache_sem.at[slot, 0])]
        return [
            pltpu.make_async_copy(ct_ref.at[b, pl.ds(0, lat)], cbuf.at[slot, pl.ds(0, lat)], cache_sem.at[slot, 0]),
            pltpu.make_async_copy(ct_ref.at[b, pl.ds(lat, ROPE)], cbuf.at[slot, pl.ds(wd, ROPE)], cache_sem.at[slot, 1]),
        ]

    def fetch(pair):
        for par in range(2):
            for cp in cache_copies(pair, par):
                cp.start()

    barrier = pltpu.get_barrier_semaphore()
    peers = [dev(1, k), dev(-1, k), partner]
    for peer in peers:
        pl.semaphore_signal(barrier, inc=1, device_id={'dcp': peer}, device_id_type=MESH)

    def raw(c):
        part = pl.ds(c * CHUNK, CHUNK)
        return pltpu.make_async_copy(q_ref.at[part], qraw.at[part], raw_sem.at[c])

    for c in range(nc):
        raw(c).start()
    lengths = pltpu.make_async_copy(len_hbm, len_ref, len_sem)
    lengths.start()

    def pack(g, _):
        for par in range(2):
            qg[me, g, :, pl.ds(par * lat, lat)] = qraw[2 * g + par, :, pl.ds(0, lat)]
        r0 = qraw[2 * g, :, pl.ds(lat, ROPE)]
        r1 = qraw[2 * g + 1, :, pl.ds(lat, ROPE)]
        qg[me, g, :, pl.ds(2 * lat, 2 * ROPE)] = jnp.concatenate([r0, r1], axis=1)
        return 0

    raw(0).wait()
    lax.fori_loop(0, half, pack, 0)
    pl.semaphore_wait(barrier, len(peers))

    def q_copy(kind, src, c, to):
        part = qg.at[src, pl.ds(c * half, half)]
        return pltpu.make_async_remote_copy(
            src_ref=part, dst_ref=part, send_sem=q_send.at[kind, c], recv_sem=q_recv.at[kind, c],
            device_id={'dcp': to}, device_id_type=MESH)

    def q_wait(kind, src, c):
        q_copy(kind, src, c, me).wait_recv()

    def sign(c):
        return 1 - 2 * (c % 2)

    def q0(c, _):
        @pl.when(c + 1 < nc)
        def _():
            raw(c + 1).wait()
            lax.fori_loop((c + 1) * half, (c + 2) * half, pack, 0)

        q_copy(0, me, c, dev(1, k)).start()
        q_copy(1, me, c, dev(-1, k)).start()
        q_copy(2, me, c, partner).start()
        return 0

    lax.fori_loop(0, AHEAD, q0, 0)

    for g in range(PAIRS):
        fetch(g)
        cbuf[2 * g, pl.ds(wd, ROPE), :] = jnp.zeros((ROPE, sl), BF16)
        cbuf[2 * g + 1, pl.ds(lat, ROPE), :] = jnp.zeros((ROPE, sl), BF16)

    def q1(c, _):
        way = -sign(c)
        q_wait(0, dev(-1, k), c)
        q_copy(3, dev(-1, k), c, partner).start()
        q_wait(1, dev(1, k), c)
        q_copy(4, dev(1, k), c, partner).start()
        q_copy(5, dev(-way, k), c, dev(way, k)).start()

        @pl.when(c + AHEAD < nc)
        def _():
            q0(c + AHEAD, 0)

        return 0

    lax.fori_loop(0, LEAD, q1, 0)
    lengths.wait()

    def q2(c):
        q_wait(5, dev(2, k), c)
        q_copy(6, dev(2, k), c, partner).start()

    def q3(c):
        q_wait(2, partner, c)
        q_wait(3, dev(-1, 1 - k), c)
        q_wait(4, dev(1, 1 - k), c)
        q_wait(6, dev(2, 1 - k), c)

    lane = lax.broadcasted_iota(jnp.int32, (heads, 128), 1)
    where_t = lax.broadcasted_iota(jnp.int32, (1, sl), 1)
    base = me * sl

    def arrive(g):
        for par in range(2):
            for cp in cache_copies(g, par):
                cp.wait()

    def scores(g, par):
        b = g * 2 + par
        slot = (g % PAIRS) * 2 + par
        qa = qg[:, g, :, pl.ds(par * lat, lat)].reshape(heads, lat)
        qr = qg[:, g, :, pl.ds(2 * lat, 2 * ROPE)].reshape(heads, 2 * ROPE)
        s = jnp.dot(qa, cbuf[slot, pl.ds(0, lat), :], preferred_element_type=F32)
        s = s + jnp.dot(qr, cbuf[slot, pl.ds(lat, 2 * ROPE), :], preferred_element_type=F32)
        return jnp.where(where_t < len_ref[b] - base, s * SCALE, -jnp.inf)

    def finish(g, par, s):
        b = g * 2 + par
        slot = (g % PAIRS) * 2 + par
        m = jnp.maximum(jnp.max(s, axis=1, keepdims=True), jnp.finfo(F32).min)
        p = jnp.exp(s - m)
        l = jnp.sum(p, axis=1, keepdims=True)
        pv = lax.dot_general(p.astype(BF16), cbuf[slot, pl.ds(0, lat), :], (((1,), (1,)), ((), ())),
                             preferred_element_type=F32)
        o = (pv * (1.0 / jnp.maximum(l, 1.0))).astype(BF16)
        od[:, b] = o.reshape(chips, CORES, hl, lat)
        return m + jnp.log(l)

    def attend(c):
        stat = jnp.full((heads, 128), -jnp.inf, F32)
        first = c * half
        arrive(first)
        s0 = scores(first, 0)
        for i in range(half):
            g = first + i
            if i + 1 < half:
                arrive(g + 1)
            s1 = scores(g, 1)
            stat = jnp.where(lane == 2 * i, finish(g, 0, s0), stat)
            if i + 1 < half:
                s0 = scores(g + 1, 0)
            stat = jnp.where(lane == 2 * i + 1, finish(g, 1, s1), stat)

            @pl.when(g + PAIRS < npair)
            def _():
                fetch(g + PAIRS)

        lse = by_owner(stat, n, hl)
        for j in range(n):
            st[j // CORES, c, j % CORES] = lse[j:j + 1]

    def rows(c):
        return pl.ds(c * CHUNK, CHUNK)

    def o_copies(c, kind, src, srcs, dst, dsts, to):
        return [
            pltpu.make_async_remote_copy(
                src_ref=src, dst_ref=dst, send_sem=o_send.at[kind, c], recv_sem=o_recv.at[kind, c],
                device_id={'dcp': to}, device_id_type=MESH),
            pltpu.make_async_remote_copy(
                src_ref=srcs, dst_ref=dsts, send_sem=t_send.at[kind, c], recv_sem=t_recv.at[kind, c],
                device_id={'dcp': to}, device_id_type=MESH),
        ]

    def to_chip(c, kind, head, step):
        return o_copies(c, kind, od.at[head, rows(c)], st.at[head, c], two.at[kind, rows(c)], twos.at[kind, c],
                        dev(step, k))

    def to_partner(c, kind, src, srcs):
        return o_copies(c, kind, src, srcs, inc.at[kind - MINE, rows(c)], ins.at[kind, c], partner)

    def chip(step):
        return (x + step + chips) % chips

    def sends(c):
        way = sign(c)
        relayed = chip(way)
        return (to_chip(c, VIA, chip(2), way)
                + to_partner(c, PASS, od.at[relayed, rows(c), 1 - k], st.at[relayed, c, 1 - k])
                + to_partner(c, MINE, od.at[x, rows(c), 1 - k], st.at[x, c, 1 - k])
                + to_chip(c, DIRECT, chip(-way), -way))

    def share(c, kind):
        return to_partner(c, kind + VIA2, two.at[kind, rows(c), 1 - k], twos.at[kind, c, 1 - k])

    def pass_on(c, kind):
        for cp in to_chip(c, kind, x, 0):
            cp.wait_recv()
        for cp in share(c, kind):
            cp.start()

    def partner_wait(c, kind):
        for cp in to_partner(c, kind, inc.at[kind - MINE, rows(c)], ins.at[kind, c]):
            cp.wait_recv()

    def sum_copies(c):
        return o_copies(c, SUM, rs.at[rows(c)], rss.at[c], lg.at[rows(c)], ins.at[SUM, c], dev(sign(c), k))

    def relay(c):
        for kind in (PASS, VIA2):
            partner_wait(c, kind)
        mine = chip(sign(c))
        w, lse = weights([st[mine, c, k], ins[PASS, c], twos[VIA, c, k], ins[VIA2, c]])
        w = [columns(r) for r in w]
        for i in range(CHUNK):
            b = c * CHUNK + i
            acc = scaled(w[0], i, od[mine, b, k])
            acc = acc + scaled(w[1], i, inc[PASS - MINE, b])
            acc = acc + scaled(w[2], i, two[VIA, b, k])
            acc = acc + scaled(w[3], i, inc[VIA2 - MINE, b])
            rs[b] = acc
        rss[c] = lse
        for cp in sum_copies(c):
            cp.start()

    def merge(c):
        for kind in (MINE, DIRECT2):
            partner_wait(c, kind)
        for cp in sum_copies(c):
            cp.wait_recv()
        w, _ = weights([st[x, c, k], ins[MINE, c], twos[DIRECT, c, k], ins[DIRECT2, c], ins[SUM, c]])
        w = [columns(r) for r in w]
        for i in range(CHUNK):
            b = c * CHUNK + i
            acc = scaled(w[0], i, od[x, b, k])
            acc = acc + scaled(w[1], i, inc[MINE - MINE, b])
            acc = acc + scaled(w[2], i, two[DIRECT, b, k])
            acc = acc + scaled(w[3], i, inc[DIRECT2 - MINE, b])
            acc = acc + scaled(w[4], i, lg[b])
            o_ref[b] = acc.astype(BF16)

    def step(t, _):
        @pl.when(t + LEAD < nc)
        def _():
            q1(t + LEAD, 0)

        @pl.when(t < nc)
        def _():
            @pl.when(t == 0)
            def _():
                q2(0)

            @pl.when(t + 1 < nc)
            def _():
                q2(t + 1)

            q3(t)
            attend(t)
            for cp in sends(t):
                cp.start()

        @pl.when(jnp.logical_and(t >= LAG_V, t < nc + LAG_V))
        def _():
            pass_on(t - LAG_V, VIA)

        @pl.when(jnp.logical_and(t >= LAG_R, t < nc + LAG_R))
        def _():
            relay(t - LAG_R)

        @pl.when(jnp.logical_and(t >= LAG_D, t < nc + LAG_D))
        def _():
            pass_on(t - LAG_D, DIRECT)

        @pl.when(t >= LAG_F)
        def _():
            merge(t - LAG_F)

        return 0

    lax.fori_loop(0, nc + LAG_F, step, 0)

    def drain(c, _):
        for kind in range(7):
            q_copy(kind, me, c, me).wait_send()
        for cp in sends(c) + share(c, VIA) + share(c, DIRECT) + sum_copies(c):
            cp.wait_send()
        return 0

    lax.fori_loop(0, nc, drain, 0)


def solution(mesh):
    n = mesh.shape['dcp']

    def local(q, cache, lengths):
        nb, hl, wd = q.shape
        sl = cache.shape[1]
        lat = wd - ROPE
        nc = nb // CHUNK
        anyspace = pl.BlockSpec(memory_space=pl.ANY)
        dma = pltpu.SemaphoreType.DMA
        return pl.pallas_call(
            functools.partial(kernel, n),
            out_shape=pltpu.VMEM((nb, hl, lat), BF16),
            in_specs=[anyspace, anyspace, anyspace],
            out_specs=pl.BlockSpec(memory_space=pltpu.VMEM),
            scratch_shapes=[
                pltpu.SMEM((nb,), jnp.int32),
                pltpu.VMEM((nb, hl, wd), BF16),
                pltpu.VMEM((n, nb // 2, hl, 2 * wd), BF16),
                pltpu.VMEM((n // CORES, nb, CORES, hl, lat), BF16),
                pltpu.VMEM((n // CORES, nc, CORES, 1, 128), F32),
                pltpu.VMEM((2, nb, CORES, hl, lat), BF16),
                pltpu.VMEM((2, nc, CORES, 1, 128), F32),
                pltpu.VMEM((4, nb, hl, lat), BF16),
                pltpu.VMEM((7, nc, 1, 128), F32),
                pltpu.VMEM((nb, hl, lat), F32),
                pltpu.VMEM((nb, hl, lat), F32),
                pltpu.VMEM((nc, 1, 128), F32),
                pltpu.VMEM((2 * PAIRS, wd + ROPE, sl), BF16),
                dma,
                dma((nc,)),
                dma((2 * PAIRS, 2)),
                dma((7, nc)),
                dma((7, nc)),
                dma((7, nc)),
                dma((7, nc)),
                dma((7, nc)),
                dma((7, nc)),
            ],
            compiler_params=pltpu.CompilerParams(
                collective_id=0, has_side_effects=True, vmem_limit_bytes=56 * 1024 * 1024),
            name='mla_decode',
        )(lengths, q, jnp.swapaxes(cache, 1, 2))

    return jax.shard_map(local, mesh=mesh, in_specs=(P('dp', 'dcp', None), P('dp', 'dcp', None), P('dp')),
                         out_specs=P('dp', 'dcp', None), check_vma=False)
```

```python
import functools

import jax
import jax.numpy as jnp
from jax import lax
from jax.experimental import pallas as pl
from jax.experimental.pallas import tpu as pltpu
from jax.sharding import PartitionSpec as P

ROPE = 64
SCALE = 192 ** -0.5
CORES = 2
CHUNK = 8
PAIRS = 4
AHEAD = 4
LEAD = 3
LAG_V = 2
LAG_R = 3
LAG_D = 4
LAG_F = 6

MESH = pl.DeviceIdType.MESH
F32 = jnp.float32
BF16 = jnp.bfloat16
OWN, PARTNERS, PASSED, OWN2, NEAR2, FAR2 = range(6)
VIA, DIRECT, MINE, PASS, VIA2, DIRECT2, SUM = range(7)


def weights(stats):
    top = functools.reduce(jnp.maximum, stats)
    top = jnp.maximum(top, jnp.finfo(F32).min)
    w = [jnp.exp(t - top) for t in stats]
    total = functools.reduce(jnp.add, w)
    inv = 1.0 / jnp.maximum(total, 1.0)
    return [x * inv for x in w], top + jnp.log(total)


def by_owner(stat, n, hl):
    t = stat.T[:n]
    block = lax.broadcasted_iota(jnp.int32, t.shape, 1) // hl
    row = lax.broadcasted_iota(jnp.int32, t.shape, 0)
    out = t
    for r in range(1, n):
        moved = pltpu.roll(pltpu.roll(t, r * hl, 1), n - r, 0)
        out = jnp.where((block - row + n) % n == r, moved, out)
    return out


def columns(row):
    return jnp.broadcast_to(row, (128, 128)).T


def scaled(w, i, o):
    hl, lat = o.shape
    return jnp.concatenate([w[i * hl:(i + 1) * hl]] * (lat // 128), axis=1) * o.astype(F32)


def kernel(n, len_hbm, q_ref, ct_ref, o_ref, len_ref, qraw, qg, od, st, two, twos, inc, ins, lg, rs, rss, cbuf,
           len_sem, raw_sem, cache_sem, q_send, q_recv, o_send, o_recv, t_send, t_recv):
    chips = n // CORES
    nb, hl, wd = q_ref.shape
    lat = wd - ROPE
    heads = n * hl
    sl = ct_ref.shape[2]
    nc = nb // CHUNK
    half = CHUNK // 2
    npair = nb // 2

    me = lax.axis_index('dcp')
    x = me // CORES
    k = me % CORES
    partner = x * CORES + (1 - k)

    def dev(step, core):
        return ((x + step + chips) % chips) * CORES + core

    def cache_copies(pair, par):
        slot = (pair % PAIRS) * 2 + par
        b = pair * 2 + par
        if par == 0:
            return [pltpu.make_async_copy(ct_ref.at[b], cbuf.at[slot, pl.ds(0, wd)], cache_sem.at[slot, 0])]
        return [
            pltpu.make_async_copy(ct_ref.at[b, pl.ds(0, lat)], cbuf.at[slot, pl.ds(0, lat)], cache_sem.at[slot, 0]),
            pltpu.make_async_copy(ct_ref.at[b, pl.ds(lat, ROPE)], cbuf.at[slot, pl.ds(wd, ROPE)], cache_sem.at[slot, 1]),
        ]

    def fetch(pair):
        for par in range(2):
            for cp in cache_copies(pair, par):
                cp.start()

    barrier = pltpu.get_barrier_semaphore()
    peers = [dev(1, k), dev(-1, k), partner]
    for peer in peers:
        pl.semaphore_signal(barrier, inc=1, device_id={'dcp': peer}, device_id_type=MESH)

    def raw(c):
        part = pl.ds(c * CHUNK, CHUNK)
        return pltpu.make_async_copy(q_ref.at[part], qraw.at[part], raw_sem.at[c])

    for c in range(nc):
        raw(c).start()
    lengths = pltpu.make_async_copy(len_hbm, len_ref, len_sem)
    lengths.start()

    def pack(g, _):
        for par in range(2):
            qg[x, g, k, :, pl.ds(par * lat, lat)] = qraw[2 * g + par, :, pl.ds(0, lat)]
        r0 = qraw[2 * g, :, pl.ds(lat, ROPE)]
        r1 = qraw[2 * g + 1, :, pl.ds(lat, ROPE)]
        qg[x, g, k, :, pl.ds(2 * lat, 2 * ROPE)] = jnp.concatenate([r0, r1], axis=1)
        return 0

    raw(0).wait()
    lax.fori_loop(0, half, pack, 0)
    pl.semaphore_wait(barrier, len(peers))

    def sign(c):
        return 1 - 2 * (c % 2)

    ahead = 2 * k - 1

    def q_copy(kind, chip, core, c, to):
        part = qg.at[chip, pl.ds(c * half, half)] if core is None else qg.at[chip, pl.ds(c * half, half), core]
        return pltpu.make_async_remote_copy(
            src_ref=part, dst_ref=part, send_sem=q_send.at[kind, c], recv_sem=q_recv.at[kind, c],
            device_id={'dcp': to}, device_id_type=MESH)

    def chip(step):
        return (x + step + chips) % chips

    def relays(c):
        return c % 2 == k

    def own(c):
        return q_copy(OWN, x, k, c, dev(ahead, k))

    def own_share(c):
        return q_copy(OWN2, x, k, c, partner)

    def partners(c):
        return q_copy(PARTNERS, x, 1 - k, c, dev(ahead, k))

    def near_share(c):
        return q_copy(NEAR2, chip(-ahead), None, c, partner)

    def passed(c):
        return q_copy(PASSED, chip(-ahead), None, c, dev(ahead, k))

    def far_share(c):
        return q_copy(FAR2, chip(2), None, c, partner)

    def q0(c, _):
        @pl.when(c + 1 < nc)
        def _():
            raw(c + 1).wait()
            lax.fori_loop((c + 1) * half, (c + 2) * half, pack, 0)

        own(c).start()
        own_share(c).start()
        return 0

    def q0b(c):
        q_copy(OWN2, x, 1 - k, c, me).wait_recv()
        partners(c).start()

    for c in range(AHEAD):
        q0(c, 0)
        if c > 0:
            q0b(c - 1)

    for g in range(PAIRS):
        fetch(g)
        cbuf[2 * g, pl.ds(wd, ROPE), :] = jnp.zeros((ROPE, sl), BF16)
        cbuf[2 * g + 1, pl.ds(lat, ROPE), :] = jnp.zeros((ROPE, sl), BF16)

    def q1(c, _):
        q_copy(OWN, chip(-ahead), k, c, me).wait_recv()
        q_copy(PARTNERS, chip(-ahead), 1 - k, c, me).wait_recv()
        near_share(c).start()

        @pl.when(relays(c))
        def _():
            passed(c).start()

        @pl.when(c + AHEAD < nc)
        def _():
            q0(c + AHEAD, 0)

        @pl.when(c + AHEAD - 1 < nc)
        def _():
            q0b(c + AHEAD - 1)

        return 0

    lax.fori_loop(0, LEAD, q1, 0)
    lengths.wait()

    def q2(c):
        @pl.when(relays(c))
        def _():
            q_copy(PASSED, chip(2), None, c, me).wait_recv()
            far_share(c).start()

    def q3(c):
        q_copy(NEAR2, chip(ahead), None, c, me).wait_recv()

        @pl.when(jnp.logical_not(relays(c)))
        def _():
            q_copy(FAR2, chip(2), None, c, me).wait_recv()

    lane = lax.broadcasted_iota(jnp.int32, (heads, 128), 1)
    where_t = lax.broadcasted_iota(jnp.int32, (1, sl), 1)
    base = me * sl

    def arrive(g):
        for par in range(2):
            for cp in cache_copies(g, par):
                cp.wait()

    def scores(g, par):
        b = g * 2 + par
        slot = (g % PAIRS) * 2 + par
        qa = qg[:, g, :, :, pl.ds(par * lat, lat)].reshape(heads, lat)
        qr = qg[:, g, :, :, pl.ds(2 * lat, 2 * ROPE)].reshape(heads, 2 * ROPE)
        s = jnp.dot(qa, cbuf[slot, pl.ds(0, lat), :], preferred_element_type=F32)
        s = s + jnp.dot(qr, cbuf[slot, pl.ds(lat, 2 * ROPE), :], preferred_element_type=F32)
        return jnp.where(where_t < len_ref[b] - base, s * SCALE, -jnp.inf)

    def finish(g, par, s):
        b = g * 2 + par
        slot = (g % PAIRS) * 2 + par
        m = jnp.maximum(jnp.max(s, axis=1, keepdims=True), jnp.finfo(F32).min)
        p = jnp.exp(s - m)
        l = jnp.sum(p, axis=1, keepdims=True)
        pv = lax.dot_general(p.astype(BF16), cbuf[slot, pl.ds(0, lat), :], (((1,), (1,)), ((), ())),
                             preferred_element_type=F32)
        o = (pv * (1.0 / jnp.maximum(l, 1.0))).astype(BF16)
        od[:, b] = o.reshape(chips, CORES, hl, lat)
        return m + jnp.log(l)

    def attend(c):
        stat = jnp.full((heads, 128), -jnp.inf, F32)
        first = c * half
        arrive(first)
        s0 = scores(first, 0)
        for i in range(half):
            g = first + i
            if i + 1 < half:
                arrive(g + 1)
            s1 = scores(g, 1)
            stat = jnp.where(lane == 2 * i, finish(g, 0, s0), stat)
            if i + 1 < half:
                s0 = scores(g + 1, 0)
            stat = jnp.where(lane == 2 * i + 1, finish(g, 1, s1), stat)

            @pl.when(g + PAIRS < npair)
            def _():
                fetch(g + PAIRS)

        lse = by_owner(stat, n, hl)
        for j in range(n):
            st[j // CORES, c, j % CORES] = lse[j:j + 1]

    def rows(c):
        return pl.ds(c * CHUNK, CHUNK)

    def o_copies(c, kind, src, srcs, dst, dsts, to):
        return [
            pltpu.make_async_remote_copy(
                src_ref=src, dst_ref=dst, send_sem=o_send.at[kind, c], recv_sem=o_recv.at[kind, c],
                device_id={'dcp': to}, device_id_type=MESH),
            pltpu.make_async_remote_copy(
                src_ref=srcs, dst_ref=dsts, send_sem=t_send.at[kind, c], recv_sem=t_recv.at[kind, c],
                device_id={'dcp': to}, device_id_type=MESH),
        ]

    def to_chip(c, kind, head, step):
        return o_copies(c, kind, od.at[head, rows(c)], st.at[head, c], two.at[kind, rows(c)], twos.at[kind, c],
                        dev(step, k))

    def to_partner(c, kind, src, srcs):
        return o_copies(c, kind, src, srcs, inc.at[kind - MINE, rows(c)], ins.at[kind, c], partner)

    def sends(c):
        way = sign(c)
        relayed = chip(way)
        return (to_chip(c, VIA, chip(2), way)
                + to_partner(c, PASS, od.at[relayed, rows(c), 1 - k], st.at[relayed, c, 1 - k])
                + to_partner(c, MINE, od.at[x, rows(c), 1 - k], st.at[x, c, 1 - k])
                + to_chip(c, DIRECT, chip(-way), -way))

    def share(c, kind):
        return to_partner(c, kind + VIA2, two.at[kind, rows(c), 1 - k], twos.at[kind, c, 1 - k])

    def pass_on(c, kind):
        for cp in to_chip(c, kind, x, 0):
            cp.wait_recv()
        for cp in share(c, kind):
            cp.start()

    def partner_wait(c, kind):
        for cp in to_partner(c, kind, inc.at[kind - MINE, rows(c)], ins.at[kind, c]):
            cp.wait_recv()

    def sum_copies(c):
        return o_copies(c, SUM, rs.at[rows(c)], rss.at[c], lg.at[rows(c)], ins.at[SUM, c], dev(sign(c), k))

    def relay(c):
        for kind in (PASS, VIA2):
            partner_wait(c, kind)
        mine = chip(sign(c))
        w, lse = weights([st[mine, c, k], ins[PASS, c], twos[VIA, c, k], ins[VIA2, c]])
        w = [columns(r) for r in w]
        for i in range(CHUNK):
            b = c * CHUNK + i
            acc = scaled(w[0], i, od[mine, b, k])
            acc = acc + scaled(w[1], i, inc[PASS - MINE, b])
            acc = acc + scaled(w[2], i, two[VIA, b, k])
            acc = acc + scaled(w[3], i, inc[VIA2 - MINE, b])
            rs[b] = acc
        rss[c] = lse
        for cp in sum_copies(c):
            cp.start()

    def merge(c):
        for kind in (MINE, DIRECT2):
            partner_wait(c, kind)
        for cp in sum_copies(c):
            cp.wait_recv()
        w, _ = weights([st[x, c, k], ins[MINE, c], twos[DIRECT, c, k], ins[DIRECT2, c], ins[SUM, c]])
        w = [columns(r) for r in w]
        for i in range(CHUNK):
            b = c * CHUNK + i
            acc = scaled(w[0], i, od[x, b, k])
            acc = acc + scaled(w[1], i, inc[MINE - MINE, b])
            acc = acc + scaled(w[2], i, two[DIRECT, b, k])
            acc = acc + scaled(w[3], i, inc[DIRECT2 - MINE, b])
            acc = acc + scaled(w[4], i, lg[b])
            o_ref[b] = acc.astype(BF16)

    def step(t, _):
        @pl.when(t + LEAD < nc)
        def _():
            q1(t + LEAD, 0)

        @pl.when(t < nc)
        def _():
            @pl.when(t == 0)
            def _():
                q2(0)

            @pl.when(t + 1 < nc)
            def _():
                q2(t + 1)

            q3(t)
            attend(t)
            for cp in sends(t):
                cp.start()

        @pl.when(jnp.logical_and(t >= LAG_V, t < nc + LAG_V))
        def _():
            pass_on(t - LAG_V, VIA)

        @pl.when(jnp.logical_and(t >= LAG_R, t < nc + LAG_R))
        def _():
            relay(t - LAG_R)

        @pl.when(jnp.logical_and(t >= LAG_D, t < nc + LAG_D))
        def _():
            pass_on(t - LAG_D, DIRECT)

        @pl.when(t >= LAG_F)
        def _():
            merge(t - LAG_F)

        return 0

    lax.fori_loop(0, nc + LAG_F, step, 0)

    def drain(c, _):
        for cp in (own(c), own_share(c), partners(c), near_share(c)):
            cp.wait_send()

        @pl.when(relays(c))
        def _():
            passed(c).wait_send()
            far_share(c).wait_send()

        for cp in sends(c) + share(c, VIA) + share(c, DIRECT) + sum_copies(c):
            cp.wait_send()
        return 0

    lax.fori_loop(0, nc, drain, 0)


def solution(mesh):
    n = mesh.shape['dcp']

    def local(q, cache, lengths):
        nb, hl, wd = q.shape
        sl = cache.shape[1]
        lat = wd - ROPE
        nc = nb // CHUNK
        anyspace = pl.BlockSpec(memory_space=pl.ANY)
        dma = pltpu.SemaphoreType.DMA
        return pl.pallas_call(
            functools.partial(kernel, n),
            out_shape=pltpu.VMEM((nb, hl, lat), BF16),
            in_specs=[anyspace, anyspace, anyspace],
            out_specs=pl.BlockSpec(memory_space=pltpu.VMEM),
            scratch_shapes=[
                pltpu.SMEM((nb,), jnp.int32),
                pltpu.VMEM((nb, hl, wd), BF16),
                pltpu.VMEM((n // CORES, nb // 2, CORES, hl, 2 * wd), BF16),
                pltpu.VMEM((n // CORES, nb, CORES, hl, lat), BF16),
                pltpu.VMEM((n // CORES, nc, CORES, 1, 128), F32),
                pltpu.VMEM((2, nb, CORES, hl, lat), BF16),
                pltpu.VMEM((2, nc, CORES, 1, 128), F32),
                pltpu.VMEM((4, nb, hl, lat), BF16),
                pltpu.VMEM((7, nc, 1, 128), F32),
                pltpu.VMEM((nb, hl, lat), F32),
                pltpu.VMEM((nb, hl, lat), F32),
                pltpu.VMEM((nc, 1, 128), F32),
                pltpu.VMEM((2 * PAIRS, wd + ROPE, sl), BF16),
                dma,
                dma((nc,)),
                dma((2 * PAIRS, 2)),
                dma((7, nc)),
                dma((7, nc)),
                dma((7, nc)),
                dma((7, nc)),
                dma((7, nc)),
                dma((7, nc)),
            ],
            compiler_params=pltpu.CompilerParams(
                collective_id=0, has_side_effects=True, vmem_limit_bytes=56 * 1024 * 1024),
            name='mla_decode',
        )(lengths, q, jnp.swapaxes(cache, 1, 2))

    return jax.shard_map(local, mesh=mesh, in_specs=(P('dp', 'dcp', None), P('dp', 'dcp', None), P('dp')),
                         out_specs=P('dp', 'dcp', None), check_vma=False)
```

```python
import functools

import jax
import jax.numpy as jnp
from jax import lax
from jax.experimental import pallas as pl
from jax.experimental.pallas import tpu as pltpu
from jax.sharding import PartitionSpec as P

ROPE = 64
SCALE = 192 ** -0.5
CORES = 2
CHUNK = 8
PAIRS = 4
AHEAD = 4
LEAD = 3
LAG_V = 2
LAG_R = 3
LAG_D = 4
LAG_F = 6

MESH = pl.DeviceIdType.MESH
F32 = jnp.float32
BF16 = jnp.bfloat16
VIA, DIRECT, MINE, PASS, VIA2, DIRECT2, SUM = range(7)
FOR_RELAY, FOR_MERGE = 2, 3
TWO, ONE, TOTAL, ROWS = range(4)
NEAR, FAR, MATE = range(3)


def weights(stats):
    top = functools.reduce(jnp.maximum, stats)
    top = jnp.maximum(top, jnp.finfo(F32).min)
    w = [jnp.exp(t - top) for t in stats]
    total = functools.reduce(jnp.add, w)
    inv = 1.0 / jnp.maximum(total, 1.0)
    return [x * inv for x in w], top + jnp.log(total)


def by_owner(stat, n, hl):
    t = stat.T[:n]
    block = lax.broadcasted_iota(jnp.int32, t.shape, 1) // hl
    row = lax.broadcasted_iota(jnp.int32, t.shape, 0)
    out = t
    for r in range(1, n):
        moved = pltpu.roll(pltpu.roll(t, r * hl, 1), n - r, 0)
        out = jnp.where((block - row + n) % n == r, moved, out)
    return out


def columns(row):
    return jnp.broadcast_to(row, (128, 128)).T


def scaled(w, i, o):
    hl, lat = o.shape
    return jnp.concatenate([w[i * hl:(i + 1) * hl]] * (lat // 128), axis=1) * o.astype(F32)


def kernel(n, len_hbm, q_ref, ct_ref, o_ref, len_ref, qraw, qg, od, st, two, twos, inc, ins, lg, rs, rss, cbuf, tally,
           len_sem, raw_sem, cache_sem, q_send, q_recv, o_send, o_recv):
    chips = n // CORES
    nb, hl, wd = q_ref.shape
    lat = wd - ROPE
    heads = n * hl
    sl = ct_ref.shape[2]
    nc = nb // CHUNK
    half = CHUNK // 2
    npair = nb // 2

    me = lax.axis_index('dcp')
    x = me // CORES
    k = me % CORES
    partner = x * CORES + (1 - k)

    def dev(step, core):
        return ((x + step + chips) % chips) * CORES + core

    def wait_bytes(like, sem):
        pltpu.make_async_copy(like, like, sem).wait()

    def cache_copies(pair, par):
        slot = (pair % PAIRS) * 2 + par
        b = pair * 2 + par
        if par == 0:
            return [pltpu.make_async_copy(ct_ref.at[b], cbuf.at[slot, pl.ds(0, wd)], cache_sem.at[slot])]
        return [
            pltpu.make_async_copy(ct_ref.at[b, pl.ds(0, lat)], cbuf.at[slot, pl.ds(0, lat)], cache_sem.at[slot]),
            pltpu.make_async_copy(ct_ref.at[b, pl.ds(lat, ROPE)], cbuf.at[slot, pl.ds(wd, ROPE)], cache_sem.at[slot]),
        ]

    def fetch(pair):
        for par in range(2):
            for cp in cache_copies(pair, par):
                cp.start()

    barrier = pltpu.get_barrier_semaphore()
    peers = [dev(1, k), dev(-1, k), partner]
    for peer in peers:
        pl.semaphore_signal(barrier, inc=1, device_id={'dcp': peer}, device_id_type=MESH)

    def raw(i):
        part = pl.ds(0, CHUNK) if i == 0 else pl.ds(CHUNK, nb - CHUNK)
        return pltpu.make_async_copy(q_ref.at[part], qraw.at[part], raw_sem.at[i])

    for i in range(2):
        raw(i).start()
    lengths = pltpu.make_async_copy(len_hbm, len_ref, len_sem)
    lengths.start()

    def pack(g, _):
        for par in range(2):
            qg[me, g, :, pl.ds(par * lat, lat)] = qraw[2 * g + par, :, pl.ds(0, lat)]
        r0 = qraw[2 * g, :, pl.ds(lat, ROPE)]
        r1 = qraw[2 * g + 1, :, pl.ds(lat, ROPE)]
        qg[me, g, :, pl.ds(2 * lat, 2 * ROPE)] = jnp.concatenate([r0, r1], axis=1)
        return 0

    raw(0).wait()
    lax.fori_loop(0, half, pack, 0)
    pl.semaphore_wait(barrier, len(peers))

    def q_copy(kind, src, c, to):
        part = qg.at[src, pl.ds(c * half, half)]
        return pltpu.make_async_remote_copy(
            src_ref=part, dst_ref=part, send_sem=q_send, recv_sem=q_recv.at[kind, c],
            device_id={'dcp': to}, device_id_type=MESH)

    def q_wait(kind, count, c):
        wait_bytes(qg.at[pl.ds(0, count), pl.ds(c * half, half)], q_recv.at[kind, c])

    def sign(c):
        return 1 - 2 * (c % 2)

    def q0(c, _):
        @pl.when(c + 1 < nc)
        def _():
            @pl.when(c == 0)
            def _():
                raw(1).wait()

            lax.fori_loop((c + 1) * half, (c + 2) * half, pack, 0)

        q_copy(NEAR, me, c, dev(1, k)).start()
        q_copy(NEAR, me, c, dev(-1, k)).start()
        q_copy(MATE, me, c, partner).start()
        return 0

    lax.fori_loop(0, AHEAD, q0, 0)

    for g in range(PAIRS):
        fetch(g)
        cbuf[2 * g, pl.ds(wd, ROPE), :] = jnp.zeros((ROPE, sl), BF16)
        cbuf[2 * g + 1, pl.ds(lat, ROPE), :] = jnp.zeros((ROPE, sl), BF16)

    def q1(c, _):
        way = -sign(c)
        q_wait(NEAR, 2, c)
        q_copy(FAR, dev(-way, k), c, dev(way, k)).start()
        q_copy(MATE, dev(-1, k), c, partner).start()
        q_copy(MATE, dev(1, k), c, partner).start()

        @pl.when(c + AHEAD < nc)
        def _():
            q0(c + AHEAD, 0)

        return 0

    lax.fori_loop(0, LEAD, q1, 0)
    lengths.wait()

    def q2(c):
        q_wait(FAR, 1, c)
        q_copy(MATE, dev(2, k), c, partner).start()

    def q3(c):
        q_wait(MATE, chips, c)

    lane = lax.broadcasted_iota(jnp.int32, (heads, 128), 1)
    where_t = lax.broadcasted_iota(jnp.int32, (1, sl), 1)
    base = me * sl

    def arrive(g):
        for par in range(2):
            slot = (g % PAIRS) * 2 + par
            wait_bytes(cbuf.at[slot, pl.ds(0, wd)], cache_sem.at[slot])

    def scores(g, par):
        b = g * 2 + par
        slot = (g % PAIRS) * 2 + par
        qa = qg[:, g, :, pl.ds(par * lat, lat)].reshape(heads, lat)
        qr = qg[:, g, :, pl.ds(2 * lat, 2 * ROPE)].reshape(heads, 2 * ROPE)
        s = jnp.dot(qa, cbuf[slot, pl.ds(0, lat), :], preferred_element_type=F32)
        s = s + jnp.dot(qr, cbuf[slot, pl.ds(lat, 2 * ROPE), :], preferred_element_type=F32)
        return jnp.where(where_t < len_ref[b] - base, s * SCALE, -jnp.inf)

    def finish(g, par, s):
        b = g * 2 + par
        slot = (g % PAIRS) * 2 + par
        m = jnp.maximum(jnp.max(s, axis=1, keepdims=True), jnp.finfo(F32).min)
        p = jnp.exp(s - m)
        l = jnp.sum(p, axis=1, keepdims=True)
        pv = lax.dot_general(p.astype(BF16), cbuf[slot, pl.ds(0, lat), :], (((1,), (1,)), ((), ())),
                             preferred_element_type=F32)
        o = (pv * (1.0 / jnp.maximum(l, 1.0))).astype(BF16)
        od[:, b] = o.reshape(chips, CORES, hl, lat)
        return m + jnp.log(l)

    def attend(c):
        stat = jnp.full((heads, 128), -jnp.inf, F32)
        first = c * half
        arrive(first)
        s0 = scores(first, 0)
        for i in range(half):
            g = first + i
            if i + 1 < half:
                arrive(g + 1)
            s1 = scores(g, 1)
            stat = jnp.where(lane == 2 * i, finish(g, 0, s0), stat)
            if i + 1 < half:
                s0 = scores(g + 1, 0)
            stat = jnp.where(lane == 2 * i + 1, finish(g, 1, s1), stat)

            @pl.when(g + PAIRS < npair)
            def _():
                fetch(g + PAIRS)

        lse = by_owner(stat, n, hl)
        for j in range(n):
            st[j // CORES, c, j % CORES] = lse[j:j + 1]

    def rows(c):
        return pl.ds(c * CHUNK, CHUNK)

    row = 128 * 4
    block = CHUNK * hl * lat * 2 // row

    def o_copies(c, send, recv, src, srcs, dst, dsts, to):
        return [
            pltpu.make_async_remote_copy(
                src_ref=src, dst_ref=dst, send_sem=o_send.at[send], recv_sem=o_recv.at[recv, c],
                device_id={'dcp': to}, device_id_type=MESH),
            pltpu.make_async_remote_copy(
                src_ref=srcs, dst_ref=dsts, send_sem=o_send.at[ROWS], recv_sem=o_recv.at[recv, c],
                device_id={'dcp': to}, device_id_type=MESH),
        ]

    def o_wait(c, recv, count):
        wait_bytes(tally.at[pl.ds(0, count)], o_recv.at[recv, c])

    def to_chip(c, kind, head, step):
        return o_copies(c, TWO, kind, od.at[head, rows(c)], st.at[head, c], two.at[kind, rows(c)], twos.at[kind, c],
                        dev(step, k))

    def to_partner(c, kind, src, srcs):
        recv = FOR_RELAY if kind in (PASS, VIA2) else FOR_MERGE
        return o_copies(c, ONE, recv, src, srcs, inc.at[kind - MINE, rows(c)], ins.at[kind, c], partner)

    def chip(step):
        return (x + step + chips) % chips

    def sends(c):
        way = sign(c)
        relayed = chip(way)
        return (to_chip(c, VIA, chip(2), way)
                + to_partner(c, PASS, od.at[relayed, rows(c), 1 - k], st.at[relayed, c, 1 - k])
                + to_partner(c, MINE, od.at[x, rows(c), 1 - k], st.at[x, c, 1 - k])
                + to_chip(c, DIRECT, chip(-way), -way))

    def share(c, kind):
        return to_partner(c, kind + VIA2, two.at[kind, rows(c), 1 - k], twos.at[kind, c, 1 - k])

    def pass_on(c, kind):
        o_wait(c, kind, 2 * (block + 1))
        for cp in share(c, kind):
            cp.start()

    def sum_copies(c):
        return o_copies(c, TOTAL, FOR_MERGE, rs.at[rows(c)], rss.at[c], lg.at[rows(c)], ins.at[SUM, c], dev(sign(c), k))

    def relay(c):
        o_wait(c, FOR_RELAY, 2 * (block + 1))
        mine = chip(sign(c))
        w, lse = weights([st[mine, c, k], ins[PASS, c], twos[VIA, c, k], ins[VIA2, c]])
        w = [columns(r) for r in w]
        for i in range(CHUNK):
            b = c * CHUNK + i
            acc = scaled(w[0], i, od[mine, b, k])
            acc = acc + scaled(w[1], i, inc[PASS - MINE, b])
            acc = acc + scaled(w[2], i, two[VIA, b, k])
            acc = acc + scaled(w[3], i, inc[VIA2 - MINE, b])
            rs[b] = acc
        rss[c] = lse
        for cp in sum_copies(c):
            cp.start()

    def merge(c):
        o_wait(c, FOR_MERGE, 4 * block + 3)
        w, _ = weights([st[x, c, k], ins[MINE, c], twos[DIRECT, c, k], ins[DIRECT2, c], ins[SUM, c]])
        w = [columns(r) for r in w]
        for i in range(CHUNK):
            b = c * CHUNK + i
            acc = scaled(w[0], i, od[x, b, k])
            acc = acc + scaled(w[1], i, inc[MINE - MINE, b])
            acc = acc + scaled(w[2], i, two[DIRECT, b, k])
            acc = acc + scaled(w[3], i, inc[DIRECT2 - MINE, b])
            acc = acc + scaled(w[4], i, lg[b])
            o_ref[b] = acc.astype(BF16)

    def step(t, _):
        @pl.when(t + LEAD < nc)
        def _():
            q1(t + LEAD, 0)

        @pl.when(t < nc)
        def _():
            @pl.when(t == 0)
            def _():
                q2(0)

            @pl.when(t + 1 < nc)
            def _():
                q2(t + 1)

            q3(t)
            attend(t)
            for cp in sends(t):
                cp.start()

        @pl.when(jnp.logical_and(t >= LAG_V, t < nc + LAG_V))
        def _():
            pass_on(t - LAG_V, VIA)

        @pl.when(jnp.logical_and(t >= LAG_R, t < nc + LAG_R))
        def _():
            relay(t - LAG_R)

        @pl.when(jnp.logical_and(t >= LAG_D, t < nc + LAG_D))
        def _():
            pass_on(t - LAG_D, DIRECT)

        @pl.when(t >= LAG_F)
        def _():
            merge(t - LAG_F)

        return 0

    lax.fori_loop(0, nc + LAG_F, step, 0)

    wait_bytes(qg.at[pl.ds(0, n - 1)], q_send)
    wait_bytes(two, o_send.at[TWO])
    wait_bytes(inc, o_send.at[ONE])
    wait_bytes(lg, o_send.at[TOTAL])
    wait_bytes(tally.at[pl.ds(0, nc * (2 * CORES + 5))], o_send.at[ROWS])


def solution(mesh):
    n = mesh.shape['dcp']

    def local(q, cache, lengths):
        nb, hl, wd = q.shape
        sl = cache.shape[1]
        lat = wd - ROPE
        nc = nb // CHUNK
        anyspace = pl.BlockSpec(memory_space=pl.ANY)
        dma = pltpu.SemaphoreType.DMA
        return pl.pallas_call(
            functools.partial(kernel, n),
            out_shape=pltpu.VMEM((nb, hl, lat), BF16),
            in_specs=[anyspace, anyspace, anyspace],
            out_specs=pl.BlockSpec(memory_space=pltpu.VMEM),
            scratch_shapes=[
                pltpu.SMEM((nb,), jnp.int32),
                pltpu.VMEM((nb, hl, wd), BF16),
                pltpu.VMEM((n, nb // 2, hl, 2 * wd), BF16),
                pltpu.VMEM((n // CORES, nb, CORES, hl, lat), BF16),
                pltpu.VMEM((n // CORES, nc, CORES, 1, 128), F32),
                pltpu.VMEM((2, nb, CORES, hl, lat), BF16),
                pltpu.VMEM((2, nc, CORES, 1, 128), F32),
                pltpu.VMEM((4, nb, hl, lat), BF16),
                pltpu.VMEM((7, nc, 1, 128), F32),
                pltpu.VMEM((nb, hl, lat), F32),
                pltpu.VMEM((nb, hl, lat), F32),
                pltpu.VMEM((nc, 1, 128), F32),
                pltpu.VMEM((2 * PAIRS, wd + ROPE, sl), BF16),
                pltpu.VMEM((4 * CHUNK * hl * lat // 256 + 3, 1, 128), F32),
                dma,
                dma((2,)),
                dma((2 * PAIRS,)),
                dma,
                dma((3, nc)),
                dma((4,)),
                dma((4, nc)),
            ],
            compiler_params=pltpu.CompilerParams(
                collective_id=0, has_side_effects=True, vmem_limit_bytes=56 * 1024 * 1024),
            name='mla_decode',
        )(lengths, q, jnp.swapaxes(cache, 1, 2))

    return jax.shard_map(local, mesh=mesh, in_specs=(P('dp', 'dcp', None), P('dp', 'dcp', None), P('dp')),
                         out_specs=P('dp', 'dcp', None), check_vma=False)
```

```python
import functools

import jax
import jax.numpy as jnp
from jax import lax
from jax.experimental import pallas as pl
from jax.experimental.pallas import tpu as pltpu
from jax.sharding import PartitionSpec as P

ROPE = 64
SCALE = 192 ** -0.5
CORES = 2
CHUNK = 8
PAIRS = 4
AHEAD = 4
LEAD = 3
LAG_V = 2
LAG_R = 3
LAG_D = 4
LAG_F = 6

MESH = pl.DeviceIdType.MESH
F32 = jnp.float32
BF16 = jnp.bfloat16
VIA, DIRECT, MINE, PASS, VIA2, DIRECT2, SUM = range(7)
FOR_RELAY, FOR_MERGE = 2, 3
TWO, ONE, TOTAL, ROWS = range(4)
NEAR, FAR, MATE = range(3)


def weights(stats):
    top = functools.reduce(jnp.maximum, stats)
    top = jnp.maximum(top, jnp.finfo(F32).min)
    w = [jnp.exp(t - top) for t in stats]
    total = functools.reduce(jnp.add, w)
    inv = 1.0 / jnp.maximum(total, 1.0)
    return [x * inv for x in w], top + jnp.log(total)


def by_owner(stat, n, hl):
    t = stat.T[:n]
    block = lax.broadcasted_iota(jnp.int32, t.shape, 1) // hl
    row = lax.broadcasted_iota(jnp.int32, t.shape, 0)
    out = t
    for r in range(1, n):
        moved = pltpu.roll(pltpu.roll(t, r * hl, 1), n - r, 0)
        out = jnp.where((block - row + n) % n == r, moved, out)
    return out


def columns(row):
    return jnp.broadcast_to(row, (128, 128)).T


def scaled(w, i, o):
    hl, lat = o.shape
    return jnp.concatenate([w[i * hl:(i + 1) * hl]] * (lat // 128), axis=1) * o.astype(F32)


def kernel(n, len_hbm, q_ref, ct_ref, o_ref, len_ref, qraw, qg, od, st, two, twos, inc, ins, lg, rs, rss, cbuf, tally,
           len_sem, raw_sem, cache_sem, q_send, q_recv, o_send, o_recv):
    chips = n // CORES
    nb, hl, wd = q_ref.shape
    lat = wd - ROPE
    heads = n * hl
    sl = ct_ref.shape[2]
    nc = nb // CHUNK
    half = CHUNK // 2
    npair = nb // 2

    me = lax.axis_index('dcp')
    x = me // CORES
    k = me % CORES
    partner = x * CORES + (1 - k)

    def dev(step, core):
        return ((x + step + chips) % chips) * CORES + core

    def wait_bytes(like, sem):
        pltpu.make_async_copy(like, like, sem).wait()

    def cache_copies(pair, par):
        slot = (pair % PAIRS) * 2 + par
        b = pair * 2 + par
        if par == 0:
            return [pltpu.make_async_copy(ct_ref.at[b], cbuf.at[slot, pl.ds(0, wd)], cache_sem.at[pair % PAIRS])]
        return [
            pltpu.make_async_copy(ct_ref.at[b, pl.ds(0, lat)], cbuf.at[slot, pl.ds(0, lat)], cache_sem.at[pair % PAIRS]),
            pltpu.make_async_copy(ct_ref.at[b, pl.ds(lat, ROPE)], cbuf.at[slot, pl.ds(wd, ROPE)], cache_sem.at[pair % PAIRS]),
        ]

    def fetch(pair):
        for par in range(2):
            for cp in cache_copies(pair, par):
                cp.start()

    barrier = pltpu.get_barrier_semaphore()
    peers = [dev(1, k), dev(-1, k), partner]
    for peer in peers:
        pl.semaphore_signal(barrier, inc=1, device_id={'dcp': peer}, device_id_type=MESH)

    def raw(i):
        part = pl.ds(i * CHUNK, CHUNK if i < 2 else nb - 2 * CHUNK)
        return pltpu.make_async_copy(q_ref.at[part], qraw.at[part], raw_sem.at[i])

    for i in range(3):
        raw(i).start()
    lengths = pltpu.make_async_copy(len_hbm, len_ref, len_sem)
    lengths.start()

    def pack(g, _):
        for par in range(2):
            qg[me, g, :, pl.ds(par * lat, lat)] = qraw[2 * g + par, :, pl.ds(0, lat)]
        r0 = qraw[2 * g, :, pl.ds(lat, ROPE)]
        r1 = qraw[2 * g + 1, :, pl.ds(lat, ROPE)]
        qg[me, g, :, pl.ds(2 * lat, 2 * ROPE)] = jnp.concatenate([r0, r1], axis=1)
        return 0

    raw(0).wait()
    lax.fori_loop(0, half, pack, 0)
    pl.semaphore_wait(barrier, len(peers))

    def q_copy(kind, src, c, to):
        part = qg.at[src, pl.ds(c * half, half)]
        return pltpu.make_async_remote_copy(
            src_ref=part, dst_ref=part, send_sem=q_send, recv_sem=q_recv.at[kind, c],
            device_id={'dcp': to}, device_id_type=MESH)

    def q_wait(kind, count, c):
        wait_bytes(qg.at[pl.ds(0, count), pl.ds(c * half, half)], q_recv.at[kind, c])

    def sign(c):
        return 1 - 2 * (c % 2)

    def q0(c, _):
        @pl.when(c + 1 < nc)
        def _():
            for i in (1, 2):
                @pl.when(c == i - 1)
                def _():
                    raw(i).wait()

            lax.fori_loop((c + 1) * half, (c + 2) * half, pack, 0)

        q_copy(NEAR, me, c, dev(1, k)).start()
        q_copy(NEAR, me, c, dev(-1, k)).start()
        q_copy(MATE, me, c, partner).start()
        return 0

    lax.fori_loop(0, AHEAD, q0, 0)

    for g in range(PAIRS):
        fetch(g)
        cbuf[2 * g, pl.ds(wd, ROPE), :] = jnp.zeros((ROPE, sl), BF16)
        cbuf[2 * g + 1, pl.ds(lat, ROPE), :] = jnp.zeros((ROPE, sl), BF16)

    def q1(c, _):
        way = -sign(c)
        q_wait(NEAR, 2, c)
        q_copy(FAR, dev(-way, k), c, dev(way, k)).start()
        q_copy(MATE, dev(-1, k), c, partner).start()
        q_copy(MATE, dev(1, k), c, partner).start()

        @pl.when(c + AHEAD < nc)
        def _():
            q0(c + AHEAD, 0)

        return 0

    lax.fori_loop(0, LEAD, q1, 0)
    lengths.wait()

    def q2(c):
        q_wait(FAR, 1, c)
        q_copy(MATE, dev(2, k), c, partner).start()

    def q3(c):
        q_wait(MATE, chips, c)

    lane = lax.broadcasted_iota(jnp.int32, (heads, 128), 1)
    where_t = lax.broadcasted_iota(jnp.int32, (1, sl), 1)
    base = me * sl

    def arrive(g):
        wait_bytes(cbuf.at[pl.ds((g % PAIRS) * 2, 2), pl.ds(0, wd)], cache_sem.at[g % PAIRS])

    def scores(g, par):
        b = g * 2 + par
        slot = (g % PAIRS) * 2 + par
        qa = qg[:, g, :, pl.ds(par * lat, lat)].reshape(heads, lat)
        qr = qg[:, g, :, pl.ds(2 * lat, 2 * ROPE)].reshape(heads, 2 * ROPE)
        s = jnp.dot(qa, cbuf[slot, pl.ds(0, lat), :], preferred_element_type=F32)
        s = s + jnp.dot(qr, cbuf[slot, pl.ds(lat, 2 * ROPE), :], preferred_element_type=F32)
        return jnp.where(where_t < len_ref[b] - base, s * SCALE, -jnp.inf)

    def finish(g, par, s):
        b = g * 2 + par
        slot = (g % PAIRS) * 2 + par
        m = jnp.maximum(jnp.max(s, axis=1, keepdims=True), jnp.finfo(F32).min)
        p = jnp.exp(s - m)
        l = jnp.sum(p, axis=1, keepdims=True)
        pv = lax.dot_general(p.astype(BF16), cbuf[slot, pl.ds(0, lat), :], (((1,), (1,)), ((), ())),
                             preferred_element_type=F32)
        o = (pv * (1.0 / jnp.maximum(l, 1.0))).astype(BF16)
        od[:, b] = o.reshape(chips, CORES, hl, lat)
        return m + jnp.log(l)

    def attend(c):
        stat = jnp.full((heads, 128), -jnp.inf, F32)
        first = c * half
        arrive(first)
        s0 = scores(first, 0)
        for i in range(half):
            g = first + i
            if i + 1 < half:
                arrive(g + 1)
            s1 = scores(g, 1)
            stat = jnp.where(lane == 2 * i, finish(g, 0, s0), stat)
            if i + 1 < half:
                s0 = scores(g + 1, 0)
            stat = jnp.where(lane == 2 * i + 1, finish(g, 1, s1), stat)

            @pl.when(g + PAIRS < npair)
            def _():
                fetch(g + PAIRS)

        lse = by_owner(stat, n, hl)
        for j in range(n):
            st[j // CORES, c, j % CORES] = lse[j:j + 1]

    def rows(c):
        return pl.ds(c * CHUNK, CHUNK)

    row = 128 * 4
    block = CHUNK * hl * lat * 2 // row

    def arrived(recv, c):
        return q_recv.at[{FOR_RELAY: FAR, FOR_MERGE: NEAR}[recv], c] if recv >= FOR_RELAY else o_recv.at[recv, c]

    def o_copies(c, send, recv, src, srcs, dst, dsts, to):
        return [
            pltpu.make_async_remote_copy(
                src_ref=src, dst_ref=dst, send_sem=o_send.at[send], recv_sem=arrived(recv, c),
                device_id={'dcp': to}, device_id_type=MESH),
            pltpu.make_async_remote_copy(
                src_ref=srcs, dst_ref=dsts, send_sem=o_send.at[ROWS], recv_sem=arrived(recv, c),
                device_id={'dcp': to}, device_id_type=MESH),
        ]

    def o_wait(c, recv, count):
        wait_bytes(tally.at[pl.ds(0, count)], arrived(recv, c))

    def to_chip(c, kind, head, step):
        return o_copies(c, TWO, kind, od.at[head, rows(c)], st.at[head, c], two.at[kind, rows(c)], twos.at[kind, c],
                        dev(step, k))

    def to_partner(c, kind, src, srcs):
        recv = FOR_RELAY if kind in (PASS, VIA2) else FOR_MERGE
        return o_copies(c, ONE, recv, src, srcs, inc.at[kind - MINE, rows(c)], ins.at[kind, c], partner)

    def chip(step):
        return (x + step + chips) % chips

    def sends(c):
        way = sign(c)
        relayed = chip(way)
        return (to_chip(c, VIA, chip(2), way)
                + to_partner(c, PASS, od.at[relayed, rows(c), 1 - k], st.at[relayed, c, 1 - k])
                + to_partner(c, MINE, od.at[x, rows(c), 1 - k], st.at[x, c, 1 - k])
                + to_chip(c, DIRECT, chip(-way), -way))

    def share(c, kind):
        return to_partner(c, kind + VIA2, two.at[kind, rows(c), 1 - k], twos.at[kind, c, 1 - k])

    def pass_on(c, kind):
        o_wait(c, kind, 2 * (block + 1))
        for cp in share(c, kind):
            cp.start()

    def sum_copies(c):
        return o_copies(c, TOTAL, FOR_MERGE, rs.at[rows(c)], rss.at[c], lg.at[rows(c)], ins.at[SUM, c], dev(sign(c), k))

    def relay(c):
        o_wait(c, FOR_RELAY, 2 * (block + 1))
        mine = chip(sign(c))
        w, lse = weights([st[mine, c, k], ins[PASS, c], twos[VIA, c, k], ins[VIA2, c]])
        w = [columns(r) for r in w]
        for i in range(CHUNK):
            b = c * CHUNK + i
            acc = scaled(w[0], i, od[mine, b, k])
            acc = acc + scaled(w[1], i, inc[PASS - MINE, b])
            acc = acc + scaled(w[2], i, two[VIA, b, k])
            acc = acc + scaled(w[3], i, inc[VIA2 - MINE, b])
            rs[b] = acc
        rss[c] = lse
        for cp in sum_copies(c):
            cp.start()

    def merge(c):
        o_wait(c, FOR_MERGE, 4 * block + 3)
        w, _ = weights([st[x, c, k], ins[MINE, c], twos[DIRECT, c, k], ins[DIRECT2, c], ins[SUM, c]])
        w = [columns(r) for r in w]
        for i in range(CHUNK):
            b = c * CHUNK + i
            acc = scaled(w[0], i, od[x, b, k])
            acc = acc + scaled(w[1], i, inc[MINE - MINE, b])
            acc = acc + scaled(w[2], i, two[DIRECT, b, k])
            acc = acc + scaled(w[3], i, inc[DIRECT2 - MINE, b])
            acc = acc + scaled(w[4], i, lg[b])
            o_ref[b] = acc.astype(BF16)

    def step(t, _):
        @pl.when(t + LEAD < nc)
        def _():
            q1(t + LEAD, 0)

        @pl.when(t < nc)
        def _():
            @pl.when(t == 0)
            def _():
                q2(0)

            @pl.when(t + 1 < nc)
            def _():
                q2(t + 1)

            q3(t)
            attend(t)
            for cp in sends(t):
                cp.start()

        @pl.when(jnp.logical_and(t >= LAG_V, t < nc + LAG_V))
        def _():
            pass_on(t - LAG_V, VIA)

        @pl.when(jnp.logical_and(t >= LAG_R, t < nc + LAG_R))
        def _():
            relay(t - LAG_R)

        @pl.when(jnp.logical_and(t >= LAG_D, t < nc + LAG_D))
        def _():
            pass_on(t - LAG_D, DIRECT)

        @pl.when(t >= LAG_F)
        def _():
            merge(t - LAG_F)

        return 0

    lax.fori_loop(0, nc + LAG_F, step, 0)

    wait_bytes(qg.at[pl.ds(0, n - 1)], q_send)
    wait_bytes(two, o_send.at[TWO])
    wait_bytes(inc, o_send.at[ONE])
    wait_bytes(lg, o_send.at[TOTAL])
    wait_bytes(tally.at[pl.ds(0, nc * (2 * CORES + 5))], o_send.at[ROWS])


def solution(mesh):
    n = mesh.shape['dcp']

    def local(q, cache, lengths):
        nb, hl, wd = q.shape
        sl = cache.shape[1]
        lat = wd - ROPE
        nc = nb // CHUNK
        anyspace = pl.BlockSpec(memory_space=pl.ANY)
        dma = pltpu.SemaphoreType.DMA
        return pl.pallas_call(
            functools.partial(kernel, n),
            out_shape=pltpu.VMEM((nb, hl, lat), BF16),
            in_specs=[anyspace, anyspace, anyspace],
            out_specs=pl.BlockSpec(memory_space=pltpu.VMEM),
            scratch_shapes=[
                pltpu.SMEM((nb,), jnp.int32),
                pltpu.VMEM((nb, hl, wd), BF16),
                pltpu.VMEM((n, nb // 2, hl, 2 * wd), BF16),
                pltpu.VMEM((n // CORES, nb, CORES, hl, lat), BF16),
                pltpu.VMEM((n // CORES, nc, CORES, 1, 128), F32),
                pltpu.VMEM((2, nb, CORES, hl, lat), BF16),
                pltpu.VMEM((2, nc, CORES, 1, 128), F32),
                pltpu.VMEM((4, nb, hl, lat), BF16),
                pltpu.VMEM((7, nc, 1, 128), F32),
                pltpu.VMEM((nb, hl, lat), F32),
                pltpu.VMEM((nb, hl, lat), F32),
                pltpu.VMEM((nc, 1, 128), F32),
                pltpu.VMEM((2 * PAIRS, wd + ROPE, sl), BF16),
                pltpu.VMEM((4 * CHUNK * hl * lat // 256 + 3, 1, 128), F32),
                dma,
                dma((3,)),
                dma((PAIRS,)),
                dma,
                dma((3, nc)),
                dma((4,)),
                dma((2, nc)),
            ],
            compiler_params=pltpu.CompilerParams(
                collective_id=0, has_side_effects=True, vmem_limit_bytes=56 * 1024 * 1024),
            name='mla_decode',
        )(lengths, q, jnp.swapaxes(cache, 1, 2))

    return jax.shard_map(local, mesh=mesh, in_specs=(P('dp', 'dcp', None), P('dp', 'dcp', None), P('dp')),
                         out_specs=P('dp', 'dcp', None), check_vma=False)
```

```python
import functools

import jax
import jax.numpy as jnp
from jax import lax
from jax.experimental import pallas as pl
from jax.experimental.pallas import tpu as pltpu
from jax.sharding import PartitionSpec as P

ROPE = 64
SCALE = 192 ** -0.5
CORES = 2
CHUNK = 8
PAIRS = 4
AHEAD = 4
LEAD = 3
LAG_V = 2
LAG_R = 3
LAG_F = 6

MESH = pl.DeviceIdType.MESH
F32 = jnp.float32
BF16 = jnp.bfloat16
VIA, DIRECT, MINE, PASS, VIA2, DIRECT2, SUM = range(7)
FOR_RELAY, FOR_MERGE = 2, 3
TWO, ONE, TOTAL, ROWS = range(4)
NEAR, FAR, MATE = range(3)


def weights(stats):
    top = functools.reduce(jnp.maximum, stats)
    top = jnp.maximum(top, jnp.finfo(F32).min)
    w = [jnp.exp(t - top) for t in stats]
    total = functools.reduce(jnp.add, w)
    inv = 1.0 / jnp.maximum(total, 1.0)
    return [x * inv for x in w], top + jnp.log(total)


def by_owner(stat, n, hl):
    t = stat.T[:n]
    block = lax.broadcasted_iota(jnp.int32, t.shape, 1) // hl
    row = lax.broadcasted_iota(jnp.int32, t.shape, 0)
    out = t
    for r in range(1, n):
        moved = pltpu.roll(pltpu.roll(t, r * hl, 1), n - r, 0)
        out = jnp.where((block - row + n) % n == r, moved, out)
    return out


def columns(row):
    return jnp.broadcast_to(row, (128, 128)).T


def scaled(w, i, o):
    hl, lat = o.shape
    return jnp.concatenate([w[i * hl:(i + 1) * hl]] * (lat // 128), axis=1) * o.astype(F32)


def kernel(n, len_hbm, q_ref, ct_ref, o_ref, len_ref, qraw, qg, od, st, two, twos, inc, ins, lg, rs, rss, cbuf, tally,
           cache_sem, q_send, q_recv, mate_recv, o_send, o_recv):
    chips = n // CORES
    nb, hl, wd = q_ref.shape
    lat = wd - ROPE
    heads = n * hl
    sl = ct_ref.shape[2]
    nc = nb // CHUNK
    half = CHUNK // 2
    npair = nb // 2

    me = lax.axis_index('dcp')
    x = me // CORES
    k = me % CORES
    partner = x * CORES + (1 - k)

    def dev(step, core):
        return ((x + step + chips) % chips) * CORES + core

    def wait_bytes(like, sem):
        pltpu.make_async_copy(like, like, sem).wait()

    def cache_copies(pair, par):
        slot = (pair % PAIRS) * 2 + par
        b = pair * 2 + par
        if par == 0:
            return [pltpu.make_async_copy(ct_ref.at[b], cbuf.at[slot, pl.ds(0, wd)], cache_sem.at[pair % PAIRS])]
        return [
            pltpu.make_async_copy(ct_ref.at[b, pl.ds(0, lat)], cbuf.at[slot, pl.ds(0, lat)], cache_sem.at[pair % PAIRS]),
            pltpu.make_async_copy(ct_ref.at[b, pl.ds(lat, ROPE)], cbuf.at[slot, pl.ds(wd, ROPE)], cache_sem.at[pair % PAIRS]),
        ]

    def fetch(pair):
        for par in range(2):
            for cp in cache_copies(pair, par):
                cp.start()

    def raw(i):
        part = pl.ds(i * CHUNK, CHUNK if i < 2 else nb - 2 * CHUNK)
        return pltpu.make_async_copy(q_ref.at[part], qraw.at[part], cache_sem.at[i])

    for i in range(3):
        raw(i).start()
    lengths = pltpu.make_async_copy(len_hbm, len_ref, cache_sem.at[3])
    lengths.start()

    barrier = pltpu.get_barrier_semaphore()
    peers = [dev(1, k), dev(-1, k), partner]
    for peer in peers:
        pl.semaphore_signal(barrier, inc=1, device_id={'dcp': peer}, device_id_type=MESH)

    def pack(g, _):
        for par in range(2):
            qg[me, g, :, pl.ds(par * lat, lat)] = qraw[2 * g + par, :, pl.ds(0, lat)]
        r0 = qraw[2 * g, :, pl.ds(lat, ROPE)]
        r1 = qraw[2 * g + 1, :, pl.ds(lat, ROPE)]
        qg[me, g, :, pl.ds(2 * lat, 2 * ROPE)] = jnp.concatenate([r0, r1], axis=1)
        return 0

    raw(0).wait()
    lax.fori_loop(0, half, pack, 0)
    pl.semaphore_wait(barrier, len(peers))

    def q_copy(kind, src, c, to):
        part = qg.at[src, pl.ds(c * half, half)]
        return pltpu.make_async_remote_copy(
            src_ref=part, dst_ref=part, send_sem=q_send, recv_sem=mate_recv.at[c // 2] if kind == MATE else q_recv.at[kind, c],
            device_id={'dcp': to}, device_id_type=MESH)

    def q_wait(kind, count, c):
        wait_bytes(qg.at[pl.ds(0, count), pl.ds(c * half, half)], q_recv.at[kind, c])

    def sign(c):
        return 1 - 2 * (c % 2)

    def q0(c, _):
        @pl.when(c + 1 < nc)
        def _():
            for i in (1, 2):
                @pl.when(c == i - 1)
                def _():
                    raw(i).wait()

            lax.fori_loop((c + 1) * half, (c + 2) * half, pack, 0)

        q_copy(NEAR, me, c, dev(1, k)).start()
        q_copy(NEAR, me, c, dev(-1, k)).start()
        q_copy(MATE, me, c, partner).start()
        return 0

    lax.fori_loop(0, AHEAD, q0, 0)

    lengths.wait()
    for g in range(PAIRS):
        fetch(g)
        cbuf[2 * g, pl.ds(wd, ROPE), :] = jnp.zeros((ROPE, sl), BF16)
        cbuf[2 * g + 1, pl.ds(lat, ROPE), :] = jnp.zeros((ROPE, sl), BF16)

    def q1(c, _):
        way = -sign(c)
        q_wait(NEAR, 2, c)
        q_copy(FAR, dev(-way, k), c, dev(way, k)).start()
        q_copy(MATE, dev(-1, k), c, partner).start()
        q_copy(MATE, dev(1, k), c, partner).start()

        @pl.when(c + AHEAD < nc)
        def _():
            q0(c + AHEAD, 0)

        return 0

    lax.fori_loop(0, LEAD, q1, 0)

    def q2(c):
        q_wait(FAR, 1, c)
        q_copy(MATE, dev(2, k), c, partner).start()

    def q3(c):
        @pl.when(c % 2 == 0)
        def _():
            wait_bytes(qg.at[pl.ds(0, chips), pl.ds(c * half, 2 * half)], mate_recv.at[c // 2])

    lane = lax.broadcasted_iota(jnp.int32, (heads, 128), 1)
    where_t = lax.broadcasted_iota(jnp.int32, (1, sl), 1)
    base = me * sl

    def arrive(g):
        wait_bytes(cbuf.at[pl.ds((g % PAIRS) * 2, 2), pl.ds(0, wd)], cache_sem.at[g % PAIRS])

    def scores(g, par):
        b = g * 2 + par
        slot = (g % PAIRS) * 2 + par
        qa = qg[:, g, :, pl.ds(par * lat, lat)].reshape(heads, lat)
        qr = qg[:, g, :, pl.ds(2 * lat, 2 * ROPE)].reshape(heads, 2 * ROPE)
        s = jnp.dot(qa, cbuf[slot, pl.ds(0, lat), :], preferred_element_type=F32)
        s = s + jnp.dot(qr, cbuf[slot, pl.ds(lat, 2 * ROPE), :], preferred_element_type=F32)
        return jnp.where(where_t < len_ref[b] - base, s * SCALE, -jnp.inf)

    def finish(g, par, s):
        b = g * 2 + par
        slot = (g % PAIRS) * 2 + par
        m = jnp.maximum(jnp.max(s, axis=1, keepdims=True), jnp.finfo(F32).min)
        p = jnp.exp(s - m)
        l = jnp.sum(p, axis=1, keepdims=True)
        pv = lax.dot_general(p.astype(BF16), cbuf[slot, pl.ds(0, lat), :], (((1,), (1,)), ((), ())),
                             preferred_element_type=F32)
        o = (pv * (1.0 / jnp.maximum(l, 1.0))).astype(BF16)
        od[:, b] = o.reshape(chips, CORES, hl, lat)
        return m + jnp.log(l)

    def attend(c):
        stat = jnp.full((heads, 128), -jnp.inf, F32)
        first = c * half
        arrive(first)
        s0 = scores(first, 0)
        for i in range(half):
            g = first + i
            if i + 1 < half:
                arrive(g + 1)
            s1 = scores(g, 1)
            stat = jnp.where(lane == 2 * i, finish(g, 0, s0), stat)
            if i + 1 < half:
                s0 = scores(g + 1, 0)
            stat = jnp.where(lane == 2 * i + 1, finish(g, 1, s1), stat)

            @pl.when(g + PAIRS < npair)
            def _():
                fetch(g + PAIRS)

        lse = by_owner(stat, n, hl)
        for j in range(n):
            st[j // CORES, c, j % CORES] = lse[j:j + 1]

    def rows(c):
        return pl.ds(c * CHUNK, CHUNK)

    row = 128 * 4
    block = CHUNK * hl * lat * 2 // row

    def arrived(recv, c):
        return q_recv.at[{FOR_RELAY: FAR, FOR_MERGE: NEAR}[recv], c] if recv >= FOR_RELAY else o_recv.at[c]

    def o_copies(c, send, recv, src, srcs, dst, dsts, to):
        return [
            pltpu.make_async_remote_copy(
                src_ref=src, dst_ref=dst, send_sem=o_send.at[send], recv_sem=arrived(recv, c),
                device_id={'dcp': to}, device_id_type=MESH),
            pltpu.make_async_remote_copy(
                src_ref=srcs, dst_ref=dsts, send_sem=o_send.at[ROWS], recv_sem=arrived(recv, c),
                device_id={'dcp': to}, device_id_type=MESH),
        ]

    def o_wait(c, recv, count):
        wait_bytes(tally.at[pl.ds(0, count)], arrived(recv, c))

    def to_chip(c, kind, head, step):
        return o_copies(c, TWO, kind, od.at[head, rows(c)], st.at[head, c], two.at[kind, rows(c)], twos.at[kind, c],
                        dev(step, k))

    def to_partner(c, kind, src, srcs):
        recv = FOR_RELAY if kind in (PASS, VIA2) else FOR_MERGE
        return o_copies(c, ONE, recv, src, srcs, inc.at[kind - MINE, rows(c)], ins.at[kind, c], partner)

    def chip(step):
        return (x + step + chips) % chips

    def sends(c):
        way = sign(c)
        relayed = chip(way)
        return (to_chip(c, VIA, chip(2), way)
                + to_partner(c, PASS, od.at[relayed, rows(c), 1 - k], st.at[relayed, c, 1 - k])
                + to_partner(c, MINE, od.at[x, rows(c), 1 - k], st.at[x, c, 1 - k])
                + to_chip(c, DIRECT, chip(-way), -way))

    def share(c, kind):
        return to_partner(c, kind + VIA2, two.at[kind, rows(c), 1 - k], twos.at[kind, c, 1 - k])

    def pass_on(c):
        o_wait(c, VIA, 4 * (block + 1))
        for cp in share(c, VIA) + share(c, DIRECT):
            cp.start()

    def sum_copies(c):
        return o_copies(c, TOTAL, FOR_MERGE, rs.at[rows(c)], rss.at[c], lg.at[rows(c)], ins.at[SUM, c], dev(sign(c), k))

    def relay(c):
        o_wait(c, FOR_RELAY, 2 * (block + 1))
        mine = chip(sign(c))
        w, lse = weights([st[mine, c, k], ins[PASS, c], twos[VIA, c, k], ins[VIA2, c]])
        w = [columns(r) for r in w]
        for i in range(CHUNK):
            b = c * CHUNK + i
            acc = scaled(w[0], i, od[mine, b, k])
            acc = acc + scaled(w[1], i, inc[PASS - MINE, b])
            acc = acc + scaled(w[2], i, two[VIA, b, k])
            acc = acc + scaled(w[3], i, inc[VIA2 - MINE, b])
            rs[b] = acc
        rss[c] = lse
        for cp in sum_copies(c):
            cp.start()

    def merge(c):
        o_wait(c, FOR_MERGE, 4 * block + 3)
        w, _ = weights([st[x, c, k], ins[MINE, c], twos[DIRECT, c, k], ins[DIRECT2, c], ins[SUM, c]])
        w = [columns(r) for r in w]
        for i in range(CHUNK):
            b = c * CHUNK + i
            acc = scaled(w[0], i, od[x, b, k])
            acc = acc + scaled(w[1], i, inc[MINE - MINE, b])
            acc = acc + scaled(w[2], i, two[DIRECT, b, k])
            acc = acc + scaled(w[3], i, inc[DIRECT2 - MINE, b])
            acc = acc + scaled(w[4], i, lg[b])
            o_ref[b] = acc.astype(BF16)

    def step(t, _):
        @pl.when(t + LEAD < nc)
        def _():
            q1(t + LEAD, 0)

        @pl.when(t < nc)
        def _():
            @pl.when(t == 0)
            def _():
                q2(0)

            @pl.when(t + 1 < nc)
            def _():
                q2(t + 1)

            q3(t)
            attend(t)
            for cp in sends(t):
                cp.start()

        @pl.when(jnp.logical_and(t >= LAG_V, t < nc + LAG_V))
        def _():
            pass_on(t - LAG_V)

        @pl.when(jnp.logical_and(t >= LAG_R, t < nc + LAG_R))
        def _():
            relay(t - LAG_R)

        @pl.when(t >= LAG_F)
        def _():
            merge(t - LAG_F)

        return 0

    lax.fori_loop(0, nc + LAG_F, step, 0)

    wait_bytes(qg.at[pl.ds(0, n - 1)], q_send)
    wait_bytes(two, o_send.at[TWO])
    wait_bytes(inc, o_send.at[ONE])
    wait_bytes(lg, o_send.at[TOTAL])
    wait_bytes(tally.at[pl.ds(0, nc * (2 * CORES + 5))], o_send.at[ROWS])


def solution(mesh):
    n = mesh.shape['dcp']

    def local(q, cache, lengths):
        nb, hl, wd = q.shape
        sl = cache.shape[1]
        lat = wd - ROPE
        nc = nb // CHUNK
        anyspace = pl.BlockSpec(memory_space=pl.ANY)
        dma = pltpu.SemaphoreType.DMA
        return pl.pallas_call(
            functools.partial(kernel, n),
            out_shape=pltpu.VMEM((nb, hl, lat), BF16),
            in_specs=[anyspace, anyspace, anyspace],
            out_specs=pl.BlockSpec(memory_space=pltpu.VMEM),
            scratch_shapes=[
                pltpu.SMEM((nb,), jnp.int32),
                pltpu.VMEM((nb, hl, wd), BF16),
                pltpu.VMEM((n, nb // 2, hl, 2 * wd), BF16),
                pltpu.VMEM((n // CORES, nb, CORES, hl, lat), BF16),
                pltpu.VMEM((n // CORES, nc, CORES, 1, 128), F32),
                pltpu.VMEM((2, nb, CORES, hl, lat), BF16),
                pltpu.VMEM((2, nc, CORES, 1, 128), F32),
                pltpu.VMEM((4, nb, hl, lat), BF16),
                pltpu.VMEM((7, nc, 1, 128), F32),
                pltpu.VMEM((nb, hl, lat), F32),
                pltpu.VMEM((nb, hl, lat), F32),
                pltpu.VMEM((nc, 1, 128), F32),
                pltpu.VMEM((2 * PAIRS, wd + ROPE, sl), BF16),
                pltpu.VMEM((4 * CHUNK * hl * lat // 256 + 4, 1, 128), F32),
                dma((PAIRS,)),
                dma,
                dma((2, nc)),
                dma((nc // 2,)),
                dma((4,)),
                dma((nc,)),
            ],
            compiler_params=pltpu.CompilerParams(
                collective_id=0, has_side_effects=True, vmem_limit_bytes=56 * 1024 * 1024),
            name='mla_decode',
        )(lengths, q, jnp.swapaxes(cache, 1, 2))

    return jax.shard_map(local, mesh=mesh, in_specs=(P('dp', 'dcp', None), P('dp', 'dcp', None), P('dp')),
                         out_specs=P('dp', 'dcp', None), check_vma=False)
```

```python
import functools

import jax
import jax.numpy as jnp
from jax import lax
from jax.experimental import pallas as pl
from jax.experimental.pallas import tpu as pltpu
from jax.sharding import PartitionSpec as P

ROPE = 64
SCALE = 192 ** -0.5
CORES = 2
CHUNK = 8
PAIRS = 4
AHEAD = 4
LEAD = 3
LAG_V = 2
LAG_R = 3
LAG_F = 6

MESH = pl.DeviceIdType.MESH
F32 = jnp.float32
BF16 = jnp.bfloat16
VIA, DIRECT, MINE, PASS, VIA2, DIRECT2, SUM = range(7)
FOR_RELAY, FOR_MERGE = 2, 3
TWO, ONE, TOTAL, ROWS = range(4)
NEAR, FAR, MATE, OWN = range(4)


def weights(stats):
    top = functools.reduce(jnp.maximum, stats)
    top = jnp.maximum(top, jnp.finfo(F32).min)
    w = [jnp.exp(t - top) for t in stats]
    total = functools.reduce(jnp.add, w)
    inv = 1.0 / jnp.maximum(total, 1.0)
    return [x * inv for x in w], top + jnp.log(total)


def by_owner(stat, n, hl):
    t = stat.T[:n]
    block = lax.broadcasted_iota(jnp.int32, t.shape, 1) // hl
    row = lax.broadcasted_iota(jnp.int32, t.shape, 0)
    out = t
    for r in range(1, n):
        moved = pltpu.roll(pltpu.roll(t, r * hl, 1), n - r, 0)
        out = jnp.where((block - row + n) % n == r, moved, out)
    return out


def columns(row):
    return jnp.broadcast_to(row, (128, 128)).T


def scaled(w, i, o):
    hl, lat = o.shape
    return jnp.concatenate([w[i * hl:(i + 1) * hl]] * (lat // 128), axis=1) * o.astype(F32)


def kernel(n, len_hbm, q_ref, ct_ref, o_ref, len_ref, qraw, qg, od, st, two, twos, inc, ins, lg, rs, rss, cbuf, tally,
           cache_sem, q_send, q_recv, mate_recv, o_send, o_recv):
    chips = n // CORES
    nb, hl, wd = q_ref.shape
    lat = wd - ROPE
    heads = n * hl
    sl = ct_ref.shape[2]
    nc = nb // CHUNK
    half = CHUNK // 2
    npair = nb // 2

    me = lax.axis_index('dcp')
    x = me // CORES
    k = me % CORES
    partner = x * CORES + (1 - k)

    def dev(step, core):
        return ((x + step + chips) % chips) * CORES + core

    def wait_bytes(like, sem):
        pltpu.make_async_copy(like, like, sem).wait()

    def cache_copies(pair, par):
        slot = (pair % PAIRS) * 2 + par
        b = pair * 2 + par
        if par == 0:
            return [pltpu.make_async_copy(ct_ref.at[b], cbuf.at[slot, pl.ds(0, wd)], cache_sem.at[pair % PAIRS])]
        return [
            pltpu.make_async_copy(ct_ref.at[b, pl.ds(0, lat)], cbuf.at[slot, pl.ds(0, lat)], cache_sem.at[pair % PAIRS]),
            pltpu.make_async_copy(ct_ref.at[b, pl.ds(lat, ROPE)], cbuf.at[slot, pl.ds(wd, ROPE)], cache_sem.at[pair % PAIRS]),
        ]

    def fetch(pair):
        for par in range(2):
            for cp in cache_copies(pair, par):
                cp.start()

    def raw(i):
        part = pl.ds(i * CHUNK, CHUNK if i < 2 else nb - 2 * CHUNK)
        return pltpu.make_async_copy(q_ref.at[part], qraw.at[part], cache_sem.at[i])

    for i in range(3):
        raw(i).start()
    lengths = pltpu.make_async_copy(len_hbm, len_ref, cache_sem.at[3])
    lengths.start()

    barrier = pltpu.get_barrier_semaphore()
    peers = [dev(1, 0), dev(1, 1), dev(-1, 0), dev(-1, 1), partner]
    for peer in peers:
        pl.semaphore_signal(barrier, inc=1, device_id={'dcp': peer}, device_id_type=MESH)

    def pack(g, _):
        for par in range(2):
            qg[me, g, :, pl.ds(par * lat, lat)] = qraw[2 * g + par, :, pl.ds(0, lat)]
        r0 = qraw[2 * g, :, pl.ds(lat, ROPE)]
        r1 = qraw[2 * g + 1, :, pl.ds(lat, ROPE)]
        qg[me, g, :, pl.ds(2 * lat, 2 * ROPE)] = jnp.concatenate([r0, r1], axis=1)
        return 0

    raw(0).wait()
    lax.fori_loop(0, half, pack, 0)
    pl.semaphore_wait(barrier, len(peers))

    def q_copy(kind, src, c, to):
        part = qg.at[src, pl.ds(c * half, half)]
        return pltpu.make_async_remote_copy(
            src_ref=part, dst_ref=part, send_sem=q_send.at[c // (nc - 1)], recv_sem=q_arrived(kind, c),
            device_id={'dcp': to}, device_id_type=MESH)

    def q_arrived(kind, c):
        if kind == OWN:
            return mate_recv.at[c // 2 + c // (nc - 1)]
        return mate_recv.at[c // 2] if kind == MATE else q_recv.at[kind, c]

    def q_wait(kind, count, c):
        wait_bytes(qg.at[pl.ds(0, count), pl.ds(c * half, half)], q_recv.at[kind, c])

    def sign(c):
        return 1 - 2 * (c % 2)

    def q0(c, _):
        @pl.when(c + 1 < nc)
        def _():
            for i in (1, 2):
                @pl.when(c == i - 1)
                def _():
                    raw(i).wait()

            lax.fori_loop((c + 1) * half, (c + 2) * half, pack, 0)

        @pl.when(jnp.logical_or(c < nc - 1, k == 1))
        def _():
            q_copy(NEAR, me, c, dev(1, k)).start()
            q_copy(NEAR, me, c, dev(-1, k)).start()

        q_copy(OWN, me, c, partner).start()

        @pl.when(c == nc - 1)
        def _():
            wait_bytes(qg.at[0, pl.ds(c * half, half)], q_arrived(OWN, nc - 1))

            @pl.when(k == 1)
            def _():
                q_copy(NEAR, partner, c, dev(1, 0)).start()
                q_copy(NEAR, partner, c, dev(-1, 0)).start()

        return 0

    lax.fori_loop(0, AHEAD, q0, 0)

    lengths.wait()
    for g in range(PAIRS):
        fetch(g)
        cbuf[2 * g, pl.ds(wd, ROPE), :] = jnp.zeros((ROPE, sl), BF16)
        cbuf[2 * g + 1, pl.ds(lat, ROPE), :] = jnp.zeros((ROPE, sl), BF16)

    def q1(c, _):
        way = -sign(c)
        q_wait(NEAR, 2, c)
        q_copy(FAR, dev(-way, k), c, dev(way, k)).start()
        q_copy(MATE, dev(-1, k), c, partner).start()
        q_copy(MATE, dev(1, k), c, partner).start()

        @pl.when(c + AHEAD < nc)
        def _():
            q0(c + AHEAD, 0)

        return 0

    lax.fori_loop(0, LEAD, q1, 0)

    def q2(c):
        q_wait(FAR, 1, c)
        q_copy(MATE, dev(2, k), c, partner).start()

    def q3(c):
        @pl.when(jnp.logical_and(c % 2 == 0, c < nc - 2))
        def _():
            wait_bytes(qg.at[pl.ds(0, chips), pl.ds(c * half, 2 * half)], mate_recv.at[c // 2])

        @pl.when(c == nc - 2)
        def _():
            wait_bytes(qg.at[pl.ds(0, 2 * chips - 1), pl.ds(c * half, half)], mate_recv.at[c // 2])

    lane = lax.broadcasted_iota(jnp.int32, (heads, 128), 1)
    where_t = lax.broadcasted_iota(jnp.int32, (1, sl), 1)
    base = me * sl

    def arrive(g):
        wait_bytes(cbuf.at[pl.ds((g % PAIRS) * 2, 2), pl.ds(0, wd)], cache_sem.at[g % PAIRS])

    def scores(g, par):
        b = g * 2 + par
        slot = (g % PAIRS) * 2 + par
        qa = qg[:, g, :, pl.ds(par * lat, lat)].reshape(heads, lat)
        qr = qg[:, g, :, pl.ds(2 * lat, 2 * ROPE)].reshape(heads, 2 * ROPE)
        s = jnp.dot(qa, cbuf[slot, pl.ds(0, lat), :], preferred_element_type=F32)
        s = s + jnp.dot(qr, cbuf[slot, pl.ds(lat, 2 * ROPE), :], preferred_element_type=F32)
        return jnp.where(where_t < len_ref[b] - base, s * SCALE, -jnp.inf)

    def finish(g, par, s):
        b = g * 2 + par
        slot = (g % PAIRS) * 2 + par
        m = jnp.maximum(jnp.max(s, axis=1, keepdims=True), jnp.finfo(F32).min)
        p = jnp.exp(s - m)
        l = jnp.sum(p, axis=1, keepdims=True)
        pv = lax.dot_general(p.astype(BF16), cbuf[slot, pl.ds(0, lat), :], (((1,), (1,)), ((), ())),
                             preferred_element_type=F32)
        o = (pv * (1.0 / jnp.maximum(l, 1.0))).astype(BF16)
        od[:, b] = o.reshape(chips, CORES, hl, lat)
        return m + jnp.log(l)

    def attend(c):
        stat = jnp.full((heads, 128), -jnp.inf, F32)
        first = c * half
        arrive(first)
        s0 = scores(first, 0)
        for i in range(half):
            g = first + i
            if i + 1 < half:
                arrive(g + 1)
            s1 = scores(g, 1)
            stat = jnp.where(lane == 2 * i, finish(g, 0, s0), stat)
            if i + 1 < half:
                s0 = scores(g + 1, 0)
            stat = jnp.where(lane == 2 * i + 1, finish(g, 1, s1), stat)

            @pl.when(g + PAIRS < npair)
            def _():
                fetch(g + PAIRS)

        lse = by_owner(stat, n, hl)
        for j in range(n):
            st[j // CORES, c, j % CORES] = lse[j:j + 1]

    def rows(c):
        return pl.ds(c * CHUNK, CHUNK)

    row = 128 * 4
    block = CHUNK * hl * lat * 2 // row

    def arrived(recv, c):
        return q_recv.at[{FOR_RELAY: FAR, FOR_MERGE: NEAR}[recv], c] if recv >= FOR_RELAY else o_recv.at[c]

    def o_copies(c, send, recv, src, srcs, dst, dsts, to):
        return [
            pltpu.make_async_remote_copy(
                src_ref=src, dst_ref=dst, send_sem=o_send.at[send], recv_sem=arrived(recv, c),
                device_id={'dcp': to}, device_id_type=MESH),
            pltpu.make_async_remote_copy(
                src_ref=srcs, dst_ref=dsts, send_sem=o_send.at[ROWS], recv_sem=arrived(recv, c),
                device_id={'dcp': to}, device_id_type=MESH),
        ]

    def o_wait(c, recv, count):
        wait_bytes(tally.at[pl.ds(0, count)], arrived(recv, c))

    def to_chip(c, kind, head, step):
        return o_copies(c, TWO, kind, od.at[head, rows(c)], st.at[head, c], two.at[kind, rows(c)], twos.at[kind, c],
                        dev(step, k))

    def to_partner(c, kind, src, srcs):
        recv = FOR_RELAY if kind in (PASS, VIA2) else FOR_MERGE
        return o_copies(c, ONE, recv, src, srcs, inc.at[kind - MINE, rows(c)], ins.at[kind, c], partner)

    def chip(step):
        return (x + step + chips) % chips

    def sends(c):
        way = sign(c)
        relayed = chip(way)
        return (to_chip(c, VIA, chip(2), way)
                + to_partner(c, PASS, od.at[relayed, rows(c), 1 - k], st.at[relayed, c, 1 - k])
                + to_partner(c, MINE, od.at[x, rows(c), 1 - k], st.at[x, c, 1 - k])
                + to_chip(c, DIRECT, chip(-way), -way))

    def share(c, kind):
        return to_partner(c, kind + VIA2, two.at[kind, rows(c), 1 - k], twos.at[kind, c, 1 - k])

    def pass_on(c):
        o_wait(c, VIA, 4 * (block + 1))
        for cp in share(c, VIA) + share(c, DIRECT):
            cp.start()

    def sum_copies(c):
        return o_copies(c, TOTAL, FOR_MERGE, rs.at[rows(c)], rss.at[c], lg.at[rows(c)], ins.at[SUM, c], dev(sign(c), k))

    def relay(c):
        o_wait(c, FOR_RELAY, 2 * (block + 1))
        mine = chip(sign(c))
        w, lse = weights([st[mine, c, k], ins[PASS, c], twos[VIA, c, k], ins[VIA2, c]])
        w = [columns(r) for r in w]
        for i in range(CHUNK):
            b = c * CHUNK + i
            acc = scaled(w[0], i, od[mine, b, k])
            acc = acc + scaled(w[1], i, inc[PASS - MINE, b])
            acc = acc + scaled(w[2], i, two[VIA, b, k])
            acc = acc + scaled(w[3], i, inc[VIA2 - MINE, b])
            rs[b] = acc
        rss[c] = lse
        for cp in sum_copies(c):
            cp.start()

    def merge(c):
        o_wait(c, FOR_MERGE, 4 * block + 3)
        w, _ = weights([st[x, c, k], ins[MINE, c], twos[DIRECT, c, k], ins[DIRECT2, c], ins[SUM, c]])
        w = [columns(r) for r in w]
        for i in range(CHUNK):
            b = c * CHUNK + i
            acc = scaled(w[0], i, od[x, b, k])
            acc = acc + scaled(w[1], i, inc[MINE - MINE, b])
            acc = acc + scaled(w[2], i, two[DIRECT, b, k])
            acc = acc + scaled(w[3], i, inc[DIRECT2 - MINE, b])
            acc = acc + scaled(w[4], i, lg[b])
            o_ref[b] = acc.astype(BF16)

    def step(t, _):
        @pl.when(t + LEAD < nc)
        def _():
            q1(t + LEAD, 0)

        @pl.when(t < nc)
        def _():
            @pl.when(t == 0)
            def _():
                q2(0)

            @pl.when(t + 1 < nc)
            def _():
                q2(t + 1)

            q3(t)
            attend(t)
            for cp in sends(t):
                cp.start()

        @pl.when(jnp.logical_and(t >= LAG_V, t < nc + LAG_V))
        def _():
            pass_on(t - LAG_V)

        @pl.when(jnp.logical_and(t >= LAG_R, t < nc + LAG_R))
        def _():
            relay(t - LAG_R)

        @pl.when(t >= LAG_F)
        def _():
            merge(t - LAG_F)

        return 0

    lax.fori_loop(0, nc + LAG_F, step, 0)

    wait_bytes(qg.at[pl.ds(0, 7), pl.ds(0, (nc - 1) * half)], q_send.at[0])

    @pl.when(k == 0)
    def _():
        wait_bytes(qg.at[pl.ds(0, 5), pl.ds(0, half)], q_send.at[1])

    @pl.when(k == 1)
    def _():
        wait_bytes(qg.at[pl.ds(0, 3), pl.ds(0, 3 * half)], q_send.at[1])

    wait_bytes(two, o_send.at[TWO])
    wait_bytes(inc, o_send.at[ONE])
    wait_bytes(lg, o_send.at[TOTAL])
    wait_bytes(tally.at[pl.ds(0, nc * (2 * CORES + 5))], o_send.at[ROWS])


def solution(mesh):
    n = mesh.shape['dcp']

    def local(q, cache, lengths):
        nb, hl, wd = q.shape
        sl = cache.shape[1]
        lat = wd - ROPE
        nc = nb // CHUNK
        anyspace = pl.BlockSpec(memory_space=pl.ANY)
        dma = pltpu.SemaphoreType.DMA
        return pl.pallas_call(
            functools.partial(kernel, n),
            out_shape=pltpu.VMEM((nb, hl, lat), BF16),
            in_specs=[anyspace, anyspace, anyspace],
            out_specs=pl.BlockSpec(memory_space=pltpu.VMEM),
            scratch_shapes=[
                pltpu.SMEM((nb,), jnp.int32),
                pltpu.VMEM((nb, hl, wd), BF16),
                pltpu.VMEM((n, nb // 2, hl, 2 * wd), BF16),
                pltpu.VMEM((n // CORES, nb, CORES, hl, lat), BF16),
                pltpu.VMEM((n // CORES, nc, CORES, 1, 128), F32),
                pltpu.VMEM((2, nb, CORES, hl, lat), BF16),
                pltpu.VMEM((2, nc, CORES, 1, 128), F32),
                pltpu.VMEM((4, nb, hl, lat), BF16),
                pltpu.VMEM((7, nc, 1, 128), F32),
                pltpu.VMEM((nb, hl, lat), F32),
                pltpu.VMEM((nb, hl, lat), F32),
                pltpu.VMEM((nc, 1, 128), F32),
                pltpu.VMEM((2 * PAIRS, wd + ROPE, sl), BF16),
                pltpu.VMEM((4 * CHUNK * hl * lat // 256 + 4, 1, 128), F32),
                dma((PAIRS,)),
                dma((2,)),
                dma((2, nc)),
                dma((nc // 2 + 1,)),
                dma((4,)),
                dma((nc,)),
            ],
            compiler_params=pltpu.CompilerParams(
                collective_id=0, has_side_effects=True, vmem_limit_bytes=56 * 1024 * 1024),
            name='mla_decode',
        )(lengths, q, jnp.swapaxes(cache, 1, 2))

    return jax.shard_map(local, mesh=mesh, in_specs=(P('dp', 'dcp', None), P('dp', 'dcp', None), P('dp')),
                         out_specs=P('dp', 'dcp', None), check_vma=False)
```

```python
import functools

import jax
import jax.numpy as jnp
from jax import lax
from jax.experimental import pallas as pl
from jax.experimental.pallas import tpu as pltpu
from jax.sharding import PartitionSpec as P

ROPE = 64
SCALE = 192 ** -0.5
CORES = 2
CHUNK = 8
PAIRS = 4
AHEAD = 4
LEAD = 3
LAG_V = 2
LAG_R = 3
LAG_F = 6

MESH = pl.DeviceIdType.MESH
F32 = jnp.float32
BF16 = jnp.bfloat16
VIA, DIRECT, MINE, PASS, VIA2, DIRECT2, SUM = range(7)
FOR_RELAY, FOR_MERGE = 2, 3
TWO, ONE, TOTAL, ROWS = range(4)
NEAR, FAR, MATE, OWN = range(4)


def weights(stats):
    top = functools.reduce(jnp.maximum, stats)
    top = jnp.maximum(top, jnp.finfo(F32).min)
    w = [jnp.exp(t - top) for t in stats]
    total = functools.reduce(jnp.add, w)
    inv = 1.0 / jnp.maximum(total, 1.0)
    return [x * inv for x in w], top + jnp.log(total)


def by_owner(stat, n, hl):
    t = stat.T[:n]
    block = lax.broadcasted_iota(jnp.int32, t.shape, 1) // hl
    row = lax.broadcasted_iota(jnp.int32, t.shape, 0)
    out = t
    for r in range(1, n):
        moved = pltpu.roll(pltpu.roll(t, r * hl, 1), n - r, 0)
        out = jnp.where((block - row + n) % n == r, moved, out)
    return out


def columns(row):
    return jnp.broadcast_to(row, (128, 128)).T


def scaled(w, i, o):
    hl, lat = o.shape
    return jnp.concatenate([w[i * hl:(i + 1) * hl]] * (lat // 128), axis=1) * o.astype(F32)


def kernel(n, len_hbm, q_ref, ct_ref, o_ref, len_ref, qraw, qg, od, st, two, twos, inc, ins, lg, rs, rss, cbuf, tally,
           cache_sem, q_send, q_recv, mate_recv, o_send, o_recv):
    chips = n // CORES
    nb, hl, wd = q_ref.shape
    lat = wd - ROPE
    heads = n * hl
    sl = ct_ref.shape[2]
    nc = nb // CHUNK
    half = CHUNK // 2
    npair = nb // 2

    me = lax.axis_index('dcp')
    x = me // CORES
    k = me % CORES
    partner = x * CORES + (1 - k)

    def dev(step, core):
        return ((x + step + chips) % chips) * CORES + core

    def wait_bytes(like, sem):
        pltpu.make_async_copy(like, like, sem).wait()

    def cache_copies(pair, par):
        slot = (pair % PAIRS) * 2 + par
        b = pair * 2 + par
        if par == 0:
            return [pltpu.make_async_copy(ct_ref.at[b], cbuf.at[slot, pl.ds(0, wd)], cache_sem.at[pair % PAIRS])]
        return [
            pltpu.make_async_copy(ct_ref.at[b, pl.ds(0, lat)], cbuf.at[slot, pl.ds(0, lat)], cache_sem.at[pair % PAIRS]),
            pltpu.make_async_copy(ct_ref.at[b, pl.ds(lat, ROPE)], cbuf.at[slot, pl.ds(wd, ROPE)], cache_sem.at[pair % PAIRS]),
        ]

    def fetch(pair):
        for par in range(2):
            for cp in cache_copies(pair, par):
                cp.start()

    def raw(i):
        part = pl.ds(i * CHUNK, CHUNK if i < 2 else nb - 2 * CHUNK)
        return pltpu.make_async_copy(q_ref.at[part], qraw.at[part], cache_sem.at[i])

    for i in range(3):
        raw(i).start()
    lengths = pltpu.make_async_copy(len_hbm, len_ref, cache_sem.at[3])
    lengths.start()

    barrier = pltpu.get_barrier_semaphore()
    peers = [dev(1, 0), dev(1, 1), dev(-1, 0), dev(-1, 1), partner]
    for peer in peers:
        pl.semaphore_signal(barrier, inc=1, device_id={'dcp': peer}, device_id_type=MESH)

    def pack(g, _):
        for par in range(2):
            qg[me, g, :, pl.ds(par * lat, lat)] = qraw[2 * g + par, :, pl.ds(0, lat)]
        r0 = qraw[2 * g, :, pl.ds(lat, ROPE)]
        r1 = qraw[2 * g + 1, :, pl.ds(lat, ROPE)]
        qg[me, g, :, pl.ds(2 * lat, 2 * ROPE)] = jnp.concatenate([r0, r1], axis=1)
        return 0

    raw(0).wait()
    lax.fori_loop(0, half, pack, 0)
    pl.semaphore_wait(barrier, len(peers))

    def q_copy(kind, src, c, to, skip=0, count=half):
        part = qg.at[src, pl.ds(c * half + skip, count)]
        return pltpu.make_async_remote_copy(
            src_ref=part, dst_ref=part, send_sem=q_send.at[c // (nc - 1)], recv_sem=q_arrived(kind, c),
            device_id={'dcp': to}, device_id_type=MESH)

    def q_arrived(kind, c):
        if kind == OWN:
            return mate_recv.at[c // 2 + c // (nc - 1)]
        return mate_recv.at[c // 2] if kind == MATE else q_recv.at[kind, c]

    def q_wait(kind, count, c):
        wait_bytes(qg.at[pl.ds(0, count), pl.ds(c * half, half)], q_recv.at[kind, c])

    def sign(c):
        return 1 - 2 * (c % 2)

    def q0(c, _):
        @pl.when(c + 1 < nc)
        def _():
            for i in (1, 2):
                @pl.when(c == i - 1)
                def _():
                    raw(i).wait()

            lax.fori_loop((c + 1) * half, (c + 2) * half, pack, 0)

        @pl.when(jnp.logical_or(c < nc - 1, k == 1))
        def _():
            q_copy(NEAR, me, c, dev(1, k)).start()
            q_copy(NEAR, me, c, dev(-1, k)).start()

        @pl.when(jnp.logical_and(c == nc - 1, k == 0))
        def _():
            q_copy(NEAR, me, c, dev(1, 0), 0, half // 2).start()
            q_copy(NEAR, me, c, dev(-1, 0), 0, half // 2).start()

        q_copy(OWN, me, c, partner).start()

        @pl.when(c == nc - 1)
        def _():
            wait_bytes(qg.at[0, pl.ds(c * half, half)], q_arrived(OWN, nc - 1))

            @pl.when(k == 1)
            def _():
                q_copy(NEAR, partner, c, dev(1, 0), half // 2, half // 2).start()
                q_copy(NEAR, partner, c, dev(-1, 0), half // 2, half // 2).start()

        return 0

    lax.fori_loop(0, AHEAD, q0, 0)

    lengths.wait()
    for g in range(PAIRS):
        fetch(g)
        cbuf[2 * g, pl.ds(wd, ROPE), :] = jnp.zeros((ROPE, sl), BF16)
        cbuf[2 * g + 1, pl.ds(lat, ROPE), :] = jnp.zeros((ROPE, sl), BF16)

    def q1(c, _):
        way = -sign(c)
        q_wait(NEAR, 2, c)
        q_copy(FAR, dev(-way, k), c, dev(way, k)).start()
        q_copy(MATE, dev(-1, k), c, partner).start()
        q_copy(MATE, dev(1, k), c, partner).start()

        @pl.when(c + AHEAD < nc)
        def _():
            q0(c + AHEAD, 0)

        return 0

    lax.fori_loop(0, LEAD, q1, 0)

    def q2(c):
        q_wait(FAR, 1, c)
        q_copy(MATE, dev(2, k), c, partner).start()

    def q3(c):
        @pl.when(jnp.logical_and(c % 2 == 0, c < nc - 2))
        def _():
            wait_bytes(qg.at[pl.ds(0, chips), pl.ds(c * half, 2 * half)], mate_recv.at[c // 2])

        @pl.when(c == nc - 2)
        def _():
            wait_bytes(qg.at[pl.ds(0, 2 * chips - 1), pl.ds(c * half, half)], mate_recv.at[c // 2])

    lane = lax.broadcasted_iota(jnp.int32, (heads, 128), 1)
    where_t = lax.broadcasted_iota(jnp.int32, (1, sl), 1)
    base = me * sl

    def arrive(g):
        wait_bytes(cbuf.at[pl.ds((g % PAIRS) * 2, 2), pl.ds(0, wd)], cache_sem.at[g % PAIRS])

    def scores(g, par):
        b = g * 2 + par
        slot = (g % PAIRS) * 2 + par
        qa = qg[:, g, :, pl.ds(par * lat, lat)].reshape(heads, lat)
        qr = qg[:, g, :, pl.ds(2 * lat, 2 * ROPE)].reshape(heads, 2 * ROPE)
        s = jnp.dot(qa, cbuf[slot, pl.ds(0, lat), :], preferred_element_type=F32)
        s = s + jnp.dot(qr, cbuf[slot, pl.ds(lat, 2 * ROPE), :], preferred_element_type=F32)
        return jnp.where(where_t < len_ref[b] - base, s * SCALE, -jnp.inf)

    def finish(g, par, s):
        b = g * 2 + par
        slot = (g % PAIRS) * 2 + par
        m = jnp.maximum(jnp.max(s, axis=1, keepdims=True), jnp.finfo(F32).min)
        p = jnp.exp(s - m)
        l = jnp.sum(p, axis=1, keepdims=True)
        pv = lax.dot_general(p.astype(BF16), cbuf[slot, pl.ds(0, lat), :], (((1,), (1,)), ((), ())),
                             preferred_element_type=F32)
        o = (pv * (1.0 / jnp.maximum(l, 1.0))).astype(BF16)
        od[:, b] = o.reshape(chips, CORES, hl, lat)
        return m + jnp.log(l)

    def attend(c):
        stat = jnp.full((heads, 128), -jnp.inf, F32)
        first = c * half
        arrive(first)
        s0 = scores(first, 0)
        for i in range(half):
            g = first + i
            if i + 1 < half:
                arrive(g + 1)
            s1 = scores(g, 1)
            stat = jnp.where(lane == 2 * i, finish(g, 0, s0), stat)
            if i + 1 < half:
                s0 = scores(g + 1, 0)
            stat = jnp.where(lane == 2 * i + 1, finish(g, 1, s1), stat)

            @pl.when(g + PAIRS < npair)
            def _():
                fetch(g + PAIRS)

        lse = by_owner(stat, n, hl)
        for j in range(n):
            st[j // CORES, c, j % CORES] = lse[j:j + 1]

    def rows(c):
        return pl.ds(c * CHUNK, CHUNK)

    row = 128 * 4
    block = CHUNK * hl * lat * 2 // row

    def arrived(recv, c):
        return q_recv.at[{FOR_RELAY: FAR, FOR_MERGE: NEAR}[recv], c] if recv >= FOR_RELAY else o_recv.at[c]

    def o_copies(c, send, recv, src, srcs, dst, dsts, to):
        return [
            pltpu.make_async_remote_copy(
                src_ref=src, dst_ref=dst, send_sem=o_send.at[send], recv_sem=arrived(recv, c),
                device_id={'dcp': to}, device_id_type=MESH),
            pltpu.make_async_remote_copy(
                src_ref=srcs, dst_ref=dsts, send_sem=o_send.at[ROWS], recv_sem=arrived(recv, c),
                device_id={'dcp': to}, device_id_type=MESH),
        ]

    def o_wait(c, recv, count):
        wait_bytes(tally.at[pl.ds(0, count)], arrived(recv, c))

    def to_chip(c, kind, head, step):
        return o_copies(c, TWO, kind, od.at[head, rows(c)], st.at[head, c], two.at[kind, rows(c)], twos.at[kind, c],
                        dev(step, k))

    def to_partner(c, kind, src, srcs):
        recv = FOR_RELAY if kind in (PASS, VIA2) else FOR_MERGE
        return o_copies(c, ONE, recv, src, srcs, inc.at[kind - MINE, rows(c)], ins.at[kind, c], partner)

    def chip(step):
        return (x + step + chips) % chips

    def sends(c):
        way = sign(c)
        relayed = chip(way)
        return (to_chip(c, VIA, chip(2), way)
                + to_partner(c, PASS, od.at[relayed, rows(c), 1 - k], st.at[relayed, c, 1 - k])
                + to_partner(c, MINE, od.at[x, rows(c), 1 - k], st.at[x, c, 1 - k])
                + to_chip(c, DIRECT, chip(-way), -way))

    def share(c, kind):
        return to_partner(c, kind + VIA2, two.at[kind, rows(c), 1 - k], twos.at[kind, c, 1 - k])

    def pass_on(c):
        o_wait(c, VIA, 4 * (block + 1))
        for cp in share(c, VIA) + share(c, DIRECT):
            cp.start()

    def sum_copies(c):
        return o_copies(c, TOTAL, FOR_MERGE, rs.at[rows(c)], rss.at[c], lg.at[rows(c)], ins.at[SUM, c], dev(sign(c), k))

    def relay(c):
        o_wait(c, FOR_RELAY, 2 * (block + 1))
        mine = chip(sign(c))
        w, lse = weights([st[mine, c, k], ins[PASS, c], twos[VIA, c, k], ins[VIA2, c]])
        w = [columns(r) for r in w]
        for i in range(CHUNK):
            b = c * CHUNK + i
            acc = scaled(w[0], i, od[mine, b, k])
            acc = acc + scaled(w[1], i, inc[PASS - MINE, b])
            acc = acc + scaled(w[2], i, two[VIA, b, k])
            acc = acc + scaled(w[3], i, inc[VIA2 - MINE, b])
            rs[b] = acc
        rss[c] = lse
        for cp in sum_copies(c):
            cp.start()

    def merge(c):
        o_wait(c, FOR_MERGE, 4 * block + 3)
        w, _ = weights([st[x, c, k], ins[MINE, c], twos[DIRECT, c, k], ins[DIRECT2, c], ins[SUM, c]])
        w = [columns(r) for r in w]
        for i in range(CHUNK):
            b = c * CHUNK + i
            acc = scaled(w[0], i, od[x, b, k])
            acc = acc + scaled(w[1], i, inc[MINE - MINE, b])
            acc = acc + scaled(w[2], i, two[DIRECT, b, k])
            acc = acc + scaled(w[3], i, inc[DIRECT2 - MINE, b])
            acc = acc + scaled(w[4], i, lg[b])
            o_ref[b] = acc.astype(BF16)

    def step(t, _):
        @pl.when(t + LEAD < nc)
        def _():
            q1(t + LEAD, 0)

        @pl.when(t < nc)
        def _():
            @pl.when(t == 0)
            def _():
                q2(0)

            @pl.when(t + 1 < nc)
            def _():
                q2(t + 1)

            q3(t)
            attend(t)
            for cp in sends(t):
                cp.start()

        @pl.when(jnp.logical_and(t >= LAG_V, t < nc + LAG_V))
        def _():
            pass_on(t - LAG_V)

        @pl.when(jnp.logical_and(t >= LAG_R, t < nc + LAG_R))
        def _():
            relay(t - LAG_R)

        @pl.when(t >= LAG_F)
        def _():
            merge(t - LAG_F)

        return 0

    lax.fori_loop(0, nc + LAG_F, step, 0)

    wait_bytes(qg.at[pl.ds(0, 7), pl.ds(0, (nc - 1) * half)], q_send.at[0])

    @pl.when(k == 0)
    def _():
        wait_bytes(qg.at[pl.ds(0, 6), pl.ds(0, half)], q_send.at[1])

    @pl.when(k == 1)
    def _():
        wait_bytes(qg.at[pl.ds(0, 8), pl.ds(0, half)], q_send.at[1])

    wait_bytes(two, o_send.at[TWO])
    wait_bytes(inc, o_send.at[ONE])
    wait_bytes(lg, o_send.at[TOTAL])
    wait_bytes(tally.at[pl.ds(0, nc * (2 * CORES + 5))], o_send.at[ROWS])


def solution(mesh):
    n = mesh.shape['dcp']

    def local(q, cache, lengths):
        nb, hl, wd = q.shape
        sl = cache.shape[1]
        lat = wd - ROPE
        nc = nb // CHUNK
        anyspace = pl.BlockSpec(memory_space=pl.ANY)
        dma = pltpu.SemaphoreType.DMA
        return pl.pallas_call(
            functools.partial(kernel, n),
            out_shape=pltpu.VMEM((nb, hl, lat), BF16),
            in_specs=[anyspace, anyspace, anyspace],
            out_specs=pl.BlockSpec(memory_space=pltpu.VMEM),
            scratch_shapes=[
                pltpu.SMEM((nb,), jnp.int32),
                pltpu.VMEM((nb, hl, wd), BF16),
                pltpu.VMEM((n, nb // 2, hl, 2 * wd), BF16),
                pltpu.VMEM((n // CORES, nb, CORES, hl, lat), BF16),
                pltpu.VMEM((n // CORES, nc, CORES, 1, 128), F32),
                pltpu.VMEM((2, nb, CORES, hl, lat), BF16),
                pltpu.VMEM((2, nc, CORES, 1, 128), F32),
                pltpu.VMEM((4, nb, hl, lat), BF16),
                pltpu.VMEM((7, nc, 1, 128), F32),
                pltpu.VMEM((nb, hl, lat), F32),
                pltpu.VMEM((nb, hl, lat), F32),
                pltpu.VMEM((nc, 1, 128), F32),
                pltpu.VMEM((2 * PAIRS, wd + ROPE, sl), BF16),
                pltpu.VMEM((4 * CHUNK * hl * lat // 256 + 4, 1, 128), F32),
                dma((PAIRS,)),
                dma((2,)),
                dma((2, nc)),
                dma((nc // 2 + 1,)),
                dma((4,)),
                dma((nc,)),
            ],
            compiler_params=pltpu.CompilerParams(
                collective_id=0, has_side_effects=True, vmem_limit_bytes=56 * 1024 * 1024),
            name='mla_decode',
        )(lengths, q, jnp.swapaxes(cache, 1, 2))

    return jax.shard_map(local, mesh=mesh, in_specs=(P('dp', 'dcp', None), P('dp', 'dcp', None), P('dp')),
                         out_specs=P('dp', 'dcp', None), check_vma=False)
```

```python
import functools

import jax
import jax.numpy as jnp
from jax import lax
from jax.experimental import pallas as pl
from jax.experimental.pallas import tpu as pltpu
from jax.sharding import PartitionSpec as P

ROPE = 64
SCALE = 192 ** -0.5
CORES = 2
CHUNK = 8
PAIRS = 4
AHEAD = 4
LEAD = 3
LAG_V = 2
LAG_R = 3
LAG_F = 6

MESH = pl.DeviceIdType.MESH
F32 = jnp.float32
BF16 = jnp.bfloat16
VIA, DIRECT, MINE, PASS, VIA2, DIRECT2, SUM = range(7)
FOR_RELAY, FOR_MERGE = 2, 3
TWO, ONE, TOTAL, ROWS = range(4)
NEAR, FAR, MATE = range(3)


def weights(stats):
    top = functools.reduce(jnp.maximum, stats)
    top = jnp.maximum(top, jnp.finfo(F32).min)
    w = [jnp.exp(t - top) for t in stats]
    total = functools.reduce(jnp.add, w)
    inv = 1.0 / jnp.maximum(total, 1.0)
    return [x * inv for x in w], top + jnp.log(total)


def by_owner(stat, n, hl):
    t = stat.T[:n]
    block = lax.broadcasted_iota(jnp.int32, t.shape, 1) // hl
    row = lax.broadcasted_iota(jnp.int32, t.shape, 0)
    out = t
    for r in range(1, n):
        moved = pltpu.roll(pltpu.roll(t, r * hl, 1), n - r, 0)
        out = jnp.where((block - row + n) % n == r, moved, out)
    return out


def columns(row):
    return jnp.broadcast_to(row, (128, 128)).T


def scaled(w, i, o):
    hl, lat = o.shape
    return jnp.concatenate([w[i * hl:(i + 1) * hl]] * (lat // 128), axis=1) * o.astype(F32)


def kernel(n, len_hbm, q_ref, ct_ref, o_ref, len_ref, qraw, qg, od, st, two, twos, inc, ins, lg, rs, rss, cbuf, tally,
           cache_sem, q_send, q_recv, mate_recv, o_send, o_recv):
    chips = n // CORES
    nb, hl, wd = q_ref.shape
    lat = wd - ROPE
    heads = n * hl
    sl = ct_ref.shape[2]
    nc = nb // CHUNK
    half = CHUNK // 2
    npair = nb // 2

    me = lax.axis_index('dcp')
    x = me // CORES
    k = me % CORES
    partner = x * CORES + (1 - k)

    def dev(step, core):
        return ((x + step + chips) % chips) * CORES + core

    def wait_bytes(like, sem):
        pltpu.make_async_copy(like, like, sem).wait()

    def cache_copies(pair, par):
        slot = (pair % PAIRS) * 2 + par
        b = pair * 2 + par
        if par == 0:
            return [pltpu.make_async_copy(ct_ref.at[b], cbuf.at[slot, pl.ds(0, wd)], cache_sem.at[pair % PAIRS])]
        return [
            pltpu.make_async_copy(ct_ref.at[b, pl.ds(0, lat)], cbuf.at[slot, pl.ds(0, lat)], cache_sem.at[pair % PAIRS]),
            pltpu.make_async_copy(ct_ref.at[b, pl.ds(lat, ROPE)], cbuf.at[slot, pl.ds(wd, ROPE)], cache_sem.at[pair % PAIRS]),
        ]

    def fetch(pair):
        for par in range(2):
            for cp in cache_copies(pair, par):
                cp.start()

    def raw(i):
        part = pl.ds(i * CHUNK, CHUNK if i < 2 else nb - 2 * CHUNK)
        return pltpu.make_async_copy(q_ref.at[part], qraw.at[part], cache_sem.at[i])

    for i in range(3):
        raw(i).start()
    lengths = pltpu.make_async_copy(len_hbm, len_ref, cache_sem.at[3])
    lengths.start()

    barrier = pltpu.get_barrier_semaphore()
    peers = [dev(1, k), dev(-1, k), partner]
    for peer in peers:
        pl.semaphore_signal(barrier, inc=1, device_id={'dcp': peer}, device_id_type=MESH)

    def pack(g, _):
        for par in range(2):
            qg[me, g, :, pl.ds(par * lat, lat)] = qraw[2 * g + par, :, pl.ds(0, lat)]
        r0 = qraw[2 * g, :, pl.ds(lat, ROPE)]
        r1 = qraw[2 * g + 1, :, pl.ds(lat, ROPE)]
        qg[me, g, :, pl.ds(2 * lat, 2 * ROPE)] = jnp.concatenate([r0, r1], axis=1)
        return 0

    raw(0).wait()
    lax.fori_loop(0, half, pack, 0)
    pl.semaphore_wait(barrier, len(peers))

    def q_copy(kind, src, c, to):
        part = qg.at[src, pl.ds(c * half, half)]
        return pltpu.make_async_remote_copy(
            src_ref=part, dst_ref=part, send_sem=q_send, recv_sem=mate_recv.at[c // 2] if kind == MATE else q_recv.at[kind, c],
            device_id={'dcp': to}, device_id_type=MESH)

    def q_wait(kind, count, c):
        wait_bytes(qg.at[pl.ds(0, count), pl.ds(c * half, half)], q_recv.at[kind, c])

    def sign(c):
        return 1 - 2 * (c % 2)

    def q0(c, _):
        q_copy(NEAR, me, c, dev(1, k)).start()
        q_copy(NEAR, me, c, dev(-1, k)).start()
        q_copy(MATE, me, c, partner).start()

        @pl.when(c == 0)
        def _():
            raw(1).wait()
            raw(2).wait()
            lax.fori_loop(half, 3 * half, pack, 0)

        @pl.when(jnp.logical_and(c > 0, c + 2 < nc))
        def _():
            lax.fori_loop((c + 2) * half, (c + 3) * half, pack, 0)

        return 0

    lax.fori_loop(0, AHEAD, q0, 0)

    lengths.wait()
    for g in range(PAIRS):
        fetch(g)
        cbuf[2 * g, pl.ds(wd, ROPE), :] = jnp.zeros((ROPE, sl), BF16)
        cbuf[2 * g + 1, pl.ds(lat, ROPE), :] = jnp.zeros((ROPE, sl), BF16)

    def q1(c, _):
        way = -sign(c)
        q_wait(NEAR, 2, c)
        q_copy(FAR, dev(-way, k), c, dev(way, k)).start()
        q_copy(MATE, dev(-1, k), c, partner).start()
        q_copy(MATE, dev(1, k), c, partner).start()

        @pl.when(c + AHEAD < nc)
        def _():
            q0(c + AHEAD, 0)

        return 0

    lax.fori_loop(0, LEAD, q1, 0)

    def q2(c):
        q_wait(FAR, 1, c)
        q_copy(MATE, dev(2, k), c, partner).start()

    def q3(c):
        @pl.when(c % 2 == 0)
        def _():
            wait_bytes(qg.at[pl.ds(0, chips), pl.ds(c * half, 2 * half)], mate_recv.at[c // 2])

    lane = lax.broadcasted_iota(jnp.int32, (heads, 128), 1)
    where_t = lax.broadcasted_iota(jnp.int32, (1, sl), 1)
    base = me * sl

    def arrive(g):
        wait_bytes(cbuf.at[pl.ds((g % PAIRS) * 2, 2), pl.ds(0, wd)], cache_sem.at[g % PAIRS])

    def scores(g, par):
        b = g * 2 + par
        slot = (g % PAIRS) * 2 + par
        qa = qg[:, g, :, pl.ds(par * lat, lat)].reshape(heads, lat)
        qr = qg[:, g, :, pl.ds(2 * lat, 2 * ROPE)].reshape(heads, 2 * ROPE)
        s = jnp.dot(qa, cbuf[slot, pl.ds(0, lat), :], preferred_element_type=F32)
        s = s + jnp.dot(qr, cbuf[slot, pl.ds(lat, 2 * ROPE), :], preferred_element_type=F32)
        return jnp.where(where_t < len_ref[b] - base, s * SCALE, -jnp.inf)

    def finish(g, par, s):
        b = g * 2 + par
        slot = (g % PAIRS) * 2 + par
        m = jnp.maximum(jnp.max(s, axis=1, keepdims=True), jnp.finfo(F32).min)
        p = jnp.exp(s - m)
        l = jnp.sum(p, axis=1, keepdims=True)
        pv = lax.dot_general(p.astype(BF16), cbuf[slot, pl.ds(0, lat), :], (((1,), (1,)), ((), ())),
                             preferred_element_type=F32)
        o = (pv * (1.0 / jnp.maximum(l, 1.0))).astype(BF16)
        od[:, b] = o.reshape(chips, CORES, hl, lat)
        return m + jnp.log(l)

    def attend(c):
        stat = jnp.full((heads, 128), -jnp.inf, F32)
        first = c * half
        arrive(first)
        s0 = scores(first, 0)
        for i in range(half):
            g = first + i
            if i + 1 < half:
                arrive(g + 1)
            s1 = scores(g, 1)
            stat = jnp.where(lane == 2 * i, finish(g, 0, s0), stat)
            if i + 1 < half:
                s0 = scores(g + 1, 0)
            stat = jnp.where(lane == 2 * i + 1, finish(g, 1, s1), stat)

            @pl.when(g + PAIRS < npair)
            def _():
                fetch(g + PAIRS)

        lse = by_owner(stat, n, hl)
        for j in range(n):
            st[j // CORES, c, j % CORES] = lse[j:j + 1]

    def rows(c):
        return pl.ds(c * CHUNK, CHUNK)

    row = 128 * 4
    block = CHUNK * hl * lat * 2 // row

    def arrived(recv, c):
        return q_recv.at[{FOR_RELAY: FAR, FOR_MERGE: NEAR}[recv], c] if recv >= FOR_RELAY else o_recv.at[c]

    def o_copies(c, send, recv, src, srcs, dst, dsts, to):
        return [
            pltpu.make_async_remote_copy(
                src_ref=src, dst_ref=dst, send_sem=o_send.at[send], recv_sem=arrived(recv, c),
                device_id={'dcp': to}, device_id_type=MESH),
            pltpu.make_async_remote_copy(
                src_ref=srcs, dst_ref=dsts, send_sem=o_send.at[ROWS], recv_sem=arrived(recv, c),
                device_id={'dcp': to}, device_id_type=MESH),
        ]

    def o_wait(c, recv, count):
        wait_bytes(tally.at[pl.ds(0, count)], arrived(recv, c))

    def to_chip(c, kind, head, step):
        return o_copies(c, TWO, kind, od.at[head, rows(c)], st.at[head, c], two.at[kind, rows(c)], twos.at[kind, c],
                        dev(step, k))

    def to_partner(c, kind, src, srcs):
        recv = FOR_RELAY if kind in (PASS, VIA2) else FOR_MERGE
        return o_copies(c, ONE, recv, src, srcs, inc.at[kind - MINE, rows(c)], ins.at[kind, c], partner)

    def chip(step):
        return (x + step + chips) % chips

    def sends(c):
        way = sign(c)
        relayed = chip(way)
        return (to_chip(c, VIA, chip(2), way)
                + to_partner(c, PASS, od.at[relayed, rows(c), 1 - k], st.at[relayed, c, 1 - k])
                + to_partner(c, MINE, od.at[x, rows(c), 1 - k], st.at[x, c, 1 - k])
                + to_chip(c, DIRECT, chip(-way), -way))

    def share(c, kind):
        return to_partner(c, kind + VIA2, two.at[kind, rows(c), 1 - k], twos.at[kind, c, 1 - k])

    def pass_on(c):
        o_wait(c, VIA, 4 * (block + 1))
        for cp in share(c, VIA) + share(c, DIRECT):
            cp.start()

    def sum_copies(c):
        return o_copies(c, TOTAL, FOR_MERGE, rs.at[rows(c)], rss.at[c], lg.at[rows(c)], ins.at[SUM, c], dev(sign(c), k))

    def relay(c):
        o_wait(c, FOR_RELAY, 2 * (block + 1))
        mine = chip(sign(c))
        w, lse = weights([st[mine, c, k], ins[PASS, c], twos[VIA, c, k], ins[VIA2, c]])
        w = [columns(r) for r in w]
        for i in range(CHUNK):
            b = c * CHUNK + i
            acc = scaled(w[0], i, od[mine, b, k])
            acc = acc + scaled(w[1], i, inc[PASS - MINE, b])
            acc = acc + scaled(w[2], i, two[VIA, b, k])
            acc = acc + scaled(w[3], i, inc[VIA2 - MINE, b])
            rs[b] = acc
        rss[c] = lse
        for cp in sum_copies(c):
            cp.start()

    def merge(c):
        o_wait(c, FOR_MERGE, 4 * block + 3)
        w, _ = weights([st[x, c, k], ins[MINE, c], twos[DIRECT, c, k], ins[DIRECT2, c], ins[SUM, c]])
        w = [columns(r) for r in w]
        for i in range(CHUNK):
            b = c * CHUNK + i
            acc = scaled(w[0], i, od[x, b, k])
            acc = acc + scaled(w[1], i, inc[MINE - MINE, b])
            acc = acc + scaled(w[2], i, two[DIRECT, b, k])
            acc = acc + scaled(w[3], i, inc[DIRECT2 - MINE, b])
            acc = acc + scaled(w[4], i, lg[b])
            o_ref[b] = acc.astype(BF16)

    def step(t, _):
        @pl.when(t + LEAD < nc)
        def _():
            q1(t + LEAD, 0)

        @pl.when(t < nc)
        def _():
            @pl.when(t == 0)
            def _():
                q2(0)

            @pl.when(t + 1 < nc)
            def _():
                q2(t + 1)

            q3(t)
            attend(t)
            for cp in sends(t):
                cp.start()

        @pl.when(jnp.logical_and(t >= LAG_V, t < nc + LAG_V))
        def _():
            pass_on(t - LAG_V)

        @pl.when(jnp.logical_and(t >= LAG_R, t < nc + LAG_R))
        def _():
            relay(t - LAG_R)

        @pl.when(t >= LAG_F)
        def _():
            merge(t - LAG_F)

        return 0

    lax.fori_loop(0, nc + LAG_F, step, 0)

    wait_bytes(qg.at[pl.ds(0, n - 1)], q_send)
    wait_bytes(two, o_send.at[TWO])
    wait_bytes(inc, o_send.at[ONE])
    wait_bytes(lg, o_send.at[TOTAL])
    wait_bytes(tally.at[pl.ds(0, nc * (2 * CORES + 5))], o_send.at[ROWS])


def solution(mesh):
    n = mesh.shape['dcp']

    def local(q, cache, lengths):
        nb, hl, wd = q.shape
        sl = cache.shape[1]
        lat = wd - ROPE
        nc = nb // CHUNK
        anyspace = pl.BlockSpec(memory_space=pl.ANY)
        dma = pltpu.SemaphoreType.DMA
        return pl.pallas_call(
            functools.partial(kernel, n),
            out_shape=pltpu.VMEM((nb, hl, lat), BF16),
            in_specs=[anyspace, anyspace, anyspace],
            out_specs=pl.BlockSpec(memory_space=pltpu.VMEM),
            scratch_shapes=[
                pltpu.SMEM((nb,), jnp.int32),
                pltpu.VMEM((nb, hl, wd), BF16),
                pltpu.VMEM((n, nb // 2, hl, 2 * wd), BF16),
                pltpu.VMEM((n // CORES, nb, CORES, hl, lat), BF16),
                pltpu.VMEM((n // CORES, nc, CORES, 1, 128), F32),
                pltpu.VMEM((2, nb, CORES, hl, lat), BF16),
                pltpu.VMEM((2, nc, CORES, 1, 128), F32),
                pltpu.VMEM((4, nb, hl, lat), BF16),
                pltpu.VMEM((7, nc, 1, 128), F32),
                pltpu.VMEM((nb, hl, lat), F32),
                pltpu.VMEM((nb, hl, lat), F32),
                pltpu.VMEM((nc, 1, 128), F32),
                pltpu.VMEM((2 * PAIRS, wd + ROPE, sl), BF16),
                pltpu.VMEM((4 * CHUNK * hl * lat // 256 + 4, 1, 128), F32),
                dma((PAIRS,)),
                dma,
                dma((2, nc)),
                dma((nc // 2,)),
                dma((4,)),
                dma((nc,)),
            ],
            compiler_params=pltpu.CompilerParams(
                collective_id=0, has_side_effects=True, vmem_limit_bytes=56 * 1024 * 1024),
            name='mla_decode',
        )(lengths, q, jnp.swapaxes(cache, 1, 2))

    return jax.shard_map(local, mesh=mesh, in_specs=(P('dp', 'dcp', None), P('dp', 'dcp', None), P('dp')),
                         out_specs=P('dp', 'dcp', None), check_vma=False)
```
